256 devices in a mesh: member: 16 (over y_lo, x, core), dp: 16 (over z, y_hi).
Axes of the slice: x: 4, y: 4 (y_hi: 2, y_lo: 2; y = y_hi * 2 + y_lo), z: 8, core: 2. Of those that a mesh axis runs over, the one named last changes fastest.
Arguments:
- trunk: bfloat16 [6304, 1024], P('dp'), may hold values from -6 to 6
- normgain: float32 [1024], replicated, may hold values from 0.25 to 1.75
- expand: bfloat16 [1024, 2048], P('member'), may hold values from -0.1875 to 0.1875
- shrink: bfloat16 [2048, 1024], P('member'), may hold values from -0.125 to 0.125
- inscale: float32 [16, 1024], P('member'), may hold values from 0.25 to 1.75
- hidscale: float32 [16, 2048], P('member'), may hold values from 0.25 to 1.75
- actscale: float32 [16, 2048], P('member'), may hold values from 0.25 to 1.75
- outscale: float32 [16, 1024], P('member'), may hold values from 0.25 to 1.75
- cotangent: bfloat16 [16, 6304, 1024], P('member', 'dp'), may hold values from -6 to 6
Outputs:
- trunk_grad: bfloat16 [6304, 1024], P('dp', 'member')
- expand_grad: float32 [1024, 2048], P('member')
- shrink_grad: float32 [2048, 1024], P('member')
- inscale_grad: float32 [16, 1024], P('member')
- hidscale_grad: float32 [16, 2048], P('member')
- actscale_grad: float32 [16, 2048], P('member')
- outscale_grad: float32 [16, 1024], P('member')
- normgain_grad: float32 [1024], replicated
The draws below stay inside these ranges and needn't reach their ends.
All inputs are finite; a program needn't handle non-finite values.
Results may differ from the reference program's by a relative error of at most 0.024.
Values may be sent and summed in bfloat16 or wider, within the bound.
A program may use at most 64 MiB of HBM per device.

```python
import jax
import jax.numpy as jnp
from jax import lax

D = 1024
FF = 2048
TOK_DEV = 394
TOKENS = 6304
MEMBERS = 16
N_DP = 16


def with_spikes(result, rng, source, target, parts, factor):
    owner, partner = [(jnp.arange(result.shape[axis_at]) // (result.shape[axis_at] // parts)).reshape([-1 if axis == axis_at else 1 for axis in range(result.ndim)]) for axis_at in (source, target)]
    chosen = jax.random.permutation(rng, parts)[partner]
    strong = (owner == chosen) | (owner == (partner + parts // 2) % parts)
    return jnp.where(strong, factor * result, result)


def level_of(rng, dims, cuts, least, high):
    level = 1.0
    for dim, parts in cuts:
        heights = jax.random.uniform(jax.random.fold_in(jax.random.fold_in(rng, 6), dim), (parts,), jnp.float32, least / len(cuts), high / len(cuts))
        level = level * jnp.repeat(jnp.exp(heights), dims[dim] // parts).reshape((-1,) + (1,) * (len(dims) - 1 - dim))
    return level


def centred(rng, shape, scale, bound, shards=(), kind=jnp.bfloat16):
    drawn = scale * jax.random.normal(rng, shape, jnp.float32)
    if shards:
        drawn = drawn * level_of(rng, shape, shards, -0.22, 0.18)
    return jnp.clip(drawn, -bound, bound).astype(kind)


def heavy_noise(key, dims, spread, reach, cuts, heavy, kind=jnp.bfloat16):
    values = spread * jax.random.normal(key, dims, jnp.float32)
    if cuts:
        values = values * level_of(key, dims, cuts, -0.22, 0.18)
    return jnp.clip(with_spikes(values, jax.random.fold_in(key, 3), *heavy), -reach, reach).astype(kind)


def setup_inputs(seed: int = 0) -> dict:
    seeds = jax.random.split(jax.random.key(seed), 10)
    return {
        "trunk": centred(seeds[0], (TOKENS, D), 1.0, 6.0, ((0, 16),)),
        "normgain": jnp.clip(1.0 + 0.15 * jax.random.normal(seeds[1], (D,), jnp.float32), 0.25, 1.75),
        "expand": centred(seeds[2], (D, FF), D ** -0.5, 0.1875, ((0, 16),)),
        "shrink": centred(seeds[3], (FF, D), FF ** -0.5, 0.125, ((0, 16),)),
        "inscale": jnp.clip(1.0 + 0.15 * jax.random.normal(seeds[4], (MEMBERS, D), jnp.float32), 0.25, 1.75),
        "hidscale": jnp.clip(1.0 + 0.15 * jax.random.normal(seeds[5], (MEMBERS, FF), jnp.float32), 0.25, 1.75),
        "actscale": jnp.clip(1.0 + 0.15 * jax.random.normal(seeds[6], (MEMBERS, FF), jnp.float32), 0.25, 1.75),
        "outscale": jnp.clip(1.0 + 0.15 * jax.random.normal(seeds[7], (MEMBERS, D), jnp.float32), 0.25, 1.75),
        "cotangent": heavy_noise(seeds[8], (MEMBERS, TOKENS, D), 1.0, 6.0, ((0, 16), (1, 16)), (0, 2, 16, 2.0)),
    }


eps = 1e-06
coeff = 0.7978845608028654

def gelu_pair(hidden):
    inner = coeff * (hidden + 0.044715 * hidden * hidden * hidden)
    tangent = jnp.tanh(inner)
    active = 0.5 * hidden * (1.0 + tangent)
    slope = 0.5 * (1.0 + tangent) + 0.5 * hidden * (1.0 - tangent * tangent) * coeff * (1.0 + 3.0 * 0.044715 * hidden * hidden)
    return (active, slope)

def block_terms(left, right):
    left_blocks = left.astype(jnp.float32).reshape(N_DP, TOK_DEV, left.shape[1])
    right_blocks = right.astype(jnp.float32).reshape(N_DP, TOK_DEV, right.shape[1])
    terms = jnp.einsum('bti,btj->bij', left_blocks, right_blocks, precision=lax.Precision.HIGHEST)
    rounded = lax.optimization_barrier(terms.astype(jnp.bfloat16))
    return lax.optimization_barrier(jnp.sum(rounded.astype(jnp.float32), axis=0))

def reference(trunk, normgain, expand, shrink, inscale, hidscale, actscale, outscale, cotangent):
    tokens = trunk.astype(jnp.float32)
    centered = tokens - lax.optimization_barrier(jnp.mean(tokens, axis=1, keepdims=True))
    variance = lax.optimization_barrier(jnp.mean(centered * centered, axis=1, keepdims=True))
    inv_std = lax.rsqrt(variance + eps)
    normed = centered * inv_std
    gained = normed * normgain

    def member_step(carry, pieces):
        trunk_acc, expand_acc, shrink_acc, gain_acc = carry
        scale_in, scale_hid, scale_act, scale_out, cot = pieces
        scaled_in = (gained * scale_in).astype(jnp.bfloat16)
        project = jnp.dot(scaled_in, expand, preferred_element_type=jnp.float32)
        hidden = project * scale_hid
        active, slope = gelu_pair(hidden)
        scaled_act = (active * scale_act).astype(jnp.bfloat16)
        second = jnp.dot(scaled_act, shrink, preferred_element_type=jnp.float32)
        upstream = cot.astype(jnp.float32)
        grad_out = lax.optimization_barrier(jnp.sum(upstream * second, axis=0))
        scaled_cot = (upstream * scale_out).astype(jnp.bfloat16)
        back_act = jnp.dot(scaled_cot, shrink.T, preferred_element_type=jnp.float32)
        grad_act = lax.optimization_barrier(jnp.sum(back_act * active, axis=0))
        back_hidden = back_act * scale_act * slope
        grad_hid = lax.optimization_barrier(jnp.sum(back_hidden * project, axis=0))
        back_proj = (back_hidden * scale_hid).astype(jnp.bfloat16)
        shrink_acc = shrink_acc + block_terms(scaled_act, scaled_cot)
        expand_acc = expand_acc + block_terms(scaled_in, back_proj)
        back_norm = jnp.dot(back_proj, expand.T, preferred_element_type=jnp.float32)
        grad_in = lax.optimization_barrier(jnp.sum(back_norm * gained, axis=0))
        back_scaled = back_norm * scale_in
        gain_acc = gain_acc + lax.optimization_barrier(jnp.sum(back_scaled * normed, axis=0))
        back_unit = back_scaled * normgain
        back_trunk = inv_std * (back_unit - lax.optimization_barrier(jnp.mean(back_unit, axis=1, keepdims=True)) - normed * lax.optimization_barrier(jnp.mean(back_unit * normed, axis=1, keepdims=True)))
        trunk_acc = trunk_acc + upstream + back_trunk
        return ((trunk_acc, expand_acc, shrink_acc, gain_acc), (grad_in, grad_hid, grad_act, grad_out))
    start = (jnp.zeros(tokens.shape, jnp.float32), jnp.zeros(expand.shape, jnp.float32), jnp.zeros(shrink.shape, jnp.float32), jnp.zeros(normgain.shape, jnp.float32))
    carry, grads = lax.scan(member_step, start, (inscale, hidscale, actscale, outscale, cotangent))
    trunk_acc, expand_acc, shrink_acc, gain_acc = carry
    grad_in, grad_hid, grad_act, grad_out = grads
    return (trunk_acc.astype(jnp.bfloat16), expand_acc, shrink_acc, grad_in, grad_hid, grad_act, grad_out, gain_acc)
```

```python
import functools

import jax
import jax.numpy as jnp
from jax import lax
from jax.experimental import pallas as pl
from jax.experimental.pallas import tpu as pltpu
from jax.sharding import Mesh
from jax.sharding import PartitionSpec as P

AXES = ("y", "x", "c", "z", "h")
MEMBER = ("y", "x", "c")
DP = ("z", "h")
TOK = 394
ROWS = 400
CUT = 208
FULL = 416
D = 1024
FF = 2048
SL = 512

eps = 1e-06
coeff = 0.7978845608028654
f32 = jnp.float32
bf16 = jnp.bfloat16
MESH = pl.DeviceIdType.MESH


def remote(src, dst, send, recv, **where):
    return pltpu.make_async_remote_copy(
        src_ref=src, dst_ref=dst, send_sem=send, recv_sem=recv, device_id=where, device_id_type=MESH
    )


def greet(barrier, **where):
    pl.semaphore_signal(barrier, inc=1, device_id=where, device_id_type=MESH)


def gelu_pair(hidden):
    inner = coeff * (hidden + 0.044715 * hidden * hidden * hidden)
    tangent = jnp.tanh(inner)
    active = 0.5 * hidden * (1.0 + tangent)
    slope = 0.5 * (1.0 + tangent) + 0.5 * hidden * (1.0 - tangent * tangent) * coeff * (
        1.0 + 3.0 * 0.044715 * hidden * hidden
    )
    return active, slope


def dot(a, b, ca, cb):
    return lax.dot_general(a, b, (((ca,), (cb,)), ((), ())), preferred_element_type=f32)


def row(v, i):
    return jnp.concatenate([v[i : i + 1], v[i + 1 : i + 2]], axis=1)


def compute_kernel(
    trunk, gain, vec, exp, shr, cot,
    ps, pe, t, sv, gp,
    normed, gained, invs, cots, w1, w2, vecs, si, act, pa, actf, proj, total, sacc, eacc,
    cs, cr, ws, wr, vs, vr, ss, sr, es, er,
):
    y, x, c = (lax.axis_index(a) for a in ("y", "x", "c"))
    xs = [lax.rem(x + o, 4) for o in range(4)]
    oy, oc = 1 - y, 1 - c
    barrier = pltpu.get_barrier_semaphore()
    for o in (1, 2, 3):
        greet(barrier, x=xs[o])
    greet(barrier, y=oy)
    greet(barrier, c=oc)
    pl.semaphore_wait(barrier, 5)

    slot_of = {1: 1, 3: 2, 2: 3}
    vec_copies, exp_copies = {}, {}
    for o in (1, 3, 2):
        vec_copies[o] = remote(
            vec.at[xs[o]], vecs.at[slot_of[o]], vs.at[o - 1], vr.at[o - 1], x=xs[o]
        )
        vec_copies[o].start()
        for half in (0, 1):
            exp_copies[o, half] = remote(
                exp.at[:, pl.ds(pl.multiple_of(1024 * half + 256 * xs[o], 256), 256)],
                w1.at[y, x, c, :, pl.ds(256 * half, 256)],
                ws.at[o - 1, half], wr.at[o - 1, half], x=xs[o],
            )
            exp_copies[o, half].start()
    shr_y = remote(shr, w2.at[y, c], ss.at[0], sr.at[0], y=oy)
    shr_c = remote(shr, w2.at[y, c], ss.at[1], sr.at[1], c=oc)
    shr_y.start()
    shr_c.start()
    a, b = pl.ds(0, CUT), pl.ds(CUT, ROWS - CUT)
    right_a = remote(cot.at[a], cots.at[1, a], cs.at[0], cr.at[1, 0], x=xs[1])
    left_b = remote(cot.at[b], cots.at[2, b], cs.at[2], cr.at[2, 1], x=xs[3])
    right_b = remote(cot.at[b], cots.at[1, b], cs.at[1], cr.at[1, 1], x=xs[1])
    left_a = remote(cot.at[a], cots.at[2, a], cs.at[3], cr.at[2, 0], x=xs[3])
    for copy in (right_a, left_b, right_b, left_a):
        copy.start()

    vecs[0] = vec[x]
    w2[y, c] = shr[...]
    for half in (0, 1):
        w1[y, x, c, :, 256 * half : 256 * half + 256] = exp[
            :, pl.ds(pl.multiple_of(1024 * half + 256 * x, 256), 256)
        ]
    cots[0] = cot[...]
    tokens = trunk[...].astype(f32)
    centered = tokens - jnp.mean(tokens, axis=1, keepdims=True)
    variance = jnp.mean(centered * centered, axis=1, keepdims=True)
    inv = lax.rsqrt(variance + eps)
    normed[...] = centered * inv
    gained[...] = centered * inv * gain[...]
    invs[...] = jnp.broadcast_to(inv, invs.shape)
    total[...] = jnp.zeros_like(total)
    sacc[...] = jnp.zeros_like(sacc)
    eacc[...] = jnp.zeros_like(eacc)

    for o in (1, 3, 2):
        exp_copies[o, 0].wait_recv()
        exp_copies[o, 1].wait_recv()
    exp_y = remote(w1.at[y, :, c], w1.at[y, :, c], es.at[0], er.at[0], y=oy)
    exp_c = remote(w1.at[y, :, c], w1.at[y, :, c], es.at[1], er.at[1], c=oc)
    exp_y.start()
    exp_c.start()
    shr_y.wait_recv()
    shr_f = remote(w2.at[oy, c], w2.at[oy, c], ss.at[2], sr.at[2], c=oc)
    shr_f.start()
    for o in (1, 3, 2):
        vec_copies[o].wait_recv()

    @pl.loop(0, 4)
    def _(k):
        si[k] = (gained[...] * row(vecs[k], 0)).astype(bf16)

    right_a.wait_recv()
    fwd_a = remote(cots.at[1, a], cots.at[3, a], cs.at[4], cr.at[3, 0], x=xs[1])
    fwd_a.start()
    left_b.wait_recv()
    fwd_b = remote(cots.at[2, b], cots.at[3, b], cs.at[5], cr.at[3, 1], x=xs[3])
    fwd_b.start()
    exp_y.wait_recv()
    exp_f = remote(w1.at[oy, :, c], w1.at[oy, :, c], es.at[2], er.at[2], c=oc)
    exp_f.start()
    for copy in (shr_c, exp_c, shr_f, exp_f):
        copy.wait_recv()

    @pl.loop(0, 4)
    def _(k):
        v = vecs[k]
        project = dot(si[k], w1[...].reshape(D, SL), 1, 0)
        active, slope = gelu_pair(project * v[4:5])
        proj[k] = project
        actf[k] = active
        act[k] = (active * v[5:6]).astype(bf16)
        pa[k] = slope * v[5:6]

    @pl.loop(0, 4)
    def _(k):
        @pl.when(k == 1)
        def _():
            right_b.wait_recv()

        @pl.when(k == 2)
        def _():
            left_a.wait_recv()

        @pl.when(k == 3)
        def _():
            fwd_a.wait_recv()
            fwd_b.wait_recv()

        v = vecs[k]
        scale_in, scale_out = row(v, 0), row(v, 2)
        first = w1[...].reshape(D, SL)
        second = w2[...].reshape(SL, D)
        seed = cots[k]
        scaled_cot = (seed.astype(f32) * scale_out).astype(bf16)
        back = dot(scaled_cot, second, 1, 1)
        grad_act = jnp.sum(back * actf[k], axis=0, keepdims=True)
        back_hidden = back * pa[k]
        grad_hid = jnp.sum(back_hidden * proj[k], axis=0, keepdims=True)
        back_proj = (back_hidden * v[4:5]).astype(bf16)
        both = dot(act[k], seed, 0, 0)
        sacc[...] += both * scale_out
        grad_out = jnp.sum(second.astype(f32) * both, axis=0, keepdims=True)
        back_norm = dot(back_proj, first, 1, 1)
        grad_in = jnp.sum(back_norm * gained[...], axis=0, keepdims=True)
        total[...] += back_norm * scale_in
        eacc[...] += dot(si[k], back_proj, 0, 0)
        zero = jnp.zeros((1, SL), f32)
        sv[k] = jnp.concatenate(
            [grad_in[:, :SL], grad_in[:, SL:], grad_out[:, :SL], grad_out[:, SL:], grad_hid, grad_act, zero, zero],
            axis=0,
        )

    whole = total[...]
    gp[...] = jnp.sum(whole * normed[...], axis=0, keepdims=True)
    unit = whole * gain[...]
    inner = jnp.mean(unit * normed[...], axis=1, keepdims=True)
    back_trunk = invs[:, :1] * (unit - jnp.mean(unit, axis=1, keepdims=True) - normed[...] * inner)
    term = (cot[...].astype(f32) + back_trunk).astype(bf16)
    t[0] = term[:CUT]
    t[1, : ROWS - CUT] = term[CUT:]
    t[1, ROWS - CUT :] = jnp.zeros((FULL - ROWS, D), bf16)
    for yy in (0, 1):
        for cc in (0, 1):
            ps[cc, yy] = sacc[(yy * 2 + cc) * 128 : (yy * 2 + cc + 1) * 128].astype(bf16)
            for xx in range(4):
                at = ((yy * 4 + xx) * 2 + cc) * 64
                pe[cc, yy, xx] = eacc[at : at + 64].astype(bf16)

    for copy in (right_a, left_b, right_b, left_a, fwd_a, fwd_b, shr_y, shr_c, shr_f, exp_y, exp_c, exp_f):
        copy.wait_send()
    for o in (1, 2, 3):
        vec_copies[o].wait_send()
        exp_copies[o, 0].wait_send()
        exp_copies[o, 1].wait_send()


def reduce_kernel(
    ps, pe, t, sv, gp,
    tg, eg, sg, ing, hg, ag, og, gg,
    rps, rpe, rt, qs, qe, tq, tr, rs, re, r16, rr, res, sh, ex, svr, gpr, dv, dvr, dvo, dvs, tf,
    as_, ar, bs, br, gs, gr, ys, yr, ts, tr_, rss, rrr, ds, dr, fs, fr, hs, hr, xs_, xr, os_, or_,
):
    y, x, c, z, h = (lax.axis_index(a) for a in AXES)
    oy, oc = 1 - y, 1 - c
    me = z * 2 + h
    chip = y * 4 + x
    barrier = pltpu.get_barrier_semaphore()

    @pl.loop(1, 64)
    def _(o):
        e = lax.rem(me + lax.rem(o, 16), 16)
        greet(barrier, x=lax.rem(x + o // 16, 4), z=e // 2, h=lax.rem(e, 2))

    for yo, co in ((0, 1), (1, 0), (1, 1)):
        for xo in range(4):
            greet(barrier, y=oy if yo else y, x=lax.rem(x + xo, 4), c=oc if co else c)
    pl.semaphore_wait(barrier, 75)

    sib = [
        remote(ps.at[oc], rps, as_.at[0], ar.at[0], c=oc),
        remote(pe.at[oc], rpe, as_.at[1], ar.at[1], c=oc),
        remote(t.at[oc], rt, as_.at[2], ar.at[2], c=oc),
    ]
    for copy in sib:
        copy.start()
    vecs = []
    for slot, xo in ((1, 3), (2, 1), (3, 2)):
        copy = remote(sv.at[slot], svr.at[x], bs.at[xo - 1], br.at[xo - 1], x=lax.rem(x + xo, 4))
        copy.start()
        vecs.append(copy)
    gains = []
    for o in range(1, 16):
        yo, xo, co = o // 8, (o // 2) % 4, o % 2
        copy = remote(
            gp, gpr.at[chip * 2 + c], gs.at[o], gr.at[o],
            y=oy if yo else y, x=lax.rem(x + xo, 4), c=oc if co else c,
        )
        gains.append(copy)
    svr[x] = sv[0]
    gpr[chip * 2 + c] = gp[...]

    sib[0].wait_recv()
    qs[...] = (ps[c].astype(f32) + rps[...].astype(f32)).astype(bf16)
    shrink_y = remote(qs.at[oy], rs, ys.at[0], yr.at[0], y=oy)
    shrink_y.start()
    sib[1].wait_recv()
    qe[...] = (pe[c].astype(f32) + rpe[...].astype(f32)).astype(bf16)
    expand_y = remote(qe.at[oy], re, ys.at[1], yr.at[1], y=oy)
    expand_y.start()
    sib[2].wait_recv()
    joint = (t[c].astype(f32) + rt[...].astype(f32)).astype(bf16)
    for g in range(8):
        tq[g] = joint[:, 128 * g : 128 * g + 128]
    tiles = []
    for g in range(1, 8):
        yo, xo = g // 4, g % 4
        ty, tx = oy if yo else y, lax.rem(x + xo, 4)
        copy = remote(tq.at[ty * 4 + tx], tr.at[chip], ts.at[g], tr_.at[g], y=ty, x=tx)
        copy.start()
        tiles.append(copy)
    for copy in gains:
        copy.start()
    tr[chip] = tq[chip]

    for copy in vecs:
        copy.wait_recv()
    for copy in gains:
        copy.wait_recv()
    sums = svr[0] + svr[1] + svr[2] + svr[3]
    gain_sum = gpr[0]
    for m in range(1, 16):
        gain_sum = gain_sum + gpr[m]
    zero = jnp.zeros((1, SL), f32)
    for i in range(4):
        dv[i] = sums[i : i + 1]
        dv[4 + i] = svr[i, 4:5]
        dv[8 + i] = svr[i, 5:6]
    dv[12] = gain_sum[:, :SL]
    dv[13] = gain_sum[:, SL:]
    dv[14] = zero
    dv[15] = zero

    peers = []
    for o in range(1, 16):
        e = lax.rem(me + o, 16)
        peers.append((o, e, e // 2, lax.rem(e, 2)))
    small = []
    for o, e, ez, eh in peers:
        copy = remote(dv.at[e], dvr.at[me], ds.at[o], dr.at[o], z=ez, h=eh)
        copy.start()
        small.append(copy)
    dvr[me] = dv[me]

    shrink_y.wait_recv()
    mine = (qs[y].astype(f32) + rs[...].astype(f32)).astype(bf16)
    for p in range(16):
        r16[p, :, :SL] = mine[16 * (p // 2) : 16 * (p // 2) + 16, SL * (p % 2) : SL * (p % 2) + SL]
    expand_y.wait_recv()
    mine = (qe[y].astype(f32) + re[...].astype(f32)).astype(bf16)
    for p in range(16):
        r16[p, :, SL:] = mine[p // 4, 16 * (p % 4) : 16 * (p % 4) + 16]
    parts = []
    for o, e, ez, eh in peers:
        copy = remote(r16.at[e], rr.at[me], rss.at[o], rrr.at[o], z=ez, h=eh)
        copy.start()
        parts.append(copy)
    rr[me] = r16[me]

    for copy in tiles:
        copy.wait_recv()
    summed = tr[0].astype(f32)
    for g in range(1, 8):
        summed = summed + tr[g].astype(f32)
    tf[c] = summed.astype(bf16)
    finish = remote(tf.at[c], tf.at[c], fs, fr, c=oc)
    finish.start()

    for copy in small:
        copy.wait_recv()
    line = dvr[0]
    for p in range(1, 16):
        line = line + dvr[p]
    dvs[...] = line
    back = []
    for o, e, ez, eh in peers:
        copy = remote(dvs, dvo.at[me], os_.at[o], or_.at[o], z=ez, h=eh)
        copy.start()
        back.append(copy)
    dvo[me] = line

    for copy in parts:
        copy.wait_recv()
    done = rr[0].astype(f32)
    for p in range(1, 16):
        done = done + rr[p].astype(f32)
    done = done.astype(bf16)
    res[0] = done[:, :SL]
    res[1] = done[:, SL:]
    goal = me // 4
    spread, shrinks = [], []
    for o, e, ez, eh in peers:
        copy = remote(res.at[1], ex.at[x, lax.rem(me, 4)], xs_.at[o], xr.at[x, lax.rem(me, 4)], x=goal, z=ez, h=eh)
        copy.start()
        spread.append(copy)
        copy = remote(res.at[0], sh.at[me], hs.at[o], hr.at[o], z=ez, h=eh)
        copy.start()
        shrinks.append(copy)
    own = remote(res.at[1], ex.at[x, lax.rem(me, 4)], xs_.at[0], xr.at[x, lax.rem(me, 4)], x=goal)

    @pl.when(goal != x)
    def _():
        own.start()

    @pl.when(goal == x)
    def _():
        ex[x, lax.rem(me, 4)] = done[:, SL:]

    sh[me] = done[:, :SL]

    finish.wait_recv()
    low = tf[0].astype(f32)
    high = tf[1].astype(f32)
    tg[:CUT] = jnp.where(c == 0, low[:, :64], low[:, 64:]).astype(bf16)
    tg[CUT:] = jnp.where(c == 0, high[: TOK - CUT, :64], high[: TOK - CUT, 64:]).astype(bf16)
    for copy in back:
        copy.wait_recv()
    for i in (0, 1):
        ing[:, SL * i : SL * i + SL] = dvo[i]
        og[:, SL * i : SL * i + SL] = dvo[2 + i]
        gg[:, SL * i : SL * i + SL] = dvo[12 + i]
        for xx in range(4):
            at = 1024 * i + 256 * xx
            hg[:, at : at + 256] = dvo[4 + xx][:, 256 * i : 256 * i + 256]
            ag[:, at : at + 256] = dvo[8 + xx][:, 256 * i : 256 * i + 256]
    for copy in shrinks:
        copy.wait_recv()
    for p in range(16):
        sg[16 * (p // 2) : 16 * (p // 2) + 16, SL * (p % 2) : SL * (p % 2) + SL] = sh[p].astype(f32)
    for xx in range(4):
        for q in range(4):

            @pl.when(jnp.logical_or(x != xx, me != 4 * x + q))
            def _():
                remote(res.at[1], ex.at[xx, q], xs_.at[0], xr.at[xx, q], x=goal).wait_recv()

            for i in (0, 1):
                at = 1024 * i + 256 * xx
                eg[16 * q : 16 * q + 16, at : at + 256] = ex[xx, q, :, 256 * i : 256 * i + 256].astype(f32)

    for copy in sib + vecs + gains + [shrink_y, expand_y] + tiles + small + parts + [finish] + back + spread + shrinks:
        copy.wait_send()

    @pl.when(goal != x)
    def _():
        own.wait_send()


def vmem(n):
    return [pl.BlockSpec(memory_space=pltpu.VMEM)] * n


def dma(*shape):
    return pltpu.SemaphoreType.DMA(shape)


def body(trunk, normgain, expand, shrink, inscale, hidscale, actscale, outscale, cotangent):
    S = jax.ShapeDtypeStruct
    pad = ((0, ROWS - TOK), (0, 0))

    def sliced(v):
        return v.reshape(2, 4, 256).swapaxes(0, 1).reshape(4, 1, SL)

    def twice(v):
        return jnp.broadcast_to(v.reshape(1, 2, SL), (4, 2, SL))

    vec = jnp.concatenate(
        [twice(inscale), twice(outscale), sliced(hidscale), sliced(actscale), jnp.zeros((4, 2, SL), f32)], axis=1
    )
    ps, pe, t, sv, gp = pl.pallas_call(
        compute_kernel,
        out_shape=[
            S((2, 2, 128, D), bf16),
            S((2, 2, 4, 64, SL), bf16),
            S((2, CUT, D), bf16),
            S((4, 8, SL), f32),
            S((1, D), f32),
        ],
        in_specs=vmem(6),
        out_specs=vmem(5),
        scratch_shapes=[
            pltpu.VMEM((ROWS, D), f32),
            pltpu.VMEM((ROWS, D), f32),
            pltpu.VMEM((ROWS, 128), f32),
            pltpu.VMEM((4, ROWS, D), bf16),
            pltpu.VMEM((2, 4, 2, 64, SL), bf16),
            pltpu.VMEM((2, 2, 128, D), bf16),
            pltpu.VMEM((4, 8, SL), f32),
            pltpu.VMEM((4, ROWS, D), bf16),
            pltpu.VMEM((4, ROWS, SL), bf16),
            pltpu.VMEM((4, ROWS, SL), f32),
            pltpu.VMEM((4, ROWS, SL), f32),
            pltpu.VMEM((4, ROWS, SL), f32),
            pltpu.VMEM((ROWS, D), f32),
            pltpu.VMEM((SL, D), f32),
            pltpu.VMEM((D, SL), f32),
            dma(6), dma(4, 2), dma(3, 2), dma(3, 2), dma(3), dma(3), dma(3), dma(3), dma(3), dma(3),
        ],
        compiler_params=pltpu.CompilerParams(
            collective_id=0, has_side_effects=True, vmem_limit_bytes=60 * 1024 * 1024
        ),
        name="gather_compute",
    )(
        jnp.pad(trunk, pad), normgain.reshape(1, D), vec, expand, shrink, jnp.pad(cotangent[0], pad)
    )
    tg, eg, sg, ing, hg, ag, og, gg = pl.pallas_call(
        reduce_kernel,
        out_shape=[
            S((TOK, 64), bf16),
            S((64, FF), f32),
            S((128, D), f32),
            S((1, D), f32),
            S((1, FF), f32),
            S((1, FF), f32),
            S((1, D), f32),
            S((1, D), f32),
        ],
        in_specs=vmem(5),
        out_specs=vmem(8),
        scratch_shapes=[
            pltpu.VMEM((2, 128, D), bf16),
            pltpu.VMEM((2, 4, 64, SL), bf16),
            pltpu.VMEM((CUT, D), bf16),
            pltpu.VMEM((2, 128, D), bf16),
            pltpu.VMEM((2, 4, 64, SL), bf16),
            pltpu.VMEM((8, CUT, 128), bf16),
            pltpu.VMEM((8, CUT, 128), bf16),
            pltpu.VMEM((128, D), bf16),
            pltpu.VMEM((4, 64, SL), bf16),
            pltpu.VMEM((16, 16, D), bf16),
            pltpu.VMEM((16, 16, D), bf16),
            pltpu.VMEM((2, 16, SL), bf16),
            pltpu.VMEM((16, 16, SL), bf16),
            pltpu.VMEM((4, 4, 16, SL), bf16),
            pltpu.VMEM((4, 8, SL), f32),
            pltpu.VMEM((16, 1, D), f32),
            pltpu.VMEM((16, 1, SL), f32),
            pltpu.VMEM((16, 1, SL), f32),
            pltpu.VMEM((16, 1, SL), f32),
            pltpu.VMEM((1, SL), f32),
            pltpu.VMEM((2, CUT, 128), bf16),
            dma(3), dma(3), dma(3), dma(3), dma(16), dma(16), dma(2), dma(2), dma(8), dma(8),
            dma(16), dma(16), dma(16), dma(16), pltpu.SemaphoreType.DMA, pltpu.SemaphoreType.DMA,
            dma(16), dma(16), dma(16), dma(4, 4), dma(16), dma(16),
        ],
        compiler_params=pltpu.CompilerParams(
            collective_id=1, has_side_effects=True, vmem_limit_bytes=40 * 1024 * 1024
        ),
        name="reduce",
    )(ps, pe, t, sv, gp)
    return tg, eg, sg, ing, hg, ag, og, gg.reshape(D)


def solution(mesh):
    finer = Mesh(mesh.devices.reshape(2, 4, 2, 8, 2), AXES)
    rows = P(MEMBER, None)
    in_specs = (P(DP, None), P(), rows, rows, rows, rows, rows, rows, P(MEMBER, DP, None))
    out_specs = (P(DP, MEMBER), rows, rows, rows, rows, rows, rows, P())
    return jax.shard_map(body, mesh=finer, in_specs=in_specs, out_specs=out_specs, check_vma=False)
```

```python
import jax
import jax.numpy as jnp
from jax import lax
from jax.experimental import pallas as pl
from jax.experimental.pallas import tpu as pltpu
from jax.sharding import Mesh
from jax.sharding import PartitionSpec as P

AXES = ("y", "x", "c", "z", "h")
MEMBER = ("y", "x", "c")
DP = ("z", "h")
TOK = 394
CUT = 208
FULL = 416
D = 1024
FF = 2048
SL = 512

eps = 1e-06
coeff = 0.7978845608028654
f32 = jnp.float32
bf16 = jnp.bfloat16
MESH = pl.DeviceIdType.MESH


def remote(src, dst, send, recv, **where):
    return pltpu.make_async_remote_copy(
        src_ref=src, dst_ref=dst, send_sem=send, recv_sem=recv, device_id=where, device_id_type=MESH
    )


def greet(barrier, **where):
    pl.semaphore_signal(barrier, inc=1, device_id=where, device_id_type=MESH)


def gelu_pair(hidden):
    inner = coeff * (hidden + 0.044715 * hidden * hidden * hidden)
    tangent = jnp.tanh(inner)
    active = 0.5 * hidden * (1.0 + tangent)
    slope = 0.5 * (1.0 + tangent) + 0.5 * hidden * (1.0 - tangent * tangent) * coeff * (
        1.0 + 3.0 * 0.044715 * hidden * hidden
    )
    return active, slope


def dot(a, b, ca, cb):
    return lax.dot_general(a, b, (((ca,), (cb,)), ((), ())), preferred_element_type=f32)


def row(v, i):
    return jnp.concatenate([v[i : i + 1], v[i + 1 : i + 2]], axis=1)


def added(*refs):
    total = refs[0].astype(f32)
    for r in refs[1:]:
        total = total + r.astype(f32)
    return total


def kernel(
    trunk, exp, shr, cot, gain, inscale, hidscale, actscale, outscale,
    tf, sh, ex, dvo,
    tbuf, vec, normed, gained, invs, cots, w1, w2, vecs, si, act, pa, actf, proj, total, sacc, eacc,
    pbuf, rbuf, t, rt, q, yb, mix, r, rz, res, tq, tr, sv, svr, gp, gpr, dv, dvr, dvs,
    ls, cs, cr, ws, wr, vs, vr, ss, sr, es, er,
    as_, ar, ys, yr, zs, zr, hs, hr, xs_, xr, ts, tr_, fs, fr, bs, br, gs, gr, ds, dr, os_, or_,
):
    y, x, c, z, h = (lax.axis_index(a) for a in AXES)
    xs = [lax.rem(x + o, 4) for o in range(4)]
    oy, oc = 1 - y, 1 - c
    me = z * 2 + h
    chip = y * 4 + x
    place = h * 2 + y
    sent = []

    def go(copy):
        copy.start()
        sent.append(copy)
        return copy

    barrier = pltpu.get_barrier_semaphore()

    @pl.loop(1, 64)
    def _(o):
        e = lax.rem(me + lax.rem(o, 16), 16)
        greet(barrier, x=lax.rem(x + o // 16, 4), z=e // 2, h=lax.rem(e, 2))

    for yo, co in ((0, 1), (1, 0), (1, 1)):
        for xo in range(4):
            greet(barrier, y=oy if yo else y, x=xs[xo], c=oc if co else c)
    greet(barrier, y=oy, h=1 - h)

    here = [
        pltpu.make_async_copy(trunk, tbuf, ls.at[0]),
        pltpu.make_async_copy(shr, w2.at[y, c], ls.at[1]),
        pltpu.make_async_copy(cot.at[0], cots.at[0], ls.at[2]),
    ]
    for half in (0, 1):
        here.append(
            pltpu.make_async_copy(
                exp.at[:, pl.ds(pl.multiple_of(1024 * half + 256 * x, 256), 256)],
                w1.at[y, x, c, :, pl.ds(256 * half, 256)],
                ls.at[3 + half],
            )
        )
    for copy in here:
        copy.start()
    for xx in range(4):
        for i in (0, 1):
            vec[xx, i : i + 1] = inscale[:, SL * i : SL * i + SL]
            vec[xx, 2 + i : 3 + i] = outscale[:, SL * i : SL * i + SL]
            at = 1024 * i + 256 * xx
            vec[xx, 4:5, 256 * i : 256 * i + 256] = hidscale[:, at : at + 256]
            vec[xx, 5:6, 256 * i : 256 * i + 256] = actscale[:, at : at + 256]
        vec[xx, 6:8] = jnp.zeros((2, SL), f32)
    pl.semaphore_wait(barrier, 76)

    slot_of = {1: 1, 3: 2, 2: 3}
    vec_copies, exp_copies = {}, {}
    for o in (1, 3, 2):
        for half in (0, 1):
            exp_copies[o, half] = go(remote(
                exp.at[:, pl.ds(pl.multiple_of(1024 * half + 256 * xs[o], 256), 256)],
                w1.at[y, x, c, :, pl.ds(256 * half, 256)],
                ws.at[o - 1, half], wr.at[o - 1, half], x=xs[o],
            ))
        vec_copies[o] = go(remote(
            vec.at[xs[o]], vecs.at[slot_of[o]], vs.at[o - 1], vr.at[o - 1], x=xs[o]
        ))
    shr_y = go(remote(shr, w2.at[y, c], ss.at[0], sr.at[0], y=oy))
    shr_c = go(remote(shr, w2.at[y, c], ss.at[1], sr.at[1], c=oc))
    a, b = pl.ds(0, CUT), pl.ds(CUT, TOK - CUT)
    right_a = go(remote(cot.at[0, a], cots.at[1, a], cs.at[0], cr.at[1, 0], x=xs[1]))
    left_b = go(remote(cot.at[0, b], cots.at[2, b], cs.at[2], cr.at[2, 1], x=xs[3]))
    right_b = go(remote(cot.at[0, b], cots.at[1, b], cs.at[1], cr.at[1, 1], x=xs[1]))
    left_a = go(remote(cot.at[0, a], cots.at[2, a], cs.at[3], cr.at[2, 0], x=xs[3]))

    vecs[0] = vec[x]
    here[0].wait()
    tokens = tbuf[...].astype(f32)
    centered = tokens - jnp.mean(tokens, axis=1, keepdims=True)
    variance = jnp.mean(centered * centered, axis=1, keepdims=True)
    inv = lax.rsqrt(variance + eps)
    normed[...] = centered * inv
    gained[...] = centered * inv * gain[...]
    invs[...] = jnp.broadcast_to(inv, invs.shape)
    total[...] = jnp.zeros_like(total)
    sacc[...] = jnp.zeros_like(sacc)
    eacc[...] = jnp.zeros_like(eacc)
    for copy in here[1:]:
        copy.wait()

    for o in (1, 3, 2):
        exp_copies[o, 0].wait_recv()
        exp_copies[o, 1].wait_recv()
    exp_y = go(remote(w1.at[y, :, c], w1.at[y, :, c], es.at[0], er.at[0], y=oy))
    exp_c = go(remote(w1.at[y, :, c], w1.at[y, :, c], es.at[1], er.at[1], c=oc))
    shr_y.wait_recv()
    shr_f = go(remote(w2.at[oy, c], w2.at[oy, c], ss.at[2], sr.at[2], c=oc))
    for o in (1, 3, 2):
        vec_copies[o].wait_recv()

    @pl.loop(0, 4)
    def _(k):
        si[k] = (gained[...] * row(vecs[k], 0)).astype(bf16)

    right_a.wait_recv()
    fwd_a = go(remote(cots.at[1, a], cots.at[3, a], cs.at[4], cr.at[3, 0], x=xs[1]))
    left_b.wait_recv()
    fwd_b = go(remote(cots.at[2, b], cots.at[3, b], cs.at[5], cr.at[3, 1], x=xs[3]))
    exp_y.wait_recv()
    exp_f = go(remote(w1.at[oy, :, c], w1.at[oy, :, c], es.at[2], er.at[2], c=oc))
    for copy in (shr_c, exp_c, shr_f, exp_f):
        copy.wait_recv()

    @pl.loop(0, 4)
    def _(k):
        v = vecs[k]
        project = dot(si[k], w1[...].reshape(D, SL), 1, 0)
        active, slope = gelu_pair(project * v[4:5])
        proj[k] = project
        actf[k] = active
        act[k] = (active * v[5:6]).astype(bf16)
        pa[k] = slope * v[5:6]

    def back_part(k):
        v = vecs[k]
        scale_out = row(v, 2)
        second = w2[...].reshape(SL, D)
        seed = cots[k]
        scaled_cot = (seed.astype(f32) * scale_out).astype(bf16)
        back = dot(scaled_cot, second, 1, 1)
        grad_act = jnp.sum(back * actf[k], axis=0, keepdims=True)
        back_hidden = back * pa[k]
        grad_hid = jnp.sum(back_hidden * proj[k], axis=0, keepdims=True)
        back_proj = (back_hidden * v[4:5]).astype(bf16)
        both = dot(act[k], seed, 0, 0)
        sacc[...] += both * scale_out
        grad_out = jnp.sum(second.astype(f32) * both, axis=0, keepdims=True)
        zero = jnp.zeros((2, SL), f32)
        sv[k, 2:8] = jnp.concatenate([grad_out[:, :SL], grad_out[:, SL:], grad_hid, grad_act, zero], axis=0)
        return back_proj

    def expand_part(k, back_proj):
        eacc[...] += dot(si[k], back_proj, 0, 0)

    def norm_part(k, back_proj):
        back_norm = dot(back_proj, w1[...].reshape(D, SL), 1, 1)
        grad_in = jnp.sum(back_norm * gained[...], axis=0, keepdims=True)
        total[...] += back_norm * row(vecs[k], 0)
        sv[k, 0:2] = jnp.concatenate([grad_in[:, :SL], grad_in[:, SL:]], axis=0)

    @pl.loop(0, 3)
    def _(k):
        @pl.when(k == 1)
        def _():
            right_b.wait_recv()

        @pl.when(k == 2)
        def _():
            left_a.wait_recv()

        back_proj = back_part(k)
        expand_part(k, back_proj)
        norm_part(k, back_proj)

    right, left, far = (lax.rem(place + o, 4) for o in (1, 3, 2))
    to_right = dict(y=lax.rem(right, 2), h=right // 2)
    to_left = dict(y=lax.rem(left, 2), h=left // 2)
    top, low = pl.ds(0, 4), pl.ds(4, 4)

    def core_step(i):
        return go(remote(pbuf.at[i, oc], rbuf.at[i], as_.at[i], ar.at[i], c=oc))

    def ring_start(i, copy):
        copy.wait_recv()
        q[i] = added(pbuf[i, c], rbuf[i]).astype(bf16)
        return [
            go(remote(q.at[i, far, top], yb.at[i, 0], ys.at[i, 0], yr.at[i, 0], **to_right)),
            go(remote(q.at[i, far, low], yb.at[i, 1], ys.at[i, 1], yr.at[i, 1], **to_left)),
            go(remote(q.at[i, right, low], yb.at[i, 2], ys.at[i, 2], yr.at[i, 2], **to_right)),
            go(remote(q.at[i, left, top], yb.at[i, 3], ys.at[i, 3], yr.at[i, 3], **to_left)),
        ]

    def ring_pass(i, copies):
        copies[0].wait_recv()
        mix[i, 0] = added(q[i, right, 0:4], yb[i, 0]).astype(bf16)
        copies.append(go(remote(mix.at[i, 0], yb.at[i, 4], ys.at[i, 4], yr.at[i, 4], **to_right)))
        copies[1].wait_recv()
        mix[i, 1] = added(q[i, left, 4:8], yb[i, 1]).astype(bf16)
        copies.append(go(remote(mix.at[i, 1], yb.at[i, 5], ys.at[i, 5], yr.at[i, 5], **to_left)))

    def deep_start(i, copies):
        for copy in copies[2:]:
            copy.wait_recv()
        r[i, 0:4] = added(q[i, place, 0:4], yb[i, 3], yb[i, 4]).astype(bf16)
        r[i, 4:8] = added(q[i, place, 4:8], yb[i, 2], yb[i, 5]).astype(bf16)
        out = []
        for o in (4, 3, 5, 2, 6, 1, 7):
            e = lax.rem(z + o, 8)
            out.append(go(remote(r.at[i, e], rz.at[i, z], zs.at[i, o], zr.at[i, o], z=e)))
        rz[i, z] = r[i, z]
        return out

    def deep_sum(i, copies):
        for copy in copies:
            copy.wait_recv()
        done = added(*(rz[i, e] for e in range(8))).astype(bf16)
        res[i] = done
        return done

    peers = []
    for o in range(1, 16):
        e = lax.rem(me + o, 16)
        peers.append((o, dict(z=e // 2, h=lax.rem(e, 2))))

    fwd_a.wait_recv()
    fwd_b.wait_recv()
    back_proj = back_part(3)
    for cc in (0, 1):
        for hh in (0, 1):
            for yy in (0, 1):
                at = (yy * 2 + cc) * 128
                block = sacc[at : at + 128, SL * hh : SL * hh + SL]
                pbuf[0, cc, 2 * hh + yy] = block.astype(bf16).reshape(8, 16, SL)
    core_s = core_step(0)
    expand_part(3, back_proj)
    for cc in (0, 1):
        for hh in (0, 1):
            for yy in (0, 1):
                for zz in range(8):
                    at = ((yy * 4 + zz // 2) * 2 + cc) * 64 + zz % 2 * 32 + hh * 16
                    pbuf[1, cc, 2 * hh + yy, zz] = eacc[at : at + 16].astype(bf16)
    core_e = core_step(1)
    ring_s = ring_start(0, core_s)
    norm_part(3, back_proj)
    ring_e = ring_start(1, core_e)

    vector_copies = []
    for slot, xo in ((1, 3), (2, 1), (3, 2)):
        vector_copies.append(go(remote(sv.at[slot], svr.at[x], bs.at[xo - 1], br.at[xo - 1], x=xs[xo])))
    svr[x] = sv[0]
    whole = total[...]
    gp[...] = jnp.sum(whole * normed[...], axis=0, keepdims=True)
    gains = []
    for o in range(1, 16):
        yo, xo, co = o // 8, (o // 2) % 4, o % 2
        gains.append(go(remote(
            gp, gpr.at[chip * 2 + c], gs.at[o], gr.at[o], y=oy if yo else y, x=xs[xo], c=oc if co else c
        )))
    gpr[chip * 2 + c] = gp[...]
    unit = whole * gain[...]
    inner = jnp.mean(unit * normed[...], axis=1, keepdims=True)
    back_trunk = invs[:, :1] * (unit - jnp.mean(unit, axis=1, keepdims=True) - normed[...] * inner)
    term = (cots[0].astype(f32) + back_trunk).astype(bf16)
    t[0] = term[:CUT]
    t[1, : TOK - CUT] = term[CUT:]
    t[1, TOK - CUT :] = jnp.zeros((FULL - TOK, D), bf16)
    core_t = go(remote(t.at[oc], rt, as_.at[2], ar.at[2], c=oc))

    ring_pass(0, ring_s)
    ring_pass(1, ring_e)

    core_t.wait_recv()
    joint = added(t[c], rt[...]).astype(bf16)
    for g in range(8):
        tq[g] = joint[:, 128 * g : 128 * g + 128]
    tiles = []
    for g in range(1, 8):
        yo, xo = g // 4, g % 4
        ty, tx = oy if yo else y, xs[xo]
        tiles.append(go(remote(tq.at[ty * 4 + tx], tr.at[chip], ts.at[g], tr_.at[g], y=ty, x=tx)))
    tr[chip] = tq[chip]

    for copy in vector_copies + gains:
        copy.wait_recv()
    sums = svr[0] + svr[1] + svr[2] + svr[3]
    gain_sum = gpr[0]
    for m in range(1, 16):
        gain_sum = gain_sum + gpr[m]
    zero = jnp.zeros((1, SL), f32)
    for i in range(4):
        dv[i] = sums[i : i + 1]
        dv[4 + i] = svr[i, 4:5]
        dv[8 + i] = svr[i, 5:6]
    dv[12] = gain_sum[:, :SL]
    dv[13] = gain_sum[:, SL:]
    dv[14] = zero
    dv[15] = zero
    small = []
    for o, where in peers:
        e = where["z"] * 2 + where["h"]
        small.append(go(remote(dv.at[e], dvr.at[me], ds.at[o], dr.at[o], **where)))
    dvr[me] = dv[me]

    deep_s = deep_start(0, ring_s)
    deep_e = deep_start(1, ring_e)

    for copy in tiles:
        copy.wait_recv()
    tf[c] = added(*(tr[g] for g in range(8))).astype(bf16)
    finish = go(remote(tf.at[c], tf.at[c], fs, fr, c=oc))

    done = deep_sum(0, deep_s)
    shrinks = []
    for o, where in peers:
        shrinks.append(go(remote(res.at[0], sh.at[me], hs.at[o], hr.at[o], **where)))
    sh[me] = done

    for copy in small:
        copy.wait_recv()
    line = dvr[0]
    for p in range(1, 16):
        line = line + dvr[p]
    dvs[...] = line
    lines = []
    for o, where in peers:
        lines.append(go(remote(dvs, dvo.at[me], os_.at[o], or_.at[o], **where)))
    dvo[me] = line

    done = deep_sum(1, deep_e)
    goal, at = me // 4, lax.rem(me, 4)
    for o, where in peers:
        go(remote(res.at[1], ex.at[x, at], xs_.at[o], xr.at[x, at], x=goal, **where))
    mine = remote(res.at[1], ex.at[x, at], xs_.at[0], xr.at[x, at], x=goal)

    @pl.when(goal != x)
    def _():
        mine.start()

    @pl.when(goal == x)
    def _():
        ex[x, at] = done

    for copy in [finish] + shrinks + lines:
        copy.wait_recv()
    for xx in range(4):
        for p in range(4):

            @pl.when(jnp.logical_or(x != xx, me != 4 * x + p))
            def _():
                remote(res.at[1], ex.at[xx, p], xs_.at[0], xr.at[xx, p], x=goal).wait_recv()

    for copy in sent:
        copy.wait_send()

    @pl.when(goal != x)
    def _():
        mine.wait_send()


def finish_kernel(tf, sh, ex, dvo, tg, eg, sg, ing, hg, ag, og, gg):
    c = lax.axis_index("c")
    first, rest = tf[0].astype(f32), tf[1, : TOK - CUT].astype(f32)
    tg[:CUT] = jnp.where(c == 0, first[:, :64], first[:, 64:]).astype(bf16)
    tg[CUT:] = jnp.where(c == 0, rest[:, :64], rest[:, 64:]).astype(bf16)
    for i in (0, 1):
        ing[:, SL * i : SL * i + SL] = dvo[i]
        og[:, SL * i : SL * i + SL] = dvo[2 + i]
        gg[:, SL * i : SL * i + SL] = dvo[12 + i]
        for xx in range(4):
            at = 1024 * i + 256 * xx
            hg[:, at : at + 256] = dvo[4 + xx][:, 256 * i : 256 * i + 256]
            ag[:, at : at + 256] = dvo[8 + xx][:, 256 * i : 256 * i + 256]
            for p in range(4):
                eg[16 * p : 16 * p + 16, at : at + 256] = ex[xx, p, :, 256 * i : 256 * i + 256].astype(f32)
    for p in range(16):
        sg[16 * (p // 2) : 16 * (p // 2) + 16, SL * (p % 2) : SL * (p % 2) + SL] = sh[p].astype(f32)


def vmem(n):
    return [pl.BlockSpec(memory_space=pltpu.VMEM)] * n


def dma(*shape):
    return pltpu.SemaphoreType.DMA(shape)


def body(trunk, normgain, expand, shrink, inscale, hidscale, actscale, outscale, cotangent):
    S = jax.ShapeDtypeStruct
    V = pltpu.VMEM
    parts = pl.pallas_call(
        kernel,
        out_shape=[
            S((2, CUT, 128), bf16),
            S((16, 16, SL), bf16),
            S((4, 4, 16, SL), bf16),
            S((16, 1, SL), f32),
        ],
        in_specs=[pl.BlockSpec(memory_space=pl.ANY)] * 4 + vmem(5),
        out_specs=vmem(4),
        scratch_shapes=[
            V((TOK, D), bf16),
            V((4, 8, SL), f32),
            V((TOK, D), f32),
            V((TOK, D), f32),
            V((TOK, 128), f32),
            V((4, TOK, D), bf16),
            V((2, 4, 2, 64, SL), bf16),
            V((2, 2, 128, D), bf16),
            V((4, 8, SL), f32),
            V((4, TOK, D), bf16),
            V((4, TOK, SL), bf16),
            V((4, TOK, SL), f32),
            V((4, TOK, SL), f32),
            V((4, TOK, SL), f32),
            V((TOK, D), f32),
            V((SL, D), f32),
            V((D, SL), f32),
            V((2, 2, 4, 8, 16, SL), bf16),
            V((2, 4, 8, 16, SL), bf16),
            V((2, CUT, D), bf16),
            V((CUT, D), bf16),
            V((2, 4, 8, 16, SL), bf16),
            V((2, 6, 4, 16, SL), bf16),
            V((2, 2, 4, 16, SL), bf16),
            V((2, 8, 16, SL), bf16),
            V((2, 8, 16, SL), bf16),
            V((2, 16, SL), bf16),
            V((8, CUT, 128), bf16),
            V((8, CUT, 128), bf16),
            V((4, 8, SL), f32),
            V((4, 8, SL), f32),
            V((1, D), f32),
            V((16, 1, D), f32),
            V((16, 1, SL), f32),
            V((16, 1, SL), f32),
            V((1, SL), f32),
            dma(5), dma(6), dma(4, 2), dma(3, 2), dma(3, 2), dma(3), dma(3), dma(3), dma(3), dma(3), dma(3),
            dma(3), dma(3), dma(2, 6), dma(2, 6), dma(2, 8), dma(2, 8), dma(16), dma(16), dma(16), dma(4, 4),
            dma(8), dma(8), pltpu.SemaphoreType.DMA, pltpu.SemaphoreType.DMA, dma(3), dma(3), dma(16), dma(16),
            dma(16), dma(16), dma(16), dma(16),
        ],
        compiler_params=pltpu.CompilerParams(
            collective_id=0, has_side_effects=True, vmem_limit_bytes=60 * 1024 * 1024
        ),
        name="exchange_compute",
    )(
        trunk, expand, shrink, cotangent, normgain.reshape(1, D), inscale, hidscale, actscale, outscale
    )
    tg, eg, sg, ing, hg, ag, og, gg = pl.pallas_call(
        finish_kernel,
        out_shape=[
            S((TOK, 64), bf16),
            S((64, FF), f32),
            S((128, D), f32),
            S((1, D), f32),
            S((1, FF), f32),
            S((1, FF), f32),
            S((1, D), f32),
            S((1, D), f32),
        ],
        in_specs=vmem(4),
        out_specs=vmem(8),
        name="write_outputs",
    )(*parts)
    return tg, eg, sg, ing, hg, ag, og, gg.reshape(D)


def solution(mesh):
    finer = Mesh(mesh.devices.reshape(2, 4, 2, 8, 2), AXES)
    rows = P(MEMBER, None)
    in_specs = (P(DP, None), P(), rows, rows, rows, rows, rows, rows, P(MEMBER, DP, None))
    out_specs = (P(DP, MEMBER), rows, rows, rows, rows, rows, rows, P())
    return jax.shard_map(body, mesh=finer, in_specs=in_specs, out_specs=out_specs, check_vma=False)
```

```python
import jax
import jax.numpy as jnp
from jax import lax
from jax.experimental import pallas as pl
from jax.experimental.pallas import tpu as pltpu
from jax.sharding import Mesh
from jax.sharding import PartitionSpec as P

AXES = ("y", "x", "c", "z", "h")
MEMBER = ("y", "x", "c")
DP = ("z", "h")
TOK = 394
CUT = 208
EDGE = 112
EDGE2 = 304
PIECES = ((EDGE, CUT), (CUT, EDGE2), (0, EDGE), (EDGE2, TOK))
FULL = 416
D = 1024
FF = 2048
SL = 512

eps = 1e-06
coeff = 0.7978845608028654
f32 = jnp.float32
bf16 = jnp.bfloat16
MESH = pl.DeviceIdType.MESH


def remote(src, dst, send, recv, **where):
    return pltpu.make_async_remote_copy(
        src_ref=src, dst_ref=dst, send_sem=send, recv_sem=recv, device_id=where, device_id_type=MESH
    )


def greet(barrier, **where):
    pl.semaphore_signal(barrier, inc=1, device_id=where, device_id_type=MESH)


def gelu_pair(hidden):
    inner = coeff * (hidden + 0.044715 * hidden * hidden * hidden)
    tangent = jnp.tanh(inner)
    active = 0.5 * hidden * (1.0 + tangent)
    slope = 0.5 * (1.0 + tangent) + 0.5 * hidden * (1.0 - tangent * tangent) * coeff * (
        1.0 + 3.0 * 0.044715 * hidden * hidden
    )
    return active, slope


def dot(a, b, ca, cb):
    return lax.dot_general(a, b, (((ca,), (cb,)), ((), ())), preferred_element_type=f32)


def row(v, i):
    return jnp.concatenate([v[i : i + 1], v[i + 1 : i + 2]], axis=1)


def added(*refs):
    total = refs[0].astype(f32)
    for r in refs[1:]:
        total = total + r.astype(f32)
    return total


def kernel(
    trunk, exp, shr, cot, gain, inscale, hidscale, actscale, outscale,
    tf, sh, ex, dvo,
    tbuf, vec, normed, gained, invs, cots, w1, w2, vecs, si, act, pa, actf, proj, total, sacc, eacc,
    pbuf, rbuf, t, rt, q, yb, mix, r, rz, res, tq, tr, sv, svr, gp, gpr, dv, dvr, dvs,
    ls, cs, cr, ws, wr, vs, vr, ss, sr, es, er,
    as_, ar, ys, yr, zs, zr, hs, hr, xs_, xr, ts, tr_, fs, fr, bs, br, gs, gr, ds, dr, os_, or_, heard,
):
    y, x, c, z, h = (lax.axis_index(a) for a in AXES)
    xs = [lax.rem(x + o, 4) for o in range(4)]
    oy, oc = 1 - y, 1 - c
    me = z * 2 + h
    chip = y * 4 + x
    place = h * 2 + y
    sent = []

    def go(copy):
        copy.start()
        sent.append(copy)
        return copy

    barrier = pltpu.get_barrier_semaphore()

    for yo in (0, 1):
        for co in (0, 1):
            for xo in range(4):
                if yo or co or xo:
                    greet(barrier, y=oy if yo else y, x=xs[xo], c=oc if co else c)
    greet(barrier, y=oy, h=1 - h)
    greet(barrier, h=1 - h)
    above, below = lax.rem(z + 1, 8), lax.rem(z + 7, 8)
    greet(barrier, z=above)
    greet(barrier, z=below)

    def tell_z(i):
        greet(heard.at[i], z=above)
        greet(heard.at[i], z=below)

    def told(i, n):
        pl.semaphore_wait(heard.at[i], n)

    here = [
        pltpu.make_async_copy(trunk, tbuf, ls.at[0]),
        pltpu.make_async_copy(shr, w2.at[y, c], ls.at[1]),
        pltpu.make_async_copy(cot.at[0], cots.at[0], ls.at[2]),
    ]
    for half in (0, 1):
        here.append(
            pltpu.make_async_copy(
                exp.at[:, pl.ds(pl.multiple_of(1024 * half + 256 * x, 256), 256)],
                w1.at[y, x, c, :, pl.ds(256 * half, 256)],
                ls.at[3 + half],
            )
        )
    for copy in here:
        copy.start()
    for xx in range(4):
        for i in (0, 1):
            vec[xx, i : i + 1] = inscale[:, SL * i : SL * i + SL]
            vec[xx, 2 + i : 3 + i] = outscale[:, SL * i : SL * i + SL]
            at = 1024 * i + 256 * xx
            vec[xx, 4:5, 256 * i : 256 * i + 256] = hidscale[:, at : at + 256]
            vec[xx, 5:6, 256 * i : 256 * i + 256] = actscale[:, at : at + 256]
        vec[xx, 6:8] = jnp.zeros((2, SL), f32)
    pl.semaphore_wait(barrier, 19)
    tell_z(0)

    slot_of = {1: 1, 3: 2, 2: 3}
    vec_copies, exp_copies = {}, {}
    for o in (1, 3, 2):
        for half in (0, 1):
            exp_copies[o, half] = go(remote(
                exp.at[:, pl.ds(pl.multiple_of(1024 * half + 256 * xs[o], 256), 256)],
                w1.at[y, x, c, :, pl.ds(256 * half, 256)],
                ws.at[o - 1, half], wr.at[o - 1, half], x=xs[o],
            ))
        vec_copies[o] = go(remote(
            vec.at[xs[o]], vecs.at[slot_of[o]], vs.at[o - 1], vr.at[o - 1], x=xs[o]
        ))
    shr_y = go(remote(shr, w2.at[y, c], ss.at[0], sr.at[0], y=oy))
    shr_c = go(remote(shr, w2.at[y, c], ss.at[1], sr.at[1], c=oc))
    a, b = pl.ds(0, CUT), pl.ds(CUT, TOK - CUT)
    right_a = go(remote(cot.at[0, a], cots.at[1, a], cs.at[0], cr.at[1, 0], x=xs[1]))
    left_b = go(remote(cot.at[0, b], cots.at[2, b], cs.at[2], cr.at[2, 1], x=xs[3]))
    right_b = go(remote(cot.at[0, b], cots.at[1, b], cs.at[1], cr.at[1, 1], x=xs[1]))
    left_a = go(remote(cot.at[0, a], cots.at[2, a], cs.at[3], cr.at[2, 0], x=xs[3]))

    vecs[0] = vec[x]
    here[0].wait()
    tokens = tbuf[...].astype(f32)
    centered = tokens - jnp.mean(tokens, axis=1, keepdims=True)
    variance = jnp.mean(centered * centered, axis=1, keepdims=True)
    inv = lax.rsqrt(variance + eps)
    normed[...] = centered * inv
    gained[...] = centered * inv * gain[...]
    invs[...] = jnp.broadcast_to(inv, invs.shape)
    total[...] = jnp.zeros_like(total)
    sacc[...] = jnp.zeros_like(sacc)
    eacc[...] = jnp.zeros_like(eacc)
    for copy in here[1:]:
        copy.wait()

    for o in (1, 3, 2):
        exp_copies[o, 0].wait_recv()
        exp_copies[o, 1].wait_recv()
    exp_y = go(remote(w1.at[y, :, c], w1.at[y, :, c], es.at[0], er.at[0], y=oy))
    exp_c = go(remote(w1.at[y, :, c], w1.at[y, :, c], es.at[1], er.at[1], c=oc))
    shr_y.wait_recv()
    shr_f = go(remote(w2.at[oy, c], w2.at[oy, c], ss.at[2], sr.at[2], c=oc))
    for o in (1, 3, 2):
        vec_copies[o].wait_recv()

    @pl.loop(0, 4)
    def _(k):
        si[k] = (gained[...] * row(vecs[k], 0)).astype(bf16)

    right_a.wait_recv()
    left_b.wait_recv()
    fwd = []
    for i, (lo, hi) in enumerate(PIECES):
        src, to = ((1, xs[1]), (2, xs[3]))[i % 2]
        piece = pl.ds(lo, hi - lo)
        fwd.append(go(remote(cots.at[src, piece], cots.at[3, piece], cs.at[4 + i], cr.at[3, i], x=to)))
    exp_y.wait_recv()
    exp_f = go(remote(w1.at[oy, :, c], w1.at[oy, :, c], es.at[2], er.at[2], c=oc))
    for copy in (shr_c, exp_c, shr_f, exp_f):
        copy.wait_recv()
    told(0, 2)
    tell_z(1)

    @pl.loop(0, 4)
    def _(k):
        v = vecs[k]
        project = dot(si[k], w1[...].reshape(D, SL), 1, 0)
        active, slope = gelu_pair(project * v[4:5])
        proj[k] = project
        actf[k] = active
        act[k] = (active * v[5:6]).astype(bf16)
        pa[k] = slope * v[5:6]

    told(1, 2)
    tell_z(2)

    def take(ref, k, rows):
        blocks = [ref[k, lo:hi] for lo, hi in rows]
        return blocks[0] if len(blocks) == 1 else jnp.concatenate(blocks, axis=0)

    def back_part(k, rows, first):
        v = vecs[k]
        scale_out = row(v, 2)
        second = w2[...].reshape(SL, D)
        seed = take(cots, k, rows)
        scaled_cot = (seed.astype(f32) * scale_out).astype(bf16)
        back = dot(scaled_cot, second, 1, 1)
        grad_act = jnp.sum(back * take(actf, k, rows), axis=0, keepdims=True)
        back_hidden = back * take(pa, k, rows)
        grad_hid = jnp.sum(back_hidden * take(proj, k, rows), axis=0, keepdims=True)
        back_proj = (back_hidden * v[4:5]).astype(bf16)
        both = dot(take(act, k, rows), seed, 0, 0)
        sacc[...] += both * scale_out
        grad_out = jnp.sum(second.astype(f32) * both, axis=0, keepdims=True)
        zero = jnp.zeros((2, SL), f32)
        lines = jnp.concatenate([grad_out[:, :SL], grad_out[:, SL:], grad_hid, grad_act, zero], axis=0)
        sv[k, 2:8] = lines if first else sv[k, 2:8] + lines
        return back_proj

    def expand_part(k, rows, back_proj):
        eacc[...] += dot(take(si, k, rows), back_proj, 0, 0)

    def norm_part(k, rows, first, back_proj):
        back_norm = dot(back_proj, w1[...].reshape(D, SL), 1, 1)
        share = back_norm * row(vecs[k], 0)
        grad_in = 0.0
        at = 0
        for lo, hi in rows:
            end = at + hi - lo
            grad_in = grad_in + jnp.sum(back_norm[at:end] * gained[lo:hi], axis=0, keepdims=True)
            total[lo:hi] += share[at:end]
            at = end
        lines = jnp.concatenate([grad_in[:, :SL], grad_in[:, SL:]], axis=0)
        sv[k, 0:2] = lines if first else sv[k, 0:2] + lines

    @pl.loop(0, 3)
    def _(k):
        @pl.when(k == 1)
        def _():
            right_b.wait_recv()

        @pl.when(k == 2)
        def _():
            left_a.wait_recv()

        every = ((0, TOK),)
        back_proj = back_part(k, every, True)
        expand_part(k, every, back_proj)
        norm_part(k, every, True, back_proj)

    right, left, far = (lax.rem(place + o, 4) for o in (1, 3, 2))
    to_right = dict(y=lax.rem(right, 2), h=right // 2)
    to_left = dict(y=lax.rem(left, 2), h=left // 2)
    top, low = pl.ds(0, 4), pl.ds(4, 4)

    def core_step(i):
        return go(remote(pbuf.at[i, oc], rbuf.at[i], as_.at[i], ar.at[i], c=oc))

    def ring_start(i, copy):
        copy.wait_recv()
        q[i] = added(pbuf[i, c], rbuf[i]).astype(bf16)
        return [
            go(remote(q.at[i, far, top], yb.at[i, 0], ys.at[i, 0], yr.at[i, 0], **to_right)),
            go(remote(q.at[i, far, low], yb.at[i, 1], ys.at[i, 1], yr.at[i, 1], **to_left)),
            go(remote(q.at[i, right, low], yb.at[i, 2], ys.at[i, 2], yr.at[i, 2], **to_right)),
            go(remote(q.at[i, left, top], yb.at[i, 3], ys.at[i, 3], yr.at[i, 3], **to_left)),
        ]

    def ring_pass(i, copies):
        copies[0].wait_recv()
        mix[i, 0] = added(q[i, right, 0:4], yb[i, 0]).astype(bf16)
        copies.append(go(remote(mix.at[i, 0], yb.at[i, 4], ys.at[i, 4], yr.at[i, 4], **to_right)))
        copies[1].wait_recv()
        mix[i, 1] = added(q[i, left, 4:8], yb[i, 1]).astype(bf16)
        copies.append(go(remote(mix.at[i, 1], yb.at[i, 5], ys.at[i, 5], yr.at[i, 5], **to_left)))

    def deep_start(i, copies):
        for copy in copies[2:]:
            copy.wait_recv()
        r[i, 0:4] = added(q[i, place, 0:4], yb[i, 3], yb[i, 4]).astype(bf16)
        r[i, 4:8] = added(q[i, place, 4:8], yb[i, 2], yb[i, 5]).astype(bf16)
        out = []
        for o in (4, 3, 5, 2, 6, 1, 7):
            e = lax.rem(z + o, 8)
            out.append(go(remote(r.at[i, e], rz.at[i, z], zs.at[i, o], zr.at[i, o], z=e)))
        rz[i, z] = r[i, z]
        return out

    def deep_sum(i, copies):
        for copy in copies:
            copy.wait_recv()
        done = added(*(rz[i, e] for e in range(8))).astype(bf16)
        res[i] = done
        return done

    peers = []
    for o in range(1, 16):
        e = lax.rem(me + o, 16)
        peers.append((o, dict(z=e // 2, h=lax.rem(e, 2))))

    told(2, 2)
    greet(heard.at[3], h=1 - h)
    fwd[0].wait_recv()
    fwd[1].wait_recv()
    mid, ends = ((EDGE, EDGE2),), ((0, EDGE), (EDGE2, TOK))
    back_proj = back_part(3, mid, True)
    expand_part(3, mid, back_proj)
    norm_part(3, mid, True, back_proj)
    told(3, 1)
    for o in (1, 2, 3):
        greet(heard.at[4], x=xs[o])
    fwd[2].wait_recv()
    fwd[3].wait_recv()
    back_proj = back_part(3, ends, False)
    for cc in (0, 1):
        for hh in (0, 1):
            for yy in (0, 1):
                at = (yy * 2 + cc) * 128
                block = sacc[at : at + 128, SL * hh : SL * hh + SL]
                pbuf[0, cc, 2 * hh + yy] = block.astype(bf16).reshape(8, 16, SL)
    core_s = core_step(0)
    expand_part(3, ends, back_proj)
    for cc in (0, 1):
        for hh in (0, 1):
            for yy in (0, 1):
                for zz in range(8):
                    at = ((yy * 4 + zz // 2) * 2 + cc) * 64 + zz % 2 * 32 + hh * 16
                    pbuf[1, cc, 2 * hh + yy, zz] = eacc[at : at + 16].astype(bf16)
    core_e = core_step(1)
    ring_s = ring_start(0, core_s)
    norm_part(3, ends, False, back_proj)
    ring_e = ring_start(1, core_e)

    vector_copies = []
    for slot, xo in ((1, 3), (2, 1), (3, 2)):
        vector_copies.append(go(remote(sv.at[slot], svr.at[x], bs.at[xo - 1], br.at[xo - 1], x=xs[xo])))
    svr[x] = sv[0]
    whole = total[...]
    gp[...] = jnp.sum(whole * normed[...], axis=0, keepdims=True)
    gains = []
    for o in range(1, 16):
        yo, xo, co = o // 8, (o // 2) % 4, o % 2
        gains.append(go(remote(
            gp, gpr.at[chip * 2 + c], gs.at[o], gr.at[o], y=oy if yo else y, x=xs[xo], c=oc if co else c
        )))
    gpr[chip * 2 + c] = gp[...]
    unit = whole * gain[...]
    inner = jnp.mean(unit * normed[...], axis=1, keepdims=True)
    back_trunk = invs[:, :1] * (unit - jnp.mean(unit, axis=1, keepdims=True) - normed[...] * inner)
    term = (cots[0].astype(f32) + back_trunk).astype(bf16)
    t[0] = term[:CUT]
    t[1, : TOK - CUT] = term[CUT:]
    t[1, TOK - CUT :] = jnp.zeros((FULL - TOK, D), bf16)
    core_t = go(remote(t.at[oc], rt, as_.at[2], ar.at[2], c=oc))

    ring_pass(0, ring_s)
    ring_pass(1, ring_e)

    core_t.wait_recv()
    joint = added(t[c], rt[...]).astype(bf16)
    for g in range(8):
        tq[g] = joint[:, 128 * g : 128 * g + 128]
    tiles = []
    for g in range(1, 8):
        yo, xo = g // 4, g % 4
        ty, tx = oy if yo else y, xs[xo]
        tiles.append(go(remote(tq.at[ty * 4 + tx], tr.at[chip], ts.at[g], tr_.at[g], y=ty, x=tx)))
    tr[chip] = tq[chip]

    for copy in vector_copies + gains:
        copy.wait_recv()
    sums = svr[0] + svr[1] + svr[2] + svr[3]
    gain_sum = gpr[0]
    for m in range(1, 16):
        gain_sum = gain_sum + gpr[m]
    zero = jnp.zeros((1, SL), f32)
    for i in range(4):
        dv[i] = sums[i : i + 1]
        dv[4 + i] = svr[i, 4:5]
        dv[8 + i] = svr[i, 5:6]
    dv[12] = gain_sum[:, :SL]
    dv[13] = gain_sum[:, SL:]
    dv[14] = zero
    dv[15] = zero
    small = []
    for o, where in peers:
        e = where["z"] * 2 + where["h"]
        small.append(go(remote(dv.at[e], dvr.at[me], ds.at[o], dr.at[o], **where)))
    dvr[me] = dv[me]

    told(4, 3)
    deep_s = deep_start(0, ring_s)
    deep_e = deep_start(1, ring_e)

    for copy in tiles:
        copy.wait_recv()
    tf[c] = added(*(tr[g] for g in range(8))).astype(bf16)
    finish = go(remote(tf.at[c], tf.at[c], fs, fr, c=oc))

    done = deep_sum(0, deep_s)
    shrinks = []
    for o, where in peers:
        shrinks.append(go(remote(res.at[0], sh.at[me], hs.at[o], hr.at[o], **where)))
    sh[me] = done

    for copy in small:
        copy.wait_recv()
    line = dvr[0]
    for p in range(1, 16):
        line = line + dvr[p]
    dvs[...] = line
    lines = []
    for o, where in peers:
        lines.append(go(remote(dvs, dvo.at[me], os_.at[o], or_.at[o], **where)))
    dvo[me] = line

    done = deep_sum(1, deep_e)
    goal, at = me // 4, lax.rem(me, 4)
    for o, where in peers:
        go(remote(res.at[1], ex.at[x, at], xs_.at[o], xr.at[x, at], x=goal, **where))
    mine = remote(res.at[1], ex.at[x, at], xs_.at[0], xr.at[x, at], x=goal)

    @pl.when(goal != x)
    def _():
        mine.start()

    @pl.when(goal == x)
    def _():
        ex[x, at] = done

    for copy in [finish] + shrinks + lines:
        copy.wait_recv()
    for xx in range(4):
        for p in range(4):

            @pl.when(jnp.logical_or(x != xx, me != 4 * x + p))
            def _():
                remote(res.at[1], ex.at[xx, p], xs_.at[0], xr.at[xx, p], x=goal).wait_recv()

    for copy in sent:
        copy.wait_send()

    @pl.when(goal != x)
    def _():
        mine.wait_send()


def finish_kernel(tf, sh, ex, dvo, tg, eg, sg, ing, hg, ag, og, gg):
    c = lax.axis_index("c")
    turned = tf[...].reshape(FULL, 128).astype(f32).T
    tg[...] = jnp.where(c == 0, turned[:64], turned[64:])[:, :TOK].astype(bf16)
    for i in (0, 1):
        ing[:, SL * i : SL * i + SL] = dvo[i]
        og[:, SL * i : SL * i + SL] = dvo[2 + i]
        gg[:, SL * i : SL * i + SL] = dvo[12 + i]
        for xx in range(4):
            at = 1024 * i + 256 * xx
            hg[:, at : at + 256] = dvo[4 + xx][:, 256 * i : 256 * i + 256]
            ag[:, at : at + 256] = dvo[8 + xx][:, 256 * i : 256 * i + 256]
            for p in range(4):
                eg[16 * p : 16 * p + 16, at : at + 256] = ex[xx, p, :, 256 * i : 256 * i + 256].astype(f32)
    for p in range(16):
        sg[16 * (p // 2) : 16 * (p // 2) + 16, SL * (p % 2) : SL * (p % 2) + SL] = sh[p].astype(f32)


def vmem(n):
    return [pl.BlockSpec(memory_space=pltpu.VMEM)] * n


def dma(*shape):
    return pltpu.SemaphoreType.DMA(shape)


def body(trunk, normgain, expand, shrink, inscale, hidscale, actscale, outscale, cotangent):
    S = jax.ShapeDtypeStruct
    V = pltpu.VMEM
    parts = pl.pallas_call(
        kernel,
        out_shape=[
            S((2, CUT, 128), bf16),
            S((16, 16, SL), bf16),
            S((4, 4, 16, SL), bf16),
            S((16, 1, SL), f32),
        ],
        in_specs=[pl.BlockSpec(memory_space=pl.ANY)] * 4 + vmem(5),
        out_specs=vmem(4),
        scratch_shapes=[
            V((TOK, D), bf16),
            V((4, 8, SL), f32),
            V((TOK, D), f32),
            V((TOK, D), f32),
            V((TOK, 128), f32),
            V((4, TOK, D), bf16),
            V((2, 4, 2, 64, SL), bf16),
            V((2, 2, 128, D), bf16),
            V((4, 8, SL), f32),
            V((4, TOK, D), bf16),
            V((4, TOK, SL), bf16),
            V((4, TOK, SL), f32),
            V((4, TOK, SL), f32),
            V((4, TOK, SL), f32),
            V((TOK, D), f32),
            V((SL, D), f32),
            V((D, SL), f32),
            V((2, 2, 4, 8, 16, SL), bf16),
            V((2, 4, 8, 16, SL), bf16),
            V((2, CUT, D), bf16),
            V((CUT, D), bf16),
            V((2, 4, 8, 16, SL), bf16),
            V((2, 6, 4, 16, SL), bf16),
            V((2, 2, 4, 16, SL), bf16),
            V((2, 8, 16, SL), bf16),
            V((2, 8, 16, SL), bf16),
            V((2, 16, SL), bf16),
            V((8, CUT, 128), bf16),
            V((8, CUT, 128), bf16),
            V((4, 8, SL), f32),
            V((4, 8, SL), f32),
            V((1, D), f32),
            V((16, 1, D), f32),
            V((16, 1, SL), f32),
            V((16, 1, SL), f32),
            V((1, SL), f32),
            dma(5), dma(8), dma(4, 4), dma(3, 2), dma(3, 2), dma(3), dma(3), dma(3), dma(3), dma(3), dma(3),
            dma(3), dma(3), dma(2, 6), dma(2, 6), dma(2, 8), dma(2, 8), dma(16), dma(16), dma(16), dma(4, 4),
            dma(8), dma(8), pltpu.SemaphoreType.DMA, pltpu.SemaphoreType.DMA, dma(3), dma(3), dma(16), dma(16),
            dma(16), dma(16), dma(16), dma(16), pltpu.SemaphoreType.REGULAR((5,)),
        ],
        compiler_params=pltpu.CompilerParams(
            collective_id=0, has_side_effects=True, vmem_limit_bytes=60 * 1024 * 1024
        ),
        name="exchange_compute",
    )(
        trunk, expand, shrink, cotangent, normgain.reshape(1, D), inscale, hidscale, actscale, outscale
    )
    tg, eg, sg, ing, hg, ag, og, gg = pl.pallas_call(
        finish_kernel,
        out_shape=[
            S((64, TOK), bf16),
            S((64, FF), f32),
            S((128, D), f32),
            S((1, D), f32),
            S((1, FF), f32),
            S((1, FF), f32),
            S((1, D), f32),
            S((1, D), f32),
        ],
        in_specs=vmem(4),
        out_specs=vmem(8),
        name="write_outputs",
    )(*parts)
    return tg.T, eg, sg, ing, hg, ag, og, gg.reshape(D)


def solution(mesh):
    finer = Mesh(mesh.devices.reshape(2, 4, 2, 8, 2), AXES)
    rows = P(MEMBER, None)
    in_specs = (P(DP, None), P(), rows, rows, rows, rows, rows, rows, P(MEMBER, DP, None))
    out_specs = (P(DP, MEMBER), rows, rows, rows, rows, rows, rows, P())
    return jax.shard_map(body, mesh=finer, in_specs=in_specs, out_specs=out_specs, check_vma=False)
```

```python
import jax
import jax.numpy as jnp
from jax import lax
from jax.experimental import pallas as pl
from jax.experimental.pallas import tpu as pltpu
from jax.sharding import Mesh
from jax.sharding import PartitionSpec as P

AXES = ("y", "x", "c", "z", "h")
MEMBER = ("y", "x", "c")
DP = ("z", "h")
TOK = 394
CUT = 208
EDGE = 96
SEAM = 176
EDGE2 = 288
PIECES = ((EDGE, SEAM), (SEAM, EDGE2), (0, EDGE), (EDGE2, TOK))
FULL = 416
D = 1024
FF = 2048
SL = 512

eps = 1e-06
coeff = 0.7978845608028654
f32 = jnp.float32
bf16 = jnp.bfloat16
MESH = pl.DeviceIdType.MESH


def remote(src, dst, send, recv, **where):
    return pltpu.make_async_remote_copy(
        src_ref=src, dst_ref=dst, send_sem=send, recv_sem=recv, device_id=where, device_id_type=MESH
    )


def greet(barrier, **where):
    pl.semaphore_signal(barrier, inc=1, device_id=where, device_id_type=MESH)


def gelu_pair(hidden):
    inner = coeff * (hidden + 0.044715 * hidden * hidden * hidden)
    tangent = jnp.tanh(inner)
    active = 0.5 * hidden * (1.0 + tangent)
    slope = 0.5 * (1.0 + tangent) + 0.5 * hidden * (1.0 - tangent * tangent) * coeff * (
        1.0 + 3.0 * 0.044715 * hidden * hidden
    )
    return active, slope


def dot(a, b, ca, cb):
    return lax.dot_general(a, b, (((ca,), (cb,)), ((), ())), preferred_element_type=f32)


def row(v, i):
    return jnp.concatenate([v[i : i + 1], v[i + 1 : i + 2]], axis=1)


def added(*refs):
    total = refs[0].astype(f32)
    for r in refs[1:]:
        total = total + r.astype(f32)
    return total


def kernel(
    trunk, exp, shr, cot, gain, inscale, hidscale, actscale, outscale,
    tf, sh, ex, dvo,
    tbuf, vec, normed, gained, invs, cots, w1, w2, vecs, si, act, pa, actf, proj, total, sacc, eacc,
    pbuf, rbuf, t, rt, q, yb, mix, r, rz, res, tq, tr, sv, svr, gp, gpr, dv, dvr, dvs,
    ls, cs, cr, ws, wr, vs, vr, ss, sr, es, er,
    as_, ar, ys, yr, zs, zr, hs, hr, ts, tr_, fs, fr, bs, br, gs, gr, ds, dr, os_, or_, heard,
):
    y, x, c, z, h = (lax.axis_index(a) for a in AXES)
    xs = [lax.rem(x + o, 4) for o in range(4)]
    oy, oc = 1 - y, 1 - c
    me = z * 2 + h
    chip = y * 4 + x
    place = h * 2 + y
    sent = []

    def go(copy):
        copy.start()
        sent.append(copy)
        return copy

    barrier = pltpu.get_barrier_semaphore()

    for yo in (0, 1):
        for co in (0, 1):
            for xo in range(4):
                if yo or co or xo:
                    greet(barrier, y=oy if yo else y, x=xs[xo], c=oc if co else c)
    greet(barrier, y=oy, h=1 - h)
    greet(barrier, h=1 - h)
    above, below = lax.rem(z + 1, 8), lax.rem(z + 7, 8)
    greet(barrier, z=above)
    greet(barrier, z=below)

    def tell_z(i):
        greet(heard.at[i], z=above)
        greet(heard.at[i], z=below)

    def told(i, n):
        pl.semaphore_wait(heard.at[i], n)

    here = [
        pltpu.make_async_copy(trunk, tbuf, ls.at[0]),
        pltpu.make_async_copy(shr, w2.at[y, c], ls.at[1]),
        pltpu.make_async_copy(cot.at[0], cots.at[0], ls.at[2]),
    ]
    for half in (0, 1):
        here.append(
            pltpu.make_async_copy(
                exp.at[:, pl.ds(pl.multiple_of(1024 * half + 256 * x, 256), 256)],
                w1.at[y, x, c, :, pl.ds(256 * half, 256)],
                ls.at[3 + half],
            )
        )
    for copy in here:
        copy.start()
    for xx in range(4):
        for i in (0, 1):
            vec[xx, i : i + 1] = inscale[:, SL * i : SL * i + SL]
            vec[xx, 2 + i : 3 + i] = outscale[:, SL * i : SL * i + SL]
            at = 1024 * i + 256 * xx
            vec[xx, 4:5, 256 * i : 256 * i + 256] = hidscale[:, at : at + 256]
            vec[xx, 5:6, 256 * i : 256 * i + 256] = actscale[:, at : at + 256]
        vec[xx, 6:8] = jnp.zeros((2, SL), f32)
    pl.semaphore_wait(barrier, 19)
    tell_z(0)

    slot_of = {1: 1, 3: 2, 2: 3}
    vec_copies, exp_copies = {}, {}
    for o in (1, 3, 2):
        for half in (0, 1):
            exp_copies[o, half] = go(remote(
                exp.at[:, pl.ds(pl.multiple_of(1024 * half + 256 * xs[o], 256), 256)],
                w1.at[y, x, c, :, pl.ds(256 * half, 256)],
                ws.at[o - 1, half], wr.at[o - 1, half], x=xs[o],
            ))
        vec_copies[o] = go(remote(
            vec.at[xs[o]], vecs.at[slot_of[o]], vs.at[o - 1], vr.at[o - 1], x=xs[o]
        ))
    shr_y = go(remote(shr, w2.at[y, c], ss.at[0], sr.at[0], y=oy))
    shr_c = go(remote(shr, w2.at[y, c], ss.at[1], sr.at[1], c=oc))
    a, b = pl.ds(0, SEAM), pl.ds(SEAM, TOK - SEAM)
    right_a = go(remote(cot.at[0, a], cots.at[1, a], cs.at[0], cr.at[1, 0], x=xs[1]))
    left_b = go(remote(cot.at[0, b], cots.at[2, b], cs.at[2], cr.at[2, 1], x=xs[3]))
    right_b = go(remote(cot.at[0, b], cots.at[1, b], cs.at[1], cr.at[1, 1], x=xs[1]))
    left_a = go(remote(cot.at[0, a], cots.at[2, a], cs.at[3], cr.at[2, 0], x=xs[3]))

    vecs[0] = vec[x]
    here[0].wait()
    tokens = tbuf[...].astype(f32)
    centered = tokens - jnp.mean(tokens, axis=1, keepdims=True)
    variance = jnp.mean(centered * centered, axis=1, keepdims=True)
    inv = lax.rsqrt(variance + eps)
    normed[...] = centered * inv
    gained[...] = centered * inv * gain[...]
    invs[...] = jnp.broadcast_to(inv, invs.shape)
    total[...] = jnp.zeros_like(total)
    sacc[...] = jnp.zeros_like(sacc)
    eacc[...] = jnp.zeros_like(eacc)
    for copy in here[1:]:
        copy.wait()

    for o in (1, 3, 2):
        exp_copies[o, 0].wait_recv()
        exp_copies[o, 1].wait_recv()
    exp_y = go(remote(w1.at[y, :, c], w1.at[y, :, c], es.at[0], er.at[0], y=oy))
    exp_c = go(remote(w1.at[y, :, c], w1.at[y, :, c], es.at[1], er.at[1], c=oc))
    shr_y.wait_recv()
    shr_f = go(remote(w2.at[oy, c], w2.at[oy, c], ss.at[2], sr.at[2], c=oc))
    for o in (1, 3, 2):
        vec_copies[o].wait_recv()

    @pl.loop(0, 4)
    def _(k):
        si[k] = (gained[...] * row(vecs[k], 0)).astype(bf16)

    right_a.wait_recv()
    left_b.wait_recv()
    fwd = []
    for i, (lo, hi) in enumerate(PIECES):
        src, to = ((1, xs[1]), (2, xs[3]))[i % 2]
        piece = pl.ds(lo, hi - lo)
        fwd.append(go(remote(cots.at[src, piece], cots.at[3, piece], cs.at[4 + i], cr.at[3, i], x=to)))
    exp_y.wait_recv()
    exp_f = go(remote(w1.at[oy, :, c], w1.at[oy, :, c], es.at[2], er.at[2], c=oc))
    for copy in (shr_c, exp_c, shr_f, exp_f):
        copy.wait_recv()
    told(0, 2)
    tell_z(1)

    @pl.loop(0, 4)
    def _(k):
        v = vecs[k]
        project = dot(si[k], w1[...].reshape(D, SL), 1, 0)
        active, slope = gelu_pair(project * v[4:5])
        proj[k] = project
        actf[k] = active
        act[k] = (active * v[5:6]).astype(bf16)
        pa[k] = slope * v[5:6]

    told(1, 2)
    tell_z(2)

    def take(ref, k, rows):
        blocks = [ref[k, lo:hi] for lo, hi in rows]
        return blocks[0] if len(blocks) == 1 else jnp.concatenate(blocks, axis=0)

    def back_part(k, rows, first):
        v = vecs[k]
        scale_out = row(v, 2)
        second = w2[...].reshape(SL, D)
        seed = take(cots, k, rows)
        scaled_cot = (seed.astype(f32) * scale_out).astype(bf16)
        back = dot(scaled_cot, second, 1, 1)
        grad_act = jnp.sum(back * take(actf, k, rows), axis=0, keepdims=True)
        back_hidden = back * take(pa, k, rows)
        grad_hid = jnp.sum(back_hidden * take(proj, k, rows), axis=0, keepdims=True)
        back_proj = (back_hidden * v[4:5]).astype(bf16)
        both = dot(take(act, k, rows), seed, 0, 0)
        sacc[...] += both * scale_out
        grad_out = jnp.sum(second.astype(f32) * both, axis=0, keepdims=True)
        zero = jnp.zeros((2, SL), f32)
        lines = jnp.concatenate([grad_out[:, :SL], grad_out[:, SL:], grad_hid, grad_act, zero], axis=0)
        sv[k, 2:8] = lines if first else sv[k, 2:8] + lines
        return back_proj

    def expand_part(k, rows, back_proj):
        eacc[...] += dot(take(si, k, rows), back_proj, 0, 0)

    def norm_part(k, rows, first, back_proj):
        back_norm = dot(back_proj, w1[...].reshape(D, SL), 1, 1)
        share = back_norm * row(vecs[k], 0)
        grad_in = 0.0
        at = 0
        for lo, hi in rows:
            end = at + hi - lo
            grad_in = grad_in + jnp.sum(back_norm[at:end] * gained[lo:hi], axis=0, keepdims=True)
            total[lo:hi] += share[at:end]
            at = end
        lines = jnp.concatenate([grad_in[:, :SL], grad_in[:, SL:]], axis=0)
        sv[k, 0:2] = lines if first else sv[k, 0:2] + lines

    @pl.loop(0, 3)
    def _(k):
        @pl.when(k == 1)
        def _():
            right_b.wait_recv()

        @pl.when(k == 2)
        def _():
            left_a.wait_recv()

        every = ((0, TOK),)
        back_proj = back_part(k, every, True)
        expand_part(k, every, back_proj)
        norm_part(k, every, True, back_proj)

    right, left, far = (lax.rem(place + o, 4) for o in (1, 3, 2))
    to_right = dict(y=lax.rem(right, 2), h=right // 2)
    to_left = dict(y=lax.rem(left, 2), h=left // 2)
    top, low = pl.ds(0, 4), pl.ds(4, 4)

    def core_step(i):
        return go(remote(pbuf.at[i, oc], rbuf.at[i], as_.at[i], ar.at[i], c=oc))

    def ring_start(i, copy):
        copy.wait_recv()
        q[i] = added(pbuf[i, c], rbuf[i]).astype(bf16)
        return [
            go(remote(q.at[i, far, top], yb.at[i, 0], ys.at[i, 0], yr.at[i, 0], **to_right)),
            go(remote(q.at[i, far, low], yb.at[i, 1], ys.at[i, 1], yr.at[i, 1], **to_left)),
            go(remote(q.at[i, right, low], yb.at[i, 2], ys.at[i, 2], yr.at[i, 2], **to_right)),
            go(remote(q.at[i, left, top], yb.at[i, 3], ys.at[i, 3], yr.at[i, 3], **to_left)),
        ]

    def ring_pass(i, copies):
        copies[0].wait_recv()
        mix[i, 0] = added(q[i, right, 0:4], yb[i, 0]).astype(bf16)
        copies.append(go(remote(mix.at[i, 0], yb.at[i, 4], ys.at[i, 4], yr.at[i, 4], **to_right)))
        copies[1].wait_recv()
        mix[i, 1] = added(q[i, left, 4:8], yb[i, 1]).astype(bf16)
        copies.append(go(remote(mix.at[i, 1], yb.at[i, 5], ys.at[i, 5], yr.at[i, 5], **to_left)))

    def deep_start(i, copies):
        for copy in copies[2:]:
            copy.wait_recv()
        r[i, 0:4] = added(q[i, place, 0:4], yb[i, 3], yb[i, 4]).astype(bf16)
        r[i, 4:8] = added(q[i, place, 4:8], yb[i, 2], yb[i, 5]).astype(bf16)
        out = []
        if i == 0:
            for o in (4, 3, 5, 2, 6, 1, 7):
                e = lax.rem(z + o, 8)
                out.append(go(remote(r.at[0, e], rz.at[0, z], zs.at[0, o], zr.at[0, o], z=e)))
            rz[0, z] = r[0, z]
            return out
        mine = pl.ds(pl.multiple_of(128 * x, 128), 128)
        for o in (4, 3, 5, 2, 6, 1, 7, 0):
            e = lax.rem(z + o, 8)
            for xo in range(4):
                if o or xo:
                    block = pl.ds(pl.multiple_of(128 * xs[xo], 128), 128)
                    out.append(go(remote(
                        r.at[1, e, :, block], rz.at[1, z, :, mine], zs.at[1 + xo, o], zr.at[1 + xo, o],
                        z=e, x=xs[xo],
                    )))
        rz[1, z, :, mine] = r[1, z, :, mine]
        return out

    def deep_sum(i, copies):
        for copy in copies:
            copy.wait_recv()
        done = added(*(rz[i, e] for e in range(8))).astype(bf16)
        res[i] = done
        return done

    peers = []
    for o in range(1, 16):
        e = lax.rem(me + o, 16)
        peers.append((o, dict(z=e // 2, h=lax.rem(e, 2))))

    told(2, 2)
    greet(heard.at[3], h=1 - h)
    fwd[0].wait_recv()
    fwd[1].wait_recv()
    mid, ends = ((EDGE, EDGE2),), ((0, EDGE), (EDGE2, TOK))
    back_proj = back_part(3, mid, True)
    expand_part(3, mid, back_proj)
    norm_part(3, mid, True, back_proj)
    told(3, 1)
    for o in (1, 2, 3):
        greet(heard.at[4], x=xs[o])
    fwd[2].wait_recv()
    fwd[3].wait_recv()
    back_proj = back_part(3, ends, False)
    for cc in (0, 1):
        for hh in (0, 1):
            for yy in (0, 1):
                at = (yy * 2 + cc) * 128
                block = sacc[at : at + 128, SL * hh : SL * hh + SL]
                pbuf[0, cc, 2 * hh + yy] = block.astype(bf16).reshape(8, 16, SL)
    core_s = core_step(0)
    expand_part(3, ends, back_proj)
    for cc in (0, 1):
        for hh in (0, 1):
            for yy in (0, 1):
                for xx in range(4):
                    at = ((yy * 4 + xx) * 2 + cc) * 64
                    for zz in range(8):
                        top_row, lane = at + zz // 2 * 16, (zz % 2 * 2 + hh) * 128
                        pbuf[1, cc, 2 * hh + yy, zz, :, 128 * xx : 128 * xx + 128] = eacc[
                            top_row : top_row + 16, lane : lane + 128
                        ].astype(bf16)
    core_e = core_step(1)
    ring_s = ring_start(0, core_s)
    norm_part(3, ends, False, back_proj)
    ring_e = ring_start(1, core_e)

    vector_copies = []
    for slot, xo in ((1, 3), (2, 1), (3, 2)):
        vector_copies.append(go(remote(sv.at[slot], svr.at[x], bs.at[xo - 1], br.at[xo - 1], x=xs[xo])))
    svr[x] = sv[0]
    whole = total[...]
    gp[...] = jnp.sum(whole * normed[...], axis=0, keepdims=True)
    gains = []
    for o in range(1, 16):
        yo, xo, co = o // 8, (o // 2) % 4, o % 2
        gains.append(go(remote(
            gp, gpr.at[chip * 2 + c], gs.at[o], gr.at[o], y=oy if yo else y, x=xs[xo], c=oc if co else c
        )))
    gpr[chip * 2 + c] = gp[...]
    unit = whole * gain[...]
    inner = jnp.mean(unit * normed[...], axis=1, keepdims=True)
    back_trunk = invs[:, :1] * (unit - jnp.mean(unit, axis=1, keepdims=True) - normed[...] * inner)
    term = (cots[0].astype(f32) + back_trunk).astype(bf16)
    t[0] = term[:CUT]
    t[1, : TOK - CUT] = term[CUT:]
    t[1, TOK - CUT :] = jnp.zeros((FULL - TOK, D), bf16)
    core_t = go(remote(t.at[oc], rt, as_.at[2], ar.at[2], c=oc))

    ring_pass(0, ring_s)
    ring_pass(1, ring_e)

    core_t.wait_recv()
    joint = added(t[c], rt[...]).astype(bf16)
    for g in range(8):
        tq[g] = joint[:, 128 * g : 128 * g + 128]
    tiles = []
    for g in range(1, 8):
        yo, xo = g // 4, g % 4
        ty, tx = oy if yo else y, xs[xo]
        tiles.append(go(remote(tq.at[ty * 4 + tx], tr.at[chip], ts.at[g], tr_.at[g], y=ty, x=tx)))
    tr[chip] = tq[chip]

    told(4, 3)
    deep_s = deep_start(0, ring_s)

    for copy in vector_copies + gains:
        copy.wait_recv()
    sums = svr[0] + svr[1] + svr[2] + svr[3]
    gain_sum = gpr[0]
    for m in range(1, 16):
        gain_sum = gain_sum + gpr[m]
    zero = jnp.zeros((1, SL), f32)
    for i in range(4):
        dv[i] = sums[i : i + 1]
        dv[4 + i] = svr[i, 4:5]
        dv[8 + i] = svr[i, 5:6]
    dv[12] = gain_sum[:, :SL]
    dv[13] = gain_sum[:, SL:]
    dv[14] = zero
    dv[15] = zero
    small = []
    for o, where in peers:
        e = where["z"] * 2 + where["h"]
        small.append(go(remote(dv.at[e], dvr.at[me], ds.at[o], dr.at[o], **where)))
    dvr[me] = dv[me]

    deep_e = deep_start(1, ring_e)

    for copy in tiles:
        copy.wait_recv()
    tf[c] = added(*(tr[g] for g in range(8))).astype(bf16)
    finish = go(remote(tf.at[c], tf.at[c], fs, fr, c=oc))

    for copy in small:
        copy.wait_recv()
    line = dvr[0]
    for p in range(1, 16):
        line = line + dvr[p]
    dvs[...] = line
    lines = []
    for o, where in peers:
        lines.append(go(remote(dvs, dvo.at[me], os_.at[o], or_.at[o], **where)))
    dvo[me] = line

    outs = (sh, ex)

    def spread(i):
        copies = {}
        for o in (2, 6, 1, 7, 0):
            e = lax.rem(z + o, 8)
            for ho in (0, 1):
                if o or ho:
                    copies[o, ho] = go(remote(
                        res.at[i], outs[i].at[me], hs.at[i, o, ho], hr.at[i, o, ho],
                        z=e, h=1 - h if ho else h,
                    ))
        return copies

    def relay(i, copies):
        for o, further in ((2, (4, 3)), (6, (5,))):
            for ho in (0, 1):
                copies[o, ho].wait_recv()
                place = lax.rem(z + 8 - o, 8) * 2 + (1 - h if ho else h)
                for far_o in further:
                    copies[far_o, ho] = go(remote(
                        outs[i].at[place], outs[i].at[place], hs.at[i, far_o, ho], hr.at[i, far_o, ho],
                        z=lax.rem(z + far_o - o + 8, 8),
                    ))

    done = deep_sum(0, deep_s)
    spread_s = spread(0)
    sh[me] = done
    done = deep_sum(1, deep_e)
    spread_e = spread(1)
    ex[me] = done
    relay(0, spread_s)
    relay(1, spread_e)

    for copy in [finish] + lines:
        copy.wait_recv()
    for copies in (spread_s, spread_e):
        for (o, ho), copy in copies.items():
            if o not in (2, 6):
                copy.wait_recv()

    for copy in sent:
        copy.wait_send()


def finish_kernel(tf, sh, ex, dvo, tg, eg, sg, ing, hg, ag, og, gg):
    c = lax.axis_index("c")
    turned = tf[...].reshape(FULL, 128).astype(f32).T
    tg[...] = jnp.where(c == 0, turned[:64], turned[64:])[:, :TOK].astype(bf16)
    for i in (0, 1):
        ing[:, SL * i : SL * i + SL] = dvo[i]
        og[:, SL * i : SL * i + SL] = dvo[2 + i]
        gg[:, SL * i : SL * i + SL] = dvo[12 + i]
        for xx in range(4):
            at = 1024 * i + 256 * xx
            hg[:, at : at + 256] = dvo[4 + xx][:, 256 * i : 256 * i + 256]
            ag[:, at : at + 256] = dvo[8 + xx][:, 256 * i : 256 * i + 256]
    for p in range(16):
        low, lane = p // 4 * 16, p % 4 // 2 * 1024 + p % 2 * 128
        for xx in range(4):
            at = lane + 256 * xx
            eg[low : low + 16, at : at + 128] = ex[p, :, 128 * xx : 128 * xx + 128].astype(f32)
        sg[16 * (p // 2) : 16 * (p // 2) + 16, SL * (p % 2) : SL * (p % 2) + SL] = sh[p].astype(f32)


def vmem(n):
    return [pl.BlockSpec(memory_space=pltpu.VMEM)] * n


def dma(*shape):
    return pltpu.SemaphoreType.DMA(shape)


def body(trunk, normgain, expand, shrink, inscale, hidscale, actscale, outscale, cotangent):
    S = jax.ShapeDtypeStruct
    V = pltpu.VMEM
    parts = pl.pallas_call(
        kernel,
        out_shape=[
            S((2, CUT, 128), bf16),
            S((16, 16, SL), bf16),
            S((16, 16, SL), bf16),
            S((16, 1, SL), f32),
        ],
        in_specs=[pl.BlockSpec(memory_space=pl.ANY)] * 4 + vmem(5),
        out_specs=vmem(4),
        scratch_shapes=[
            V((TOK, D), bf16),
            V((4, 8, SL), f32),
            V((TOK, D), f32),
            V((TOK, D), f32),
            V((TOK, 128), f32),
            V((4, TOK, D), bf16),
            V((2, 4, 2, 64, SL), bf16),
            V((2, 2, 128, D), bf16),
            V((4, 8, SL), f32),
            V((4, TOK, D), bf16),
            V((4, TOK, SL), bf16),
            V((4, TOK, SL), f32),
            V((4, TOK, SL), f32),
            V((4, TOK, SL), f32),
            V((TOK, D), f32),
            V((SL, D), f32),
            V((D, SL), f32),
            V((2, 2, 4, 8, 16, SL), bf16),
            V((2, 4, 8, 16, SL), bf16),
            V((2, CUT, D), bf16),
            V((CUT, D), bf16),
            V((2, 4, 8, 16, SL), bf16),
            V((2, 6, 4, 16, SL), bf16),
            V((2, 2, 4, 16, SL), bf16),
            V((2, 8, 16, SL), bf16),
            V((2, 8, 16, SL), bf16),
            V((2, 16, SL), bf16),
            V((8, CUT, 128), bf16),
            V((8, CUT, 128), bf16),
            V((4, 8, SL), f32),
            V((4, 8, SL), f32),
            V((1, D), f32),
            V((16, 1, D), f32),
            V((16, 1, SL), f32),
            V((16, 1, SL), f32),
            V((1, SL), f32),
            dma(5), dma(8), dma(4, 4), dma(3, 2), dma(3, 2), dma(3), dma(3), dma(3), dma(3), dma(3), dma(3),
            dma(3), dma(3), dma(2, 6), dma(2, 6), dma(5, 8), dma(5, 8), dma(2, 8, 2), dma(2, 8, 2),
            dma(8), dma(8), pltpu.SemaphoreType.DMA, pltpu.SemaphoreType.DMA, dma(3), dma(3), dma(16), dma(16),
            dma(16), dma(16), dma(16), dma(16), pltpu.SemaphoreType.REGULAR((5,)),
        ],
        compiler_params=pltpu.CompilerParams(
            collective_id=0, has_side_effects=True, vmem_limit_bytes=60 * 1024 * 1024
        ),
        name="exchange_compute",
    )(
        trunk, expand, shrink, cotangent, normgain.reshape(1, D), inscale, hidscale, actscale, outscale
    )
    tg, eg, sg, ing, hg, ag, og, gg = pl.pallas_call(
        finish_kernel,
        out_shape=[
            S((64, TOK), bf16),
            S((64, FF), f32),
            S((128, D), f32),
            S((1, D), f32),
            S((1, FF), f32),
            S((1, FF), f32),
            S((1, D), f32),
            S((1, D), f32),
        ],
        in_specs=vmem(4),
        out_specs=vmem(8),
        name="write_outputs",
    )(*parts)
    return tg.T, eg, sg, ing, hg, ag, og, gg.reshape(D)


def solution(mesh):
    finer = Mesh(mesh.devices.reshape(2, 4, 2, 8, 2), AXES)
    rows = P(MEMBER, None)
    in_specs = (P(DP, None), P(), rows, rows, rows, rows, rows, rows, P(MEMBER, DP, None))
    out_specs = (P(DP, MEMBER), rows, rows, rows, rows, rows, rows, P())
    return jax.shard_map(body, mesh=finer, in_specs=in_specs, out_specs=out_specs, check_vma=False)
```

```python
import jax
import jax.numpy as jnp
from jax import lax
from jax.experimental import pallas as pl
from jax.experimental.pallas import tpu as pltpu
from jax.sharding import Mesh
from jax.sharding import PartitionSpec as P

AXES = ("y", "x", "c", "z", "h")
MEMBER = ("y", "x", "c")
DP = ("z", "h")
TOK = 394
CUT = 208
EDGE = 96
SEAM = 192
EDGE2 = 288
PIECES = ((EDGE, SEAM), (SEAM, EDGE2), (0, EDGE), (EDGE2, TOK))
FULL = 416
D = 1024
FF = 2048
SL = 512

eps = 1e-06
coeff = 0.7978845608028654
f32 = jnp.float32
bf16 = jnp.bfloat16
MESH = pl.DeviceIdType.MESH


def remote(src, dst, send, recv, **where):
    return pltpu.make_async_remote_copy(
        src_ref=src, dst_ref=dst, send_sem=send, recv_sem=recv, device_id=where, device_id_type=MESH
    )


def greet(barrier, **where):
    pl.semaphore_signal(barrier, inc=1, device_id=where, device_id_type=MESH)


def gelu_pair(hidden):
    inner = coeff * (hidden + 0.044715 * hidden * hidden * hidden)
    tangent = jnp.tanh(inner)
    active = 0.5 * hidden * (1.0 + tangent)
    slope = 0.5 * (1.0 + tangent) + 0.5 * hidden * (1.0 - tangent * tangent) * coeff * (
        1.0 + 3.0 * 0.044715 * hidden * hidden
    )
    return active, slope


def dot(a, b, ca, cb):
    return lax.dot_general(a, b, (((ca,), (cb,)), ((), ())), preferred_element_type=f32)


def row(v, i):
    return jnp.concatenate([v[i : i + 1], v[i + 1 : i + 2]], axis=1)


def added(*refs):
    total = refs[0].astype(f32)
    for r in refs[1:]:
        total = total + r.astype(f32)
    return total


def kernel(
    trunk, exp, shr, cot, gain_in, in_in, hid_in, act_in, out_in,
    tf, sh, ex, dvo,
    gain, inscale, hidscale, actscale, outscale, tbuf, vec, normed, gained, invs, cots, w1, w2, vecs, si, act, pa, actf, proj, total, sacc, eacc,
    pbuf, rbuf, t, rt, q, yb, mix, r, rz, res, tq, tr, sv, svr, gp, gpr, dv, dvr, dvs,
    ls, cs, cr, ws, wr, vs, vr, ss, sr, es, er,
    as_, ar, ys, yr, zs, zr, hs, hr, ts, tr_, fs, fr, bs, br, gs, gr, ds, dr, os_, or_, heard,
):
    y, x, c, z, h = (lax.axis_index(a) for a in AXES)
    xs = [lax.rem(x + o, 4) for o in range(4)]
    oy, oc = 1 - y, 1 - c
    me = z * 2 + h
    chip = y * 4 + x
    place = h * 2 + y
    sent = []

    def go(copy):
        copy.start()
        sent.append(copy)
        return copy

    barrier = pltpu.get_barrier_semaphore()

    for yo in (0, 1):
        for co in (0, 1):
            for xo in range(4):
                if yo or co or xo:
                    greet(barrier, y=oy if yo else y, x=xs[xo], c=oc if co else c)
    greet(barrier, y=oy, h=1 - h)
    greet(barrier, h=1 - h)
    above, below = lax.rem(z + 1, 8), lax.rem(z + 7, 8)
    greet(barrier, z=above)
    greet(barrier, z=below)

    def tell_z(i):
        greet(heard.at[i], z=above)
        greet(heard.at[i], z=below)

    def told(i, n):
        pl.semaphore_wait(heard.at[i], n)

    here = [
        pltpu.make_async_copy(trunk, tbuf, ls.at[0]),
        pltpu.make_async_copy(shr, w2.at[y, c], ls.at[1]),
        pltpu.make_async_copy(cot.at[0], cots.at[0], ls.at[2]),
    ]
    for half in (0, 1):
        here.append(
            pltpu.make_async_copy(
                exp.at[:, pl.ds(pl.multiple_of(1024 * half + 256 * x, 256), 256)],
                w1.at[y, x, c, :, pl.ds(256 * half, 256)],
                ls.at[3 + half],
            )
        )
    lines = []
    for i, (src, dst) in enumerate(
        ((in_in, inscale), (hid_in, hidscale), (act_in, actscale), (out_in, outscale), (gain_in, gain))
    ):
        lines.append(pltpu.make_async_copy(src, dst, ls.at[5 + i]))
    for copy in lines + here:
        copy.start()
    pl.semaphore_wait(barrier, 19)
    tell_z(0)

    slot_of = {1: 1, 3: 2, 2: 3}
    vec_copies, exp_copies = {}, {}
    for o in (1, 3, 2):
        for half in (0, 1):
            exp_copies[o, half] = go(remote(
                exp.at[:, pl.ds(pl.multiple_of(1024 * half + 256 * xs[o], 256), 256)],
                w1.at[y, x, c, :, pl.ds(256 * half, 256)],
                ws.at[o - 1, half], wr.at[o - 1, half], x=xs[o],
            ))
    shr_y = go(remote(shr, w2.at[y, c], ss.at[0], sr.at[0], y=oy))
    shr_c = go(remote(shr, w2.at[y, c], ss.at[1], sr.at[1], c=oc))
    for copy in lines:
        copy.wait()
    for xx in range(4):
        for i in (0, 1):
            vec[xx, i : i + 1] = inscale[:, SL * i : SL * i + SL]
            vec[xx, 2 + i : 3 + i] = outscale[:, SL * i : SL * i + SL]
            at = 1024 * i + 256 * xx
            vec[xx, 4:5, 256 * i : 256 * i + 256] = hidscale[:, at : at + 256]
            vec[xx, 5:6, 256 * i : 256 * i + 256] = actscale[:, at : at + 256]
        vec[xx, 6:8] = jnp.zeros((2, SL), f32)
    for o in (1, 3, 2):
        vec_copies[o] = go(remote(
            vec.at[xs[o]], vecs.at[slot_of[o]], vs.at[o - 1], vr.at[o - 1], x=xs[o]
        ))
    a, b = pl.ds(0, SEAM), pl.ds(SEAM, TOK - SEAM)
    right_a = go(remote(cot.at[0, a], cots.at[1, a], cs.at[0], cr.at[1, 0], x=xs[1]))
    left_b = go(remote(cot.at[0, b], cots.at[2, b], cs.at[2], cr.at[2, 1], x=xs[3]))
    right_b = go(remote(cot.at[0, b], cots.at[1, b], cs.at[1], cr.at[1, 1], x=xs[1]))
    left_a = go(remote(cot.at[0, a], cots.at[2, a], cs.at[3], cr.at[2, 0], x=xs[3]))

    vecs[0] = vec[x]
    here[0].wait()
    tokens = tbuf[...].astype(f32)
    centered = tokens - jnp.mean(tokens, axis=1, keepdims=True)
    variance = jnp.mean(centered * centered, axis=1, keepdims=True)
    inv = lax.rsqrt(variance + eps)
    normed[...] = centered * inv
    gained[...] = centered * inv * gain[...]
    invs[...] = jnp.broadcast_to(inv, invs.shape)
    total[...] = jnp.zeros_like(total)
    sacc[...] = jnp.zeros_like(sacc)
    eacc[...] = jnp.zeros_like(eacc)
    for copy in here[1:]:
        copy.wait()

    for o in (1, 3, 2):
        exp_copies[o, 0].wait_recv()
        exp_copies[o, 1].wait_recv()
    exp_y = go(remote(w1.at[y, :, c], w1.at[y, :, c], es.at[0], er.at[0], y=oy))
    exp_c = go(remote(w1.at[y, :, c], w1.at[y, :, c], es.at[1], er.at[1], c=oc))
    shr_y.wait_recv()
    shr_f = go(remote(w2.at[oy, c], w2.at[oy, c], ss.at[2], sr.at[2], c=oc))
    for o in (1, 3, 2):
        vec_copies[o].wait_recv()

    @pl.loop(0, 4)
    def _(k):
        si[k] = (gained[...] * row(vecs[k], 0)).astype(bf16)

    right_a.wait_recv()
    left_b.wait_recv()
    fwd = []
    for i, (lo, hi) in enumerate(PIECES):
        src, to = ((1, xs[1]), (2, xs[3]))[i % 2]
        piece = pl.ds(lo, hi - lo)
        fwd.append(go(remote(cots.at[src, piece], cots.at[3, piece], cs.at[4 + i], cr.at[3, i], x=to)))
    exp_y.wait_recv()
    exp_f = go(remote(w1.at[oy, :, c], w1.at[oy, :, c], es.at[2], er.at[2], c=oc))
    for copy in (shr_c, exp_c, shr_f, exp_f):
        copy.wait_recv()
    told(0, 2)
    tell_z(1)

    @pl.loop(0, 4)
    def _(k):
        v = vecs[k]
        project = dot(si[k], w1[...].reshape(D, SL), 1, 0)
        active, slope = gelu_pair(project * v[4:5])
        proj[k] = project
        actf[k] = active
        act[k] = (active * v[5:6]).astype(bf16)
        pa[k] = slope * v[5:6]

    told(1, 2)
    tell_z(2)

    def take(ref, k, rows):
        blocks = [ref[k, lo:hi] for lo, hi in rows]
        return blocks[0] if len(blocks) == 1 else jnp.concatenate(blocks, axis=0)

    def back_part(k, rows, first):
        v = vecs[k]
        scale_out = row(v, 2)
        second = w2[...].reshape(SL, D)
        seed = take(cots, k, rows)
        scaled_cot = (seed.astype(f32) * scale_out).astype(bf16)
        back = dot(scaled_cot, second, 1, 1)
        grad_act = jnp.sum(back * take(actf, k, rows), axis=0, keepdims=True)
        back_hidden = back * take(pa, k, rows)
        grad_hid = jnp.sum(back_hidden * take(proj, k, rows), axis=0, keepdims=True)
        back_proj = (back_hidden * v[4:5]).astype(bf16)
        both = dot(take(act, k, rows), seed, 0, 0)
        sacc[...] += both * scale_out
        grad_out = jnp.sum(second.astype(f32) * both, axis=0, keepdims=True)
        zero = jnp.zeros((2, SL), f32)
        lines = jnp.concatenate([grad_out[:, :SL], grad_out[:, SL:], grad_hid, grad_act, zero], axis=0)
        sv[k, 2:8] = lines if first else sv[k, 2:8] + lines
        return back_proj

    def expand_part(k, rows, back_proj):
        eacc[...] += dot(take(si, k, rows), back_proj, 0, 0)

    def norm_part(k, rows, first, back_proj):
        back_norm = dot(back_proj, w1[...].reshape(D, SL), 1, 1)
        share = back_norm * row(vecs[k], 0)
        grad_in = 0.0
        at = 0
        for lo, hi in rows:
            end = at + hi - lo
            grad_in = grad_in + jnp.sum(back_norm[at:end] * gained[lo:hi], axis=0, keepdims=True)
            total[lo:hi] += share[at:end]
            at = end
        lines = jnp.concatenate([grad_in[:, :SL], grad_in[:, SL:]], axis=0)
        sv[k, 0:2] = lines if first else sv[k, 0:2] + lines

    @pl.loop(0, 3)
    def _(k):
        @pl.when(k == 1)
        def _():
            right_b.wait_recv()

        @pl.when(k == 2)
        def _():
            left_a.wait_recv()

        every = ((0, TOK),)
        back_proj = back_part(k, every, True)
        expand_part(k, every, back_proj)
        norm_part(k, every, True, back_proj)

    right, left, far = (lax.rem(place + o, 4) for o in (1, 3, 2))
    to_right = dict(y=lax.rem(right, 2), h=right // 2)
    to_left = dict(y=lax.rem(left, 2), h=left // 2)
    top, low = pl.ds(0, 4), pl.ds(4, 4)

    def core_step(i):
        return go(remote(pbuf.at[i, oc], rbuf.at[i], as_.at[i], ar.at[i], c=oc))

    def ring_start(i, copy):
        copy.wait_recv()
        q[i] = added(pbuf[i, c], rbuf[i]).astype(bf16)
        return [
            go(remote(q.at[i, far, top], yb.at[i, 0], ys.at[i, 0], yr.at[i, 0], **to_right)),
            go(remote(q.at[i, far, low], yb.at[i, 1], ys.at[i, 1], yr.at[i, 1], **to_left)),
            go(remote(q.at[i, right, low], yb.at[i, 2], ys.at[i, 2], yr.at[i, 2], **to_right)),
            go(remote(q.at[i, left, top], yb.at[i, 3], ys.at[i, 3], yr.at[i, 3], **to_left)),
        ]

    def ring_pass(i, copies):
        copies[0].wait_recv()
        mix[i, 0] = added(q[i, right, 0:4], yb[i, 0]).astype(bf16)
        copies.append(go(remote(mix.at[i, 0], yb.at[i, 4], ys.at[i, 4], yr.at[i, 4], **to_right)))
        copies[1].wait_recv()
        mix[i, 1] = added(q[i, left, 4:8], yb[i, 1]).astype(bf16)
        copies.append(go(remote(mix.at[i, 1], yb.at[i, 5], ys.at[i, 5], yr.at[i, 5], **to_left)))

    def deep_start(i, copies):
        for copy in copies[2:]:
            copy.wait_recv()
        r[i, 0:4] = added(q[i, place, 0:4], yb[i, 3], yb[i, 4]).astype(bf16)
        r[i, 4:8] = added(q[i, place, 4:8], yb[i, 2], yb[i, 5]).astype(bf16)
        out = []
        if i == 0:
            for o in (4, 3, 5, 2, 6, 1, 7):
                e = lax.rem(z + o, 8)
                out.append(go(remote(r.at[0, e], rz.at[0, z], zs.at[0, o], zr.at[0, o], z=e)))
            rz[0, z] = r[0, z]
            return out
        mine = pl.ds(pl.multiple_of(128 * x, 128), 128)
        for o in (4, 3, 5, 2, 6, 1, 7, 0):
            e = lax.rem(z + o, 8)
            for xo in range(4):
                if o or xo:
                    block = pl.ds(pl.multiple_of(128 * xs[xo], 128), 128)
                    out.append(go(remote(
                        r.at[1, e, :, block], rz.at[1, z, :, mine], zs.at[1 + xo, o], zr.at[1 + xo, o],
                        z=e, x=xs[xo],
                    )))
        rz[1, z, :, mine] = r[1, z, :, mine]
        return out

    def deep_sum(i, copies):
        for copy in copies:
            copy.wait_recv()
        done = added(*(rz[i, e] for e in range(8))).astype(bf16)
        res[i] = done
        return done

    peers = []
    for o in range(1, 16):
        e = lax.rem(me + o, 16)
        peers.append((o, dict(z=e // 2, h=lax.rem(e, 2))))

    told(2, 2)
    greet(heard.at[3], h=1 - h)
    fwd[0].wait_recv()
    fwd[1].wait_recv()
    mid, ends = ((EDGE, EDGE2),), ((0, EDGE), (EDGE2, TOK))
    back_proj = back_part(3, mid, True)
    expand_part(3, mid, back_proj)
    norm_part(3, mid, True, back_proj)
    told(3, 1)
    for o in (1, 2, 3):
        greet(heard.at[4], x=xs[o])
    fwd[2].wait_recv()
    fwd[3].wait_recv()
    back_proj = back_part(3, ends, False)
    for cc in (0, 1):
        for hh in (0, 1):
            for yy in (0, 1):
                at = (yy * 2 + cc) * 128
                block = sacc[at : at + 128, SL * hh : SL * hh + SL]
                pbuf[0, cc, 2 * hh + yy] = block.astype(bf16).reshape(8, 16, SL)
    core_s = core_step(0)
    expand_part(3, ends, back_proj)
    for cc in (0, 1):
        for hh in (0, 1):
            for yy in (0, 1):
                for xx in range(4):
                    at = ((yy * 4 + xx) * 2 + cc) * 64
                    for zz in range(8):
                        top_row, lane = at + zz // 2 * 16, (zz % 2 * 2 + hh) * 128
                        pbuf[1, cc, 2 * hh + yy, zz, :, 128 * xx : 128 * xx + 128] = eacc[
                            top_row : top_row + 16, lane : lane + 128
                        ].astype(bf16)
    core_e = core_step(1)
    ring_s = ring_start(0, core_s)
    norm_part(3, ends, False, back_proj)
    ring_e = ring_start(1, core_e)

    vector_copies = []
    for slot, xo in ((1, 3), (2, 1), (3, 2)):
        vector_copies.append(go(remote(sv.at[slot], svr.at[x], bs.at[xo - 1], br.at[xo - 1], x=xs[xo])))
    svr[x] = sv[0]
    whole = total[...]
    gp[...] = jnp.sum(whole * normed[...], axis=0, keepdims=True)
    gains = []
    for o in range(1, 16):
        yo, xo, co = o // 8, (o // 2) % 4, o % 2
        gains.append(go(remote(
            gp, gpr.at[chip * 2 + c], gs.at[o], gr.at[o], y=oy if yo else y, x=xs[xo], c=oc if co else c
        )))
    gpr[chip * 2 + c] = gp[...]
    unit = whole * gain[...]
    inner = jnp.mean(unit * normed[...], axis=1, keepdims=True)
    back_trunk = invs[:, :1] * (unit - jnp.mean(unit, axis=1, keepdims=True) - normed[...] * inner)
    term = (cots[0].astype(f32) + back_trunk).astype(bf16)
    t[0] = term[:CUT]
    t[1, : TOK - CUT] = term[CUT:]
    t[1, TOK - CUT :] = jnp.zeros((FULL - TOK, D), bf16)
    core_t = go(remote(t.at[oc], rt, as_.at[2], ar.at[2], c=oc))

    ring_pass(0, ring_s)
    ring_pass(1, ring_e)
    told(4, 3)
    deep_s = deep_start(0, ring_s)
    deep_e = deep_start(1, ring_e)

    core_t.wait_recv()
    joint = added(t[c], rt[...]).astype(bf16)
    for g in range(8):
        tq[g] = joint[:, 128 * g : 128 * g + 128]
    tiles = []
    for g in range(1, 8):
        yo, xo = g // 4, g % 4
        ty, tx = oy if yo else y, xs[xo]
        tiles.append(go(remote(tq.at[ty * 4 + tx], tr.at[chip], ts.at[g], tr_.at[g], y=ty, x=tx)))
    tr[chip] = tq[chip]

    for copy in vector_copies + gains:
        copy.wait_recv()
    sums = svr[0] + svr[1] + svr[2] + svr[3]
    gain_sum = gpr[0]
    for m in range(1, 16):
        gain_sum = gain_sum + gpr[m]
    zero = jnp.zeros((1, SL), f32)
    for i in range(4):
        dv[i] = sums[i : i + 1]
        dv[4 + i] = svr[i, 4:5]
        dv[8 + i] = svr[i, 5:6]
    dv[12] = gain_sum[:, :SL]
    dv[13] = gain_sum[:, SL:]
    dv[14] = zero
    dv[15] = zero
    small = []
    for o, where in peers:
        e = where["z"] * 2 + where["h"]
        small.append(go(remote(dv.at[e], dvr.at[me], ds.at[o], dr.at[o], **where)))
    dvr[me] = dv[me]

    outs = (sh, ex)

    def spread(i):
        copies = {}
        for o in (2, 6, 1, 7, 0):
            e = lax.rem(z + o, 8)
            for ho in (0, 1):
                if o or ho:
                    copies[o, ho] = go(remote(
                        res.at[i], outs[i].at[me], hs.at[i, o, ho], hr.at[i, o, ho],
                        z=e, h=1 - h if ho else h,
                    ))
        return copies

    def relay(i, copies):
        for o, further in ((2, (4, 3)), (6, (5,))):
            for ho in (0, 1):
                copies[o, ho].wait_recv()
                place = lax.rem(z + 8 - o, 8) * 2 + (1 - h if ho else h)
                for far_o in further:
                    copies[far_o, ho] = go(remote(
                        outs[i].at[place], outs[i].at[place], hs.at[i, far_o, ho], hr.at[i, far_o, ho],
                        z=lax.rem(z + far_o - o + 8, 8),
                    ))

    done = deep_sum(0, deep_s)
    spread_s = spread(0)
    sh[me] = done
    done = deep_sum(1, deep_e)
    spread_e = spread(1)
    ex[me] = done

    for copy in tiles:
        copy.wait_recv()
    tf[c] = added(*(tr[g] for g in range(8))).astype(bf16)
    finish = go(remote(tf.at[c], tf.at[c], fs, fr, c=oc))

    for copy in small:
        copy.wait_recv()
    line = dvr[0]
    for p in range(1, 16):
        line = line + dvr[p]
    dvs[...] = line
    lines = []
    for o, where in peers:
        lines.append(go(remote(dvs, dvo.at[me], os_.at[o], or_.at[o], **where)))
    dvo[me] = line

    relay(0, spread_s)
    relay(1, spread_e)

    for copy in [finish] + lines:
        copy.wait_recv()
    for copies in (spread_s, spread_e):
        for (o, ho), copy in copies.items():
            if o not in (2, 6):
                copy.wait_recv()

    for copy in sent:
        copy.wait_send()


def finish_kernel(tf, sh, ex, dvo, tg, eg, sg, ing, hg, ag, og, gg):
    c = lax.axis_index("c")
    turned = tf[...].reshape(FULL, 128).astype(f32).T
    tg[...] = jnp.where(c == 0, turned[:64], turned[64:])[:, :TOK].astype(bf16)
    for i in (0, 1):
        ing[:, SL * i : SL * i + SL] = dvo[i]
        og[:, SL * i : SL * i + SL] = dvo[2 + i]
        gg[:, SL * i : SL * i + SL] = dvo[12 + i]
        for xx in range(4):
            at = 1024 * i + 256 * xx
            hg[:, at : at + 256] = dvo[4 + xx][:, 256 * i : 256 * i + 256]
            ag[:, at : at + 256] = dvo[8 + xx][:, 256 * i : 256 * i + 256]
    for p in range(16):
        low, lane = p // 4 * 16, p % 4 // 2 * 1024 + p % 2 * 128
        for xx in range(4):
            at = lane + 256 * xx
            eg[low : low + 16, at : at + 128] = ex[p, :, 128 * xx : 128 * xx + 128].astype(f32)
        sg[16 * (p // 2) : 16 * (p // 2) + 16, SL * (p % 2) : SL * (p % 2) + SL] = sh[p].astype(f32)


def vmem(n):
    return [pl.BlockSpec(memory_space=pltpu.VMEM)] * n


def dma(*shape):
    return pltpu.SemaphoreType.DMA(shape)


def body(trunk, normgain, expand, shrink, inscale, hidscale, actscale, outscale, cotangent):
    S = jax.ShapeDtypeStruct
    V = pltpu.VMEM
    parts = pl.pallas_call(
        kernel,
        out_shape=[
            V((2, CUT, 128), bf16),
            V((16, 16, SL), bf16),
            V((16, 16, SL), bf16),
            V((16, 1, SL), f32),
        ],
        in_specs=[pl.BlockSpec(memory_space=pl.ANY)] * 9,
        out_specs=vmem(4),
        scratch_shapes=[
            V((1, D), f32),
            V((1, D), f32),
            V((1, FF), f32),
            V((1, FF), f32),
            V((1, D), f32),
            V((TOK, D), bf16),
            V((4, 8, SL), f32),
            V((TOK, D), f32),
            V((TOK, D), f32),
            V((TOK, 128), f32),
            V((4, TOK, D), bf16),
            V((2, 4, 2, 64, SL), bf16),
            V((2, 2, 128, D), bf16),
            V((4, 8, SL), f32),
            V((4, TOK, D), bf16),
            V((4, TOK, SL), bf16),
            V((4, TOK, SL), f32),
            V((4, TOK, SL), f32),
            V((4, TOK, SL), f32),
            V((TOK, D), f32),
            V((SL, D), f32),
            V((D, SL), f32),
            V((2, 2, 4, 8, 16, SL), bf16),
            V((2, 4, 8, 16, SL), bf16),
            V((2, CUT, D), bf16),
            V((CUT, D), bf16),
            V((2, 4, 8, 16, SL), bf16),
            V((2, 6, 4, 16, SL), bf16),
            V((2, 2, 4, 16, SL), bf16),
            V((2, 8, 16, SL), bf16),
            V((2, 8, 16, SL), bf16),
            V((2, 16, SL), bf16),
            V((8, CUT, 128), bf16),
            V((8, CUT, 128), bf16),
            V((4, 8, SL), f32),
            V((4, 8, SL), f32),
            V((1, D), f32),
            V((16, 1, D), f32),
            V((16, 1, SL), f32),
            V((16, 1, SL), f32),
            V((1, SL), f32),
            dma(10), dma(8), dma(4, 4), dma(3, 2), dma(3, 2), dma(3), dma(3), dma(3), dma(3), dma(3), dma(3),
            dma(3), dma(3), dma(2, 6), dma(2, 6), dma(5, 8), dma(5, 8), dma(2, 8, 2), dma(2, 8, 2),
            dma(8), dma(8), pltpu.SemaphoreType.DMA, pltpu.SemaphoreType.DMA, dma(3), dma(3), dma(16), dma(16),
            dma(16), dma(16), dma(16), dma(16), pltpu.SemaphoreType.REGULAR((5,)),
        ],
        compiler_params=pltpu.CompilerParams(
            collective_id=0, has_side_effects=True, vmem_limit_bytes=60 * 1024 * 1024
        ),
        name="exchange_compute",
    )(
        trunk, expand, shrink, cotangent, normgain.reshape(1, D), inscale, hidscale, actscale, outscale
    )
    tg, eg, sg, ing, hg, ag, og, gg = pl.pallas_call(
        finish_kernel,
        out_shape=[
            S((64, TOK), bf16),
            S((64, FF), f32),
            S((128, D), f32),
            S((1, D), f32),
            S((1, FF), f32),
            S((1, FF), f32),
            S((1, D), f32),
            S((1, D), f32),
        ],
        in_specs=vmem(4),
        out_specs=vmem(8),
        name="write_outputs",
    )(*parts)
    return tg.T, eg, sg, ing, hg, ag, og, gg.reshape(D)


def solution(mesh):
    finer = Mesh(mesh.devices.reshape(2, 4, 2, 8, 2), AXES)
    rows = P(MEMBER, None)
    in_specs = (P(DP, None), P(), rows, rows, rows, rows, rows, rows, P(MEMBER, DP, None))
    out_specs = (P(DP, MEMBER), rows, rows, rows, rows, rows, rows, P())
    return jax.shard_map(body, mesh=finer, in_specs=in_specs, out_specs=out_specs, check_vma=False)
```

```python
import jax
import jax.numpy as jnp
from jax import lax
from jax.experimental import pallas as pl
from jax.experimental.pallas import tpu as pltpu
from jax.sharding import Mesh
from jax.sharding import PartitionSpec as P

AXES = ("y", "x", "c", "z", "h")
MEMBER = ("y", "x", "c")
DP = ("z", "h")
TOK = 394
CUT = 208
EDGE = 96
SEAM = 192
EDGE2 = 288
PIECES = ((0, EDGE), (EDGE2, TOK), (EDGE, SEAM), (SEAM, EDGE2))
FULL = 416
D = 1024
FF = 2048
SL = 512

eps = 1e-06
coeff = 0.7978845608028654
f32 = jnp.float32
bf16 = jnp.bfloat16
MESH = pl.DeviceIdType.MESH


def remote(src, dst, send, recv, **where):
    return pltpu.make_async_remote_copy(
        src_ref=src, dst_ref=dst, send_sem=send, recv_sem=recv, device_id=where, device_id_type=MESH
    )


def greet(barrier, **where):
    pl.semaphore_signal(barrier, inc=1, device_id=where, device_id_type=MESH)


def gelu_pair(hidden):
    inner = coeff * (hidden + 0.044715 * hidden * hidden * hidden)
    tangent = jnp.tanh(inner)
    active = 0.5 * hidden * (1.0 + tangent)
    slope = 0.5 * (1.0 + tangent) + 0.5 * hidden * (1.0 - tangent * tangent) * coeff * (
        1.0 + 3.0 * 0.044715 * hidden * hidden
    )
    return active, slope


def dot(a, b, ca, cb):
    return lax.dot_general(a, b, (((ca,), (cb,)), ((), ())), preferred_element_type=f32)


def row(v, i):
    return jnp.concatenate([v[i : i + 1], v[i + 1 : i + 2]], axis=1)


def added(*refs):
    total = refs[0].astype(f32)
    for r in refs[1:]:
        total = total + r.astype(f32)
    return total


def kernel(
    trunk, exp, shr, cot, gain_in, in_in, hid_in, act_in, out_in,
    tf, sh, ex, dvo,
    gain, inscale, hidscale, actscale, outscale, tbuf, vec, normed, gained, invs, cots, w1, w2, vecs, si, act, pa, actf, proj, total, sacc, eacc,
    pbuf, rbuf, t, rt, q, yb, mix, r, rz, res, tq, tr, sv, svr, gp, gpr, dv, dvr, dvs,
    ls, cs, cr, ws, wr, vs, vr, ss, sr, es, er,
    as_, ar, ys, yr, zs, zr, hs, hr, ts, tr_, fs, fr, bs, br, gs, gr, ds, dr, os_, or_, heard,
):
    y, x, c, z, h = (lax.axis_index(a) for a in AXES)
    xs = [lax.rem(x + o, 4) for o in range(4)]
    oy, oc = 1 - y, 1 - c
    me = z * 2 + h
    chip = y * 4 + x
    place = h * 2 + y
    sent = []

    def go(copy):
        copy.start()
        sent.append(copy)
        return copy

    barrier = pltpu.get_barrier_semaphore()

    for yo in (0, 1):
        for co in (0, 1):
            for xo in range(4):
                if yo or co or xo:
                    greet(barrier, y=oy if yo else y, x=xs[xo], c=oc if co else c)
    greet(barrier, y=oy, h=1 - h)
    greet(barrier, h=1 - h)
    above, below = lax.rem(z + 1, 8), lax.rem(z + 7, 8)
    greet(barrier, z=above)
    greet(barrier, z=below)

    def tell_z(i):
        greet(heard.at[i], z=above)
        greet(heard.at[i], z=below)

    def told(i, n):
        pl.semaphore_wait(heard.at[i], n)

    here = [
        pltpu.make_async_copy(trunk, tbuf, ls.at[0]),
        pltpu.make_async_copy(shr, w2.at[y, c], ls.at[1]),
        pltpu.make_async_copy(cot.at[0], cots.at[0], ls.at[2]),
    ]
    for half in (0, 1):
        here.append(
            pltpu.make_async_copy(
                exp.at[:, pl.ds(pl.multiple_of(1024 * half + 256 * x, 256), 256)],
                w1.at[y, x, c, :, pl.ds(256 * half, 256)],
                ls.at[3 + half],
            )
        )
    lines = []
    for i, (src, dst) in enumerate(
        ((in_in, inscale), (hid_in, hidscale), (act_in, actscale), (out_in, outscale), (gain_in, gain))
    ):
        lines.append(pltpu.make_async_copy(src, dst, ls.at[5 + i]))
    for copy in lines + here:
        copy.start()
    pl.semaphore_wait(barrier, 19)
    tell_z(0)

    slot_of = {1: 1, 3: 2, 2: 3}
    vec_copies, exp_copies = {}, {}
    for o in (1, 3, 2):
        for half in (0, 1):
            exp_copies[o, half] = go(remote(
                exp.at[:, pl.ds(pl.multiple_of(1024 * half + 256 * xs[o], 256), 256)],
                w1.at[y, x, c, :, pl.ds(256 * half, 256)],
                ws.at[o - 1, half], wr.at[o - 1, half], x=xs[o],
            ))
    shr_y = go(remote(shr, w2.at[y, c], ss.at[0], sr.at[0], y=oy))
    shr_c = go(remote(shr, w2.at[y, c], ss.at[1], sr.at[1], c=oc))
    for copy in lines:
        copy.wait()
    for xx in range(4):
        for i in (0, 1):
            vec[xx, i : i + 1] = inscale[:, SL * i : SL * i + SL]
            vec[xx, 2 + i : 3 + i] = outscale[:, SL * i : SL * i + SL]
            at = 1024 * i + 256 * xx
            vec[xx, 4:5, 256 * i : 256 * i + 256] = hidscale[:, at : at + 256]
            vec[xx, 5:6, 256 * i : 256 * i + 256] = actscale[:, at : at + 256]
        vec[xx, 6:8] = jnp.zeros((2, SL), f32)
    for o in (1, 3, 2):
        vec_copies[o] = go(remote(
            vec.at[xs[o]], vecs.at[slot_of[o]], vs.at[o - 1], vr.at[o - 1], x=xs[o]
        ))
    right_own, left_own = [], []
    for i, (lo, hi) in enumerate(((0, EDGE), (EDGE, SEAM), (SEAM, TOK))):
        piece = pl.ds(lo, hi - lo)
        right_own.append(remote(cot.at[0, piece], cots.at[1, piece], cs.at[i], cr.at[1, i], x=xs[1]))
    for i, (lo, hi) in enumerate(((EDGE2, TOK), (SEAM, EDGE2), (0, SEAM))):
        piece = pl.ds(lo, hi - lo)
        left_own.append(remote(cot.at[0, piece], cots.at[2, piece], cs.at[3 + i], cr.at[2, i], x=xs[3]))
    for i in range(3):
        go(right_own[i])
        go(left_own[i])

    vecs[0] = vec[x]
    here[0].wait()
    tokens = tbuf[...].astype(f32)
    centered = tokens - jnp.mean(tokens, axis=1, keepdims=True)
    variance = jnp.mean(centered * centered, axis=1, keepdims=True)
    inv = lax.rsqrt(variance + eps)
    normed[...] = centered * inv
    gained[...] = centered * inv * gain[...]
    invs[...] = jnp.broadcast_to(inv, invs.shape)
    total[...] = jnp.zeros_like(total)
    sacc[...] = jnp.zeros_like(sacc)
    eacc[...] = jnp.zeros_like(eacc)
    for copy in here[1:]:
        copy.wait()

    for o in (1, 3, 2):
        exp_copies[o, 0].wait_recv()
        exp_copies[o, 1].wait_recv()
    exp_y = go(remote(w1.at[y, :, c], w1.at[y, :, c], es.at[0], er.at[0], y=oy))
    exp_c = go(remote(w1.at[y, :, c], w1.at[y, :, c], es.at[1], er.at[1], c=oc))
    shr_y.wait_recv()
    shr_f = go(remote(w2.at[oy, c], w2.at[oy, c], ss.at[2], sr.at[2], c=oc))
    for o in (1, 3, 2):
        vec_copies[o].wait_recv()

    @pl.loop(0, 4)
    def _(k):
        si[k] = (gained[...] * row(vecs[k], 0)).astype(bf16)

    fwd = []
    for i, (lo, hi) in enumerate(PIECES):
        (right_own, left_own)[i % 2][i // 2].wait_recv()
        src, to = ((1, xs[1]), (2, xs[3]))[i % 2]
        piece = pl.ds(lo, hi - lo)
        fwd.append(go(remote(cots.at[src, piece], cots.at[3, piece], cs.at[6 + i], cr.at[3, i], x=to)))
    exp_y.wait_recv()
    exp_f = go(remote(w1.at[oy, :, c], w1.at[oy, :, c], es.at[2], er.at[2], c=oc))
    for copy in (shr_c, exp_c, shr_f, exp_f):
        copy.wait_recv()
    told(0, 2)
    tell_z(1)

    @pl.loop(0, 4)
    def _(k):
        v = vecs[k]
        project = dot(si[k], w1[...].reshape(D, SL), 1, 0)
        active, slope = gelu_pair(project * v[4:5])
        proj[k] = project
        actf[k] = active
        act[k] = (active * v[5:6]).astype(bf16)
        pa[k] = slope * v[5:6]

    told(1, 2)
    tell_z(2)

    def take(ref, k, rows):
        blocks = [ref[k, lo:hi] for lo, hi in rows]
        return blocks[0] if len(blocks) == 1 else jnp.concatenate(blocks, axis=0)

    def back_part(k, rows, first):
        v = vecs[k]
        scale_out = row(v, 2)
        second = w2[...].reshape(SL, D)
        seed = take(cots, k, rows)
        scaled_cot = (seed.astype(f32) * scale_out).astype(bf16)
        back = dot(scaled_cot, second, 1, 1)
        grad_act = jnp.sum(back * take(actf, k, rows), axis=0, keepdims=True)
        back_hidden = back * take(pa, k, rows)
        grad_hid = jnp.sum(back_hidden * take(proj, k, rows), axis=0, keepdims=True)
        back_proj = (back_hidden * v[4:5]).astype(bf16)
        both = dot(take(act, k, rows), seed, 0, 0)
        sacc[...] += both * scale_out
        grad_out = jnp.sum(second.astype(f32) * both, axis=0, keepdims=True)
        zero = jnp.zeros((2, SL), f32)
        lines = jnp.concatenate([grad_out[:, :SL], grad_out[:, SL:], grad_hid, grad_act, zero], axis=0)
        sv[k, 2:8] = lines if first else sv[k, 2:8] + lines
        return back_proj

    def expand_part(k, rows, back_proj):
        eacc[...] += dot(take(si, k, rows), back_proj, 0, 0)

    def norm_part(k, rows, first, back_proj):
        back_norm = dot(back_proj, w1[...].reshape(D, SL), 1, 1)
        share = back_norm * row(vecs[k], 0)
        grad_in = 0.0
        at = 0
        for lo, hi in rows:
            end = at + hi - lo
            grad_in = grad_in + jnp.sum(back_norm[at:end] * gained[lo:hi], axis=0, keepdims=True)
            total[lo:hi] += share[at:end]
            at = end
        lines = jnp.concatenate([grad_in[:, :SL], grad_in[:, SL:]], axis=0)
        sv[k, 0:2] = lines if first else sv[k, 0:2] + lines

    @pl.loop(0, 3)
    def _(k):
        @pl.when(k == 1)
        def _():
            right_own[2].wait_recv()

        @pl.when(k == 2)
        def _():
            left_own[2].wait_recv()

        every = ((0, TOK),)
        back_proj = back_part(k, every, True)
        expand_part(k, every, back_proj)
        norm_part(k, every, True, back_proj)

    right, left, far = (lax.rem(place + o, 4) for o in (1, 3, 2))
    to_right = dict(y=lax.rem(right, 2), h=right // 2)
    to_left = dict(y=lax.rem(left, 2), h=left // 2)
    top, low = pl.ds(0, 4), pl.ds(4, 4)

    def core_step(i):
        return go(remote(pbuf.at[i, oc], rbuf.at[i], as_.at[i], ar.at[i], c=oc))

    def ring_start(i, copy):
        copy.wait_recv()
        q[i] = added(pbuf[i, c], rbuf[i]).astype(bf16)
        return [
            go(remote(q.at[i, far, top], yb.at[i, 0], ys.at[i, 0], yr.at[i, 0], **to_right)),
            go(remote(q.at[i, far, low], yb.at[i, 1], ys.at[i, 1], yr.at[i, 1], **to_left)),
            go(remote(q.at[i, right, low], yb.at[i, 2], ys.at[i, 2], yr.at[i, 2], **to_right)),
            go(remote(q.at[i, left, top], yb.at[i, 3], ys.at[i, 3], yr.at[i, 3], **to_left)),
        ]

    def ring_pass(i, copies):
        copies[0].wait_recv()
        mix[i, 0] = added(q[i, right, 0:4], yb[i, 0]).astype(bf16)
        copies.append(go(remote(mix.at[i, 0], yb.at[i, 4], ys.at[i, 4], yr.at[i, 4], **to_right)))
        copies[1].wait_recv()
        mix[i, 1] = added(q[i, left, 4:8], yb[i, 1]).astype(bf16)
        copies.append(go(remote(mix.at[i, 1], yb.at[i, 5], ys.at[i, 5], yr.at[i, 5], **to_left)))

    def deep_start(i, copies):
        for copy in copies[2:]:
            copy.wait_recv()
        r[i, 0:4] = added(q[i, place, 0:4], yb[i, 3], yb[i, 4]).astype(bf16)
        r[i, 4:8] = added(q[i, place, 4:8], yb[i, 2], yb[i, 5]).astype(bf16)
        out = []
        if i == 0:
            for o in (4, 3, 5, 2, 6, 1, 7):
                e = lax.rem(z + o, 8)
                out.append(go(remote(r.at[0, e], rz.at[0, z], zs.at[0, o], zr.at[0, o], z=e)))
            rz[0, z] = r[0, z]
            return out
        mine = pl.ds(pl.multiple_of(128 * x, 128), 128)
        for o in (4, 3, 5, 2, 6, 1, 7, 0):
            e = lax.rem(z + o, 8)
            for xo in range(4):
                if o or xo:
                    block = pl.ds(pl.multiple_of(128 * xs[xo], 128), 128)
                    out.append(go(remote(
                        r.at[1, e, :, block], rz.at[1, z, :, mine], zs.at[1 + xo, o], zr.at[1 + xo, o],
                        z=e, x=xs[xo],
                    )))
        rz[1, z, :, mine] = r[1, z, :, mine]
        return out

    def deep_sum(i, copies):
        for copy in copies:
            copy.wait_recv()
        done = added(*(rz[i, e] for e in range(8))).astype(bf16)
        res[i] = done
        return done

    peers = []
    for o in range(1, 16):
        e = lax.rem(me + o, 16)
        peers.append((o, dict(z=e // 2, h=lax.rem(e, 2))))

    told(2, 2)
    greet(heard.at[3], h=1 - h)
    fwd[0].wait_recv()
    fwd[1].wait_recv()
    outer, inner = ((0, EDGE), (EDGE2, TOK)), ((EDGE, EDGE2),)
    back_proj = back_part(3, outer, True)
    expand_part(3, outer, back_proj)
    norm_part(3, outer, True, back_proj)
    told(3, 1)
    for o in (1, 2, 3):
        greet(heard.at[4], x=xs[o])
    fwd[2].wait_recv()
    fwd[3].wait_recv()
    back_proj = back_part(3, inner, False)
    for cc in (0, 1):
        for hh in (0, 1):
            for yy in (0, 1):
                at = (yy * 2 + cc) * 128
                block = sacc[at : at + 128, SL * hh : SL * hh + SL]
                pbuf[0, cc, 2 * hh + yy] = block.astype(bf16).reshape(8, 16, SL)
    core_s = core_step(0)
    expand_part(3, inner, back_proj)
    for cc in (0, 1):
        for hh in (0, 1):
            for yy in (0, 1):
                for xx in range(4):
                    at = ((yy * 4 + xx) * 2 + cc) * 64
                    for zz in range(8):
                        top_row, lane = at + zz // 2 * 16, (zz % 2 * 2 + hh) * 128
                        pbuf[1, cc, 2 * hh + yy, zz, :, 128 * xx : 128 * xx + 128] = eacc[
                            top_row : top_row + 16, lane : lane + 128
                        ].astype(bf16)
    core_e = core_step(1)
    ring_s = ring_start(0, core_s)
    norm_part(3, inner, False, back_proj)
    ring_e = ring_start(1, core_e)

    vector_copies = []
    for slot, xo in ((1, 3), (2, 1), (3, 2)):
        vector_copies.append(go(remote(sv.at[slot], svr.at[x], bs.at[xo - 1], br.at[xo - 1], x=xs[xo])))
    svr[x] = sv[0]
    whole = total[...]
    gp[...] = jnp.sum(whole * normed[...], axis=0, keepdims=True)
    gains = []
    for o in range(1, 16):
        yo, xo, co = o // 8, (o // 2) % 4, o % 2
        gains.append(go(remote(
            gp, gpr.at[chip * 2 + c], gs.at[o], gr.at[o], y=oy if yo else y, x=xs[xo], c=oc if co else c
        )))
    gpr[chip * 2 + c] = gp[...]
    unit = whole * gain[...]
    inner = jnp.mean(unit * normed[...], axis=1, keepdims=True)
    back_trunk = invs[:, :1] * (unit - jnp.mean(unit, axis=1, keepdims=True) - normed[...] * inner)
    term = (cots[0].astype(f32) + back_trunk).astype(bf16)
    t[0] = term[:CUT]
    t[1, : TOK - CUT] = term[CUT:]
    t[1, TOK - CUT :] = jnp.zeros((FULL - TOK, D), bf16)
    core_t = go(remote(t.at[oc], rt, as_.at[2], ar.at[2], c=oc))

    ring_pass(0, ring_s)
    ring_pass(1, ring_e)
    told(4, 3)
    deep_s = deep_start(0, ring_s)
    deep_e = deep_start(1, ring_e)

    core_t.wait_recv()
    joint = added(t[c], rt[...]).astype(bf16)
    for g in range(8):
        tq[g] = joint[:, 128 * g : 128 * g + 128]
    tiles = []
    for g in range(1, 8):
        yo, xo = g // 4, g % 4
        ty, tx = oy if yo else y, xs[xo]
        tiles.append(go(remote(tq.at[ty * 4 + tx], tr.at[chip], ts.at[g], tr_.at[g], y=ty, x=tx)))
    tr[chip] = tq[chip]

    for copy in vector_copies + gains:
        copy.wait_recv()
    sums = svr[0] + svr[1] + svr[2] + svr[3]
    gain_sum = gpr[0]
    for m in range(1, 16):
        gain_sum = gain_sum + gpr[m]
    zero = jnp.zeros((1, SL), f32)
    for i in range(4):
        dv[i] = sums[i : i + 1]
        dv[4 + i] = svr[i, 4:5]
        dv[8 + i] = svr[i, 5:6]
    dv[12] = gain_sum[:, :SL]
    dv[13] = gain_sum[:, SL:]
    dv[14] = zero
    dv[15] = zero
    small = []
    for o, where in peers:
        e = where["z"] * 2 + where["h"]
        small.append(go(remote(dv.at[e], dvr.at[me], ds.at[o], dr.at[o], **where)))
    dvr[me] = dv[me]

    outs = (sh, ex)

    def spread(i):
        copies = {}
        for o in (2, 6, 1, 7, 0):
            e = lax.rem(z + o, 8)
            for ho in (0, 1):
                if o or ho:
                    copies[o, ho] = go(remote(
                        res.at[i], outs[i].at[me], hs.at[i, o, ho], hr.at[i, o, ho],
                        z=e, h=1 - h if ho else h,
                    ))
        return copies

    def relay(i, copies):
        for o, further in ((2, (4, 3)), (6, (5,))):
            for ho in (0, 1):
                copies[o, ho].wait_recv()
                place = lax.rem(z + 8 - o, 8) * 2 + (1 - h if ho else h)
                for far_o in further:
                    copies[far_o, ho] = go(remote(
                        outs[i].at[place], outs[i].at[place], hs.at[i, far_o, ho], hr.at[i, far_o, ho],
                        z=lax.rem(z + far_o - o + 8, 8),
                    ))

    done = deep_sum(0, deep_s)
    spread_s = spread(0)
    sh[me] = done
    done = deep_sum(1, deep_e)
    spread_e = spread(1)
    ex[me] = done

    for copy in tiles:
        copy.wait_recv()
    tf[c] = added(*(tr[g] for g in range(8))).astype(bf16)
    finish = go(remote(tf.at[c], tf.at[c], fs, fr, c=oc))

    for copy in small:
        copy.wait_recv()
    line = dvr[0]
    for p in range(1, 16):
        line = line + dvr[p]
    dvs[...] = line
    lines = []
    for o, where in peers:
        lines.append(go(remote(dvs, dvo.at[me], os_.at[o], or_.at[o], **where)))
    dvo[me] = line

    relay(0, spread_s)
    relay(1, spread_e)

    for copy in [finish] + lines:
        copy.wait_recv()
    for copies in (spread_s, spread_e):
        for (o, ho), copy in copies.items():
            if o not in (2, 6):
                copy.wait_recv()

    for copy in sent:
        copy.wait_send()


def finish_kernel(tf, sh, ex, dvo, tg, eg, sg, ing, hg, ag, og, gg):
    c = lax.axis_index("c")
    turned = tf[...].reshape(FULL, 128).astype(f32).T
    tg[...] = jnp.where(c == 0, turned[:64], turned[64:])[:, :TOK].astype(bf16)
    for i in (0, 1):
        ing[:, SL * i : SL * i + SL] = dvo[i]
        og[:, SL * i : SL * i + SL] = dvo[2 + i]
        gg[:, SL * i : SL * i + SL] = dvo[12 + i]
        for xx in range(4):
            at = 1024 * i + 256 * xx
            hg[:, at : at + 256] = dvo[4 + xx][:, 256 * i : 256 * i + 256]
            ag[:, at : at + 256] = dvo[8 + xx][:, 256 * i : 256 * i + 256]
    for p in range(16):
        low, lane = p // 4 * 16, p % 4 // 2 * 1024 + p % 2 * 128
        for xx in range(4):
            at = lane + 256 * xx
            eg[low : low + 16, at : at + 128] = ex[p, :, 128 * xx : 128 * xx + 128].astype(f32)
        sg[16 * (p // 2) : 16 * (p // 2) + 16, SL * (p % 2) : SL * (p % 2) + SL] = sh[p].astype(f32)


def vmem(n):
    return [pl.BlockSpec(memory_space=pltpu.VMEM)] * n


def dma(*shape):
    return pltpu.SemaphoreType.DMA(shape)


def body(trunk, normgain, expand, shrink, inscale, hidscale, actscale, outscale, cotangent):
    S = jax.ShapeDtypeStruct
    V = pltpu.VMEM
    parts = pl.pallas_call(
        kernel,
        out_shape=[
            S((2, CUT, 128), bf16),
            S((16, 16, SL), bf16),
            S((16, 16, SL), bf16),
            S((16, 1, SL), f32),
        ],
        in_specs=[pl.BlockSpec(memory_space=pl.ANY)] * 9,
        out_specs=vmem(4),
        scratch_shapes=[
            V((1, D), f32),
            V((1, D), f32),
            V((1, FF), f32),
            V((1, FF), f32),
            V((1, D), f32),
            V((TOK, D), bf16),
            V((4, 8, SL), f32),
            V((TOK, D), f32),
            V((TOK, D), f32),
            V((TOK, 128), f32),
            V((4, TOK, D), bf16),
            V((2, 4, 2, 64, SL), bf16),
            V((2, 2, 128, D), bf16),
            V((4, 8, SL), f32),
            V((4, TOK, D), bf16),
            V((4, TOK, SL), bf16),
            V((4, TOK, SL), f32),
            V((4, TOK, SL), f32),
            V((4, TOK, SL), f32),
            V((TOK, D), f32),
            V((SL, D), f32),
            V((D, SL), f32),
            V((2, 2, 4, 8, 16, SL), bf16),
            V((2, 4, 8, 16, SL), bf16),
            V((2, CUT, D), bf16),
            V((CUT, D), bf16),
            V((2, 4, 8, 16, SL), bf16),
            V((2, 6, 4, 16, SL), bf16),
            V((2, 2, 4, 16, SL), bf16),
            V((2, 8, 16, SL), bf16),
            V((2, 8, 16, SL), bf16),
            V((2, 16, SL), bf16),
            V((8, CUT, 128), bf16),
            V((8, CUT, 128), bf16),
            V((4, 8, SL), f32),
            V((4, 8, SL), f32),
            V((1, D), f32),
            V((16, 1, D), f32),
            V((16, 1, SL), f32),
            V((16, 1, SL), f32),
            V((1, SL), f32),
            dma(10), dma(10), dma(4, 4), dma(3, 2), dma(3, 2), dma(3), dma(3), dma(3), dma(3), dma(3), dma(3),
            dma(3), dma(3), dma(2, 6), dma(2, 6), dma(5, 8), dma(5, 8), dma(2, 8, 2), dma(2, 8, 2),
            dma(8), dma(8), pltpu.SemaphoreType.DMA, pltpu.SemaphoreType.DMA, dma(3), dma(3), dma(16), dma(16),
            dma(16), dma(16), dma(16), dma(16), pltpu.SemaphoreType.REGULAR((5,)),
        ],
        compiler_params=pltpu.CompilerParams(
            collective_id=0, has_side_effects=True, vmem_limit_bytes=60 * 1024 * 1024
        ),
        name="exchange_compute",
    )(
        trunk, expand, shrink, cotangent, normgain.reshape(1, D), inscale, hidscale, actscale, outscale
    )
    tg, eg, sg, ing, hg, ag, og, gg = pl.pallas_call(
        finish_kernel,
        out_shape=[
            S((64, TOK), bf16),
            S((64, FF), f32),
            S((128, D), f32),
            S((1, D), f32),
            S((1, FF), f32),
            S((1, FF), f32),
            S((1, D), f32),
            S((1, D), f32),
        ],
        in_specs=vmem(4),
        out_specs=vmem(8),
        name="write_outputs",
    )(*parts)
    return tg.T, eg, sg, ing, hg, ag, og, gg.reshape(D)


def solution(mesh):
    finer = Mesh(mesh.devices.reshape(2, 4, 2, 8, 2), AXES)
    rows = P(MEMBER, None)
    in_specs = (P(DP, None), P(), rows, rows, rows, rows, rows, rows, P(MEMBER, DP, None))
    out_specs = (P(DP, MEMBER), rows, rows, rows, rows, rows, rows, P())
    return jax.shard_map(body, mesh=finer, in_specs=in_specs, out_specs=out_specs, check_vma=False)
```

```python
import jax
import jax.numpy as jnp
from jax import lax
from jax.experimental import pallas as pl
from jax.experimental.pallas import tpu as pltpu
from jax.sharding import Mesh
from jax.sharding import PartitionSpec as P

AXES = ("y", "x", "c", "z", "h")
MEMBER = ("y", "x", "c")
DP = ("z", "h")
TOK = 394
CUT = 208
EDGE = 96
SEAM = 192
EDGE2 = 288
PIECES = ((0, EDGE), (EDGE2, TOK), (EDGE, SEAM), (SEAM, EDGE2))
FULL = 416
D = 1024
FF = 2048
SL = 512

eps = 1e-06
coeff = 0.7978845608028654
f32 = jnp.float32
bf16 = jnp.bfloat16
MESH = pl.DeviceIdType.MESH


def remote(src, dst, send, recv, **where):
    return pltpu.make_async_remote_copy(
        src_ref=src, dst_ref=dst, send_sem=send, recv_sem=recv, device_id=where, device_id_type=MESH
    )


def greet(barrier, **where):
    pl.semaphore_signal(barrier, inc=1, device_id=where, device_id_type=MESH)


def gelu_pair(hidden):
    inner = coeff * (hidden + 0.044715 * hidden * hidden * hidden)
    tangent = jnp.tanh(inner)
    active = 0.5 * hidden * (1.0 + tangent)
    slope = 0.5 * (1.0 + tangent) + 0.5 * hidden * (1.0 - tangent * tangent) * coeff * (
        1.0 + 3.0 * 0.044715 * hidden * hidden
    )
    return active, slope


def dot(a, b, ca, cb):
    return lax.dot_general(a, b, (((ca,), (cb,)), ((), ())), preferred_element_type=f32)


def row(v, i):
    return jnp.concatenate([v[i : i + 1], v[i + 1 : i + 2]], axis=1)


def added(*refs):
    total = refs[0].astype(f32)
    for r in refs[1:]:
        total = total + r.astype(f32)
    return total


def kernel(
    trunk, exp, shr, cot, gain_in, in_in, hid_in, act_in, out_in,
    tf, sh, ex, dvo,
    gain, inscale, hidscale, actscale, outscale, tbuf, vec, normed, gained, invs, cots, w1, w2, vecs, si, act, pa, actf, proj, total, sacc, eacc,
    pbuf, rbuf, t, rt, q, yb, mix, r, rz, res, tq, tr, sv, svr, gp, gpr, dv, dvr, dvs,
    ls, cs, cr, ws, wr, vs, vr, ss, sr, es, er,
    as_, ar, ys, yr, zs, zr, hs, hr, ts, tr_, fs, fr, bs, br, gs, gr, ds, dr, os_, or_, heard,
):
    y, x, c, z, h = (lax.axis_index(a) for a in AXES)
    xs = [lax.rem(x + o, 4) for o in range(4)]
    oy, oc = 1 - y, 1 - c
    me = z * 2 + h
    chip = y * 4 + x
    place = h * 2 + y
    sent = []

    def go(copy):
        copy.start()
        sent.append(copy)
        return copy

    barrier = pltpu.get_barrier_semaphore()

    for yo in (0, 1):
        for co in (0, 1):
            for xo in range(4):
                if yo or co or xo:
                    greet(barrier, y=oy if yo else y, x=xs[xo], c=oc if co else c)
    greet(barrier, y=oy, h=1 - h)
    greet(barrier, h=1 - h)
    above, below = lax.rem(z + 1, 8), lax.rem(z + 7, 8)
    greet(barrier, z=above)
    greet(barrier, z=below)

    def tell_z(i):
        greet(heard.at[i], z=above)
        greet(heard.at[i], z=below)

    def told(i, n):
        pl.semaphore_wait(heard.at[i], n)

    here = [
        pltpu.make_async_copy(trunk, tbuf, ls.at[0]),
        pltpu.make_async_copy(shr, w2.at[y, c], ls.at[1]),
        pltpu.make_async_copy(cot.at[0], cots.at[0], ls.at[2]),
    ]
    for half in (0, 1):
        here.append(
            pltpu.make_async_copy(
                exp.at[:, pl.ds(pl.multiple_of(1024 * half + 256 * x, 256), 256)],
                w1.at[y, x, c, :, pl.ds(256 * half, 256)],
                ls.at[3 + half],
            )
        )
    lines = []
    for i, (src, dst) in enumerate(
        ((in_in, inscale), (hid_in, hidscale), (act_in, actscale), (out_in, outscale), (gain_in, gain))
    ):
        lines.append(pltpu.make_async_copy(src, dst, ls.at[5 + i]))
    for copy in lines + here:
        copy.start()
    pl.semaphore_wait(barrier, 19)
    tell_z(0)

    slot_of = {1: 1, 3: 2, 2: 3}
    vec_copies, exp_copies = {}, {}
    for o in (1, 3, 2):
        for half in (0, 1):
            exp_copies[o, half] = go(remote(
                exp.at[:, pl.ds(pl.multiple_of(1024 * half + 256 * xs[o], 256), 256)],
                w1.at[y, x, c, :, pl.ds(256 * half, 256)],
                ws.at[o - 1, half], wr.at[o - 1, half], x=xs[o],
            ))
    shr_y = go(remote(shr, w2.at[y, c], ss.at[0], sr.at[0], y=oy))
    shr_c = go(remote(shr, w2.at[y, c], ss.at[1], sr.at[1], c=oc))
    for copy in lines:
        copy.wait()
    for xx in range(4):
        for i in (0, 1):
            vec[xx, i : i + 1] = inscale[:, SL * i : SL * i + SL]
            vec[xx, 2 + i : 3 + i] = outscale[:, SL * i : SL * i + SL]
            at = 1024 * i + 256 * xx
            vec[xx, 4:5, 256 * i : 256 * i + 256] = hidscale[:, at : at + 256]
            vec[xx, 5:6, 256 * i : 256 * i + 256] = actscale[:, at : at + 256]
        vec[xx, 6:8] = jnp.zeros((2, SL), f32)
    for o in (1, 3, 2):
        vec_copies[o] = go(remote(
            vec.at[xs[o]], vecs.at[slot_of[o]], vs.at[o - 1], vr.at[o - 1], x=xs[o]
        ))
    right_own, left_own = [], []
    for i, (lo, hi) in enumerate(((0, EDGE), (EDGE, SEAM), (SEAM, TOK))):
        piece = pl.ds(lo, hi - lo)
        right_own.append(remote(cot.at[0, piece], cots.at[1, piece], cs.at[i], cr.at[1, i], x=xs[1]))
    for i, (lo, hi) in enumerate(((EDGE2, TOK), (SEAM, EDGE2), (0, SEAM))):
        piece = pl.ds(lo, hi - lo)
        left_own.append(remote(cot.at[0, piece], cots.at[2, piece], cs.at[3 + i], cr.at[2, i], x=xs[3]))
    for i in range(3):
        go(right_own[i])
        go(left_own[i])

    vecs[0] = vec[x]
    here[0].wait()
    tokens = tbuf[...].astype(f32)
    centered = tokens - jnp.mean(tokens, axis=1, keepdims=True)
    variance = jnp.mean(centered * centered, axis=1, keepdims=True)
    inv = lax.rsqrt(variance + eps)
    normed[...] = centered * inv
    gained[...] = centered * inv * gain[...]
    invs[...] = jnp.broadcast_to(inv, invs.shape)
    total[...] = jnp.zeros_like(total)
    sacc[...] = jnp.zeros_like(sacc)
    eacc[...] = jnp.zeros_like(eacc)
    for copy in here[1:]:
        copy.wait()

    for o in (1, 3, 2):
        exp_copies[o, 0].wait_recv()
        exp_copies[o, 1].wait_recv()
    exp_y = go(remote(w1.at[y, :, c], w1.at[y, :, c], es.at[0], er.at[0], y=oy))
    exp_c = go(remote(w1.at[y, :, c], w1.at[y, :, c], es.at[1], er.at[1], c=oc))
    shr_y.wait_recv()
    shr_f = go(remote(w2.at[oy, c], w2.at[oy, c], ss.at[2], sr.at[2], c=oc))
    for o in (1, 3, 2):
        vec_copies[o].wait_recv()

    @pl.loop(0, 4)
    def _(k):
        si[k] = (gained[...] * row(vecs[k], 0)).astype(bf16)

    fwd = []
    for i, (lo, hi) in enumerate(PIECES):
        (right_own, left_own)[i % 2][i // 2].wait_recv()
        src, to = ((1, xs[1]), (2, xs[3]))[i % 2]
        piece = pl.ds(lo, hi - lo)
        fwd.append(go(remote(cots.at[src, piece], cots.at[3, piece], cs.at[6 + i], cr.at[3, i], x=to)))
    exp_y.wait_recv()
    exp_f = go(remote(w1.at[oy, :, c], w1.at[oy, :, c], es.at[2], er.at[2], c=oc))
    for copy in (shr_c, exp_c, shr_f, exp_f):
        copy.wait_recv()
    told(0, 2)
    tell_z(1)

    @pl.loop(0, 4)
    def _(k):
        v = vecs[k]
        project = dot(si[k], w1[...].reshape(D, SL), 1, 0)
        active, slope = gelu_pair(project * v[4:5])
        proj[k] = project
        actf[k] = active
        act[k] = (active * v[5:6]).astype(bf16)
        pa[k] = slope * v[5:6]

    told(1, 2)
    tell_z(2)

    def take(ref, k, rows):
        blocks = [ref[k, lo:hi] for lo, hi in rows]
        return blocks[0] if len(blocks) == 1 else jnp.concatenate(blocks, axis=0)

    def back_part(k, rows, first):
        v = vecs[k]
        scale_out = row(v, 2)
        second = w2[...].reshape(SL, D)
        seed = take(cots, k, rows)
        scaled_cot = (seed.astype(f32) * scale_out).astype(bf16)
        back = dot(scaled_cot, second, 1, 1)
        grad_act = jnp.sum(back * take(actf, k, rows), axis=0, keepdims=True)
        back_hidden = back * take(pa, k, rows)
        grad_hid = jnp.sum(back_hidden * take(proj, k, rows), axis=0, keepdims=True)
        back_proj = (back_hidden * v[4:5]).astype(bf16)
        both = dot(take(act, k, rows), seed, 0, 0)
        sacc[...] += both * scale_out
        grad_out = jnp.sum(second.astype(f32) * both, axis=0, keepdims=True)
        zero = jnp.zeros((2, SL), f32)
        lines = jnp.concatenate([grad_out[:, :SL], grad_out[:, SL:], grad_hid, grad_act, zero], axis=0)
        sv[k, 2:8] = lines if first else sv[k, 2:8] + lines
        return back_proj

    def expand_part(k, rows, back_proj):
        eacc[...] += dot(take(si, k, rows), back_proj, 0, 0)

    def norm_part(k, rows, first, back_proj):
        back_norm = dot(back_proj, w1[...].reshape(D, SL), 1, 1)
        share = back_norm * row(vecs[k], 0)
        grad_in = 0.0
        at = 0
        for lo, hi in rows:
            end = at + hi - lo
            grad_in = grad_in + jnp.sum(back_norm[at:end] * gained[lo:hi], axis=0, keepdims=True)
            total[lo:hi] += share[at:end]
            at = end
        lines = jnp.concatenate([grad_in[:, :SL], grad_in[:, SL:]], axis=0)
        sv[k, 0:2] = lines if first else sv[k, 0:2] + lines

    @pl.loop(0, 3)
    def _(k):
        @pl.when(k == 1)
        def _():
            right_own[2].wait_recv()

        @pl.when(k == 2)
        def _():
            left_own[2].wait_recv()

        every = ((0, TOK),)
        back_proj = back_part(k, every, True)
        expand_part(k, every, back_proj)
        norm_part(k, every, True, back_proj)

    right, left, far = (lax.rem(place + o, 4) for o in (1, 3, 2))
    to_right = dict(y=lax.rem(right, 2), h=right // 2)
    to_left = dict(y=lax.rem(left, 2), h=left // 2)
    top, low = pl.ds(0, 4), pl.ds(4, 4)

    def core_step(i):
        return go(remote(pbuf.at[i, oc], rbuf.at[i], as_.at[i], ar.at[i], c=oc))

    def ring_start(i, copy):
        copy.wait_recv()
        q[i] = added(pbuf[i, c], rbuf[i]).astype(bf16)
        return [
            go(remote(q.at[i, far, top], yb.at[i, 0], ys.at[i, 0], yr.at[i, 0], **to_right)),
            go(remote(q.at[i, far, low], yb.at[i, 1], ys.at[i, 1], yr.at[i, 1], **to_left)),
            go(remote(q.at[i, right, low], yb.at[i, 2], ys.at[i, 2], yr.at[i, 2], **to_right)),
            go(remote(q.at[i, left, top], yb.at[i, 3], ys.at[i, 3], yr.at[i, 3], **to_left)),
        ]

    def ring_pass(i, copies):
        copies[0].wait_recv()
        mix[i, 0] = added(q[i, right, 0:4], yb[i, 0]).astype(bf16)
        copies.append(go(remote(mix.at[i, 0], yb.at[i, 4], ys.at[i, 4], yr.at[i, 4], **to_right)))
        copies[1].wait_recv()
        mix[i, 1] = added(q[i, left, 4:8], yb[i, 1]).astype(bf16)
        copies.append(go(remote(mix.at[i, 1], yb.at[i, 5], ys.at[i, 5], yr.at[i, 5], **to_left)))

    def deep_start(i, copies):
        for copy in copies[2:]:
            copy.wait_recv()
        r[i, 0:4] = added(q[i, place, 0:4], yb[i, 3], yb[i, 4]).astype(bf16)
        r[i, 4:8] = added(q[i, place, 4:8], yb[i, 2], yb[i, 5]).astype(bf16)
        out = []
        if i == 0:
            for o in (4, 3, 5, 2, 6, 1, 7):
                e = lax.rem(z + o, 8)
                out.append(go(remote(r.at[0, e], rz.at[0, z], zs.at[0, o], zr.at[0, o], z=e)))
            rz[0, z] = r[0, z]
            return out
        mine = pl.ds(pl.multiple_of(128 * x, 128), 128)
        for o in (4, 3, 5, 2, 6, 1, 7, 0):
            e = lax.rem(z + o, 8)
            for xo in range(4):
                if o or xo:
                    block = pl.ds(pl.multiple_of(128 * xs[xo], 128), 128)
                    out.append(go(remote(
                        r.at[1, e, :, block], rz.at[1, z, :, mine], zs.at[1 + xo, o], zr.at[1 + xo, o],
                        z=e, x=xs[xo],
                    )))
        rz[1, z, :, mine] = r[1, z, :, mine]
        return out

    def deep_sum(i, copies):
        for copy in copies:
            copy.wait_recv()
        done = added(*(rz[i, e] for e in range(8))).astype(bf16)
        res[i] = done
        return done

    peers = []
    for o in range(1, 16):
        e = lax.rem(me + o, 16)
        peers.append((o, dict(z=e // 2, h=lax.rem(e, 2))))

    told(2, 2)
    greet(heard.at[3], h=1 - h)
    fwd[0].wait_recv()
    fwd[1].wait_recv()
    outer, inner = ((0, EDGE), (EDGE2, TOK)), ((EDGE, EDGE2),)
    back_proj = back_part(3, outer, True)
    expand_part(3, outer, back_proj)
    norm_part(3, outer, True, back_proj)
    told(3, 1)
    for o in (1, 2, 3):
        greet(heard.at[4], x=xs[o])
    fwd[2].wait_recv()
    fwd[3].wait_recv()
    back_proj = back_part(3, inner, False)
    for cc in (0, 1):
        for hh in (0, 1):
            for yy in (0, 1):
                at = (yy * 2 + cc) * 128
                block = sacc[at : at + 128, SL * hh : SL * hh + SL]
                pbuf[0, cc, 2 * hh + yy] = block.astype(bf16).reshape(8, 16, SL)
    core_s = core_step(0)
    expand_part(3, inner, back_proj)
    for cc in (0, 1):
        for hh in (0, 1):
            for yy in (0, 1):
                for xx in range(4):
                    at = ((yy * 4 + xx) * 2 + cc) * 64
                    for zz in range(8):
                        top_row, lane = at + zz // 2 * 16, (zz % 2 * 2 + hh) * 128
                        pbuf[1, cc, 2 * hh + yy, zz, :, 128 * xx : 128 * xx + 128] = eacc[
                            top_row : top_row + 16, lane : lane + 128
                        ].astype(bf16)
    core_e = core_step(1)
    ring_s = ring_start(0, core_s)
    norm_part(3, inner, False, back_proj)
    ring_e = ring_start(1, core_e)

    vector_copies = []
    for slot, xo in ((1, 3), (2, 1), (3, 2)):
        vector_copies.append(go(remote(sv.at[slot], svr.at[x], bs.at[xo - 1], br.at[xo - 1], x=xs[xo])))
    svr[x] = sv[0]
    whole = total[...]
    gp[...] = jnp.sum(whole * normed[...], axis=0, keepdims=True)
    gains = []
    for o in range(1, 16):
        yo, xo, co = o // 8, (o // 2) % 4, o % 2
        gains.append(go(remote(
            gp, gpr.at[chip * 2 + c], gs.at[o], gr.at[o], y=oy if yo else y, x=xs[xo], c=oc if co else c
        )))
    gpr[chip * 2 + c] = gp[...]
    unit = whole * gain[...]
    inner = jnp.mean(unit * normed[...], axis=1, keepdims=True)
    back_trunk = invs[:, :1] * (unit - jnp.mean(unit, axis=1, keepdims=True) - normed[...] * inner)
    term = (cots[0].astype(f32) + back_trunk).astype(bf16)
    t[0] = term[:CUT]
    t[1, : TOK - CUT] = term[CUT:]
    t[1, TOK - CUT :] = jnp.zeros((FULL - TOK, D), bf16)
    core_t = go(remote(t.at[oc], rt, as_.at[2], ar.at[2], c=oc))

    ring_pass(0, ring_s)
    ring_pass(1, ring_e)
    told(4, 3)
    deep_s = deep_start(0, ring_s)
    deep_e = deep_start(1, ring_e)

    core_t.wait_recv()
    joint = added(t[c], rt[...]).astype(bf16)
    for g in range(8):
        tq[g] = joint[:, 128 * g : 128 * g + 128]
    tiles = []
    for g in range(1, 8):
        yo, xo = g // 4, g % 4
        ty, tx = oy if yo else y, xs[xo]
        tiles.append(go(remote(tq.at[ty * 4 + tx], tr.at[chip], ts.at[g], tr_.at[g], y=ty, x=tx)))
    tr[chip] = tq[chip]

    for copy in vector_copies + gains:
        copy.wait_recv()
    sums = svr[0] + svr[1] + svr[2] + svr[3]
    gain_sum = gpr[0]
    for m in range(1, 16):
        gain_sum = gain_sum + gpr[m]
    zero = jnp.zeros((1, SL), f32)
    for i in range(4):
        dv[i] = sums[i : i + 1]
        dv[4 + i] = svr[i, 4:5]
        dv[8 + i] = svr[i, 5:6]
    dv[12] = gain_sum[:, :SL]
    dv[13] = gain_sum[:, SL:]
    dv[14] = zero
    dv[15] = zero
    small = []
    for o, where in peers:
        e = where["z"] * 2 + where["h"]
        small.append(go(remote(dv.at[e], dvr.at[me], ds.at[o], dr.at[o], **where)))
    dvr[me] = dv[me]

    outs = (sh, ex)

    def spread(i):
        copies = {}
        for o in (2, 6, 1, 7, 0):
            e = lax.rem(z + o, 8)
            for ho in (0, 1):
                if o or ho:
                    copies[o, ho] = go(remote(
                        res.at[i], outs[i].at[me], hs.at[i, o, ho], hr.at[i, o, ho],
                        z=e, h=1 - h if ho else h,
                    ))
        return copies

    def relay(i, copies):
        for o, further in ((2, (4, 3)), (6, (5,))):
            for ho in (0, 1):
                copies[o, ho].wait_recv()
                place = lax.rem(z + 8 - o, 8) * 2 + (1 - h if ho else h)
                for far_o in further:
                    copies[far_o, ho] = go(remote(
                        outs[i].at[place], outs[i].at[place], hs.at[i, far_o, ho], hr.at[i, far_o, ho],
                        z=lax.rem(z + far_o - o + 8, 8),
                    ))

    done = deep_sum(0, deep_s)
    spread_s = spread(0)
    sh[me] = done
    done = deep_sum(1, deep_e)
    spread_e = spread(1)
    ex[me] = done

    for copy in tiles:
        copy.wait_recv()
    tf[c] = added(*(tr[g] for g in range(8))).astype(bf16)
    finish = go(remote(tf.at[c], tf.at[c], fs, fr, c=oc))

    for copy in small:
        copy.wait_recv()
    line = dvr[0]
    for p in range(1, 16):
        line = line + dvr[p]
    dvs[...] = line
    lines = []
    for o, where in peers:
        lines.append(go(remote(dvs, dvo.at[me], os_.at[o], or_.at[o], **where)))
    dvo[me] = line

    relay(0, spread_s)
    relay(1, spread_e)

    for copy in [finish] + lines:
        copy.wait_recv()
    for copies in (spread_s, spread_e):
        for (o, ho), copy in copies.items():
            if o not in (2, 6):
                copy.wait_recv()

    for copy in sent:
        copy.wait_send()


def finish_kernel(tf, sh, ex, dvo, tg, eg, sg, ing, hg, ag, og, gg):
    c = lax.axis_index("c")
    turned = tf[...].reshape(FULL, 128).astype(f32).T
    tg[...] = jnp.where(c == 0, turned[:64], turned[64:])[:, :TOK].astype(bf16)
    for i in (0, 1):
        ing[:, SL * i : SL * i + SL] = dvo[i]
        og[:, SL * i : SL * i + SL] = dvo[2 + i]
        gg[:, SL * i : SL * i + SL] = dvo[12 + i]
        for xx in range(4):
            at = 1024 * i + 256 * xx
            hg[:, at : at + 256] = dvo[4 + xx][:, 256 * i : 256 * i + 256]
            ag[:, at : at + 256] = dvo[8 + xx][:, 256 * i : 256 * i + 256]
    for p in range(16):
        low, lane = p // 4 * 16, p % 4 // 2 * 1024 + p % 2 * 128
        for xx in range(4):
            at = lane + 256 * xx
            eg[low : low + 16, at : at + 128] = ex[p, :, 128 * xx : 128 * xx + 128].astype(f32)
        sg[16 * (p // 2) : 16 * (p // 2) + 16, SL * (p % 2) : SL * (p % 2) + SL] = sh[p].astype(f32)


def vmem(n):
    return [pl.BlockSpec(memory_space=pltpu.VMEM)] * n


def dma(*shape):
    return pltpu.SemaphoreType.DMA(shape)


def body(trunk, normgain, expand, shrink, inscale, hidscale, actscale, outscale, cotangent):
    S = jax.ShapeDtypeStruct
    V = pltpu.VMEM
    parts = pl.pallas_call(
        kernel,
        out_shape=[
            V((2, CUT, 128), bf16),
            V((16, 16, SL), bf16),
            V((16, 16, SL), bf16),
            V((16, 1, SL), f32),
        ],
        in_specs=[pl.BlockSpec(memory_space=pl.ANY)] * 9,
        out_specs=vmem(4),
        scratch_shapes=[
            V((1, D), f32),
            V((1, D), f32),
            V((1, FF), f32),
            V((1, FF), f32),
            V((1, D), f32),
            V((TOK, D), bf16),
            V((4, 8, SL), f32),
            V((TOK, D), f32),
            V((TOK, D), f32),
            V((TOK, 128), f32),
            V((4, TOK, D), bf16),
            V((2, 4, 2, 64, SL), bf16),
            V((2, 2, 128, D), bf16),
            V((4, 8, SL), f32),
            V((4, TOK, D), bf16),
            V((4, TOK, SL), bf16),
            V((4, TOK, SL), f32),
            V((4, TOK, SL), f32),
            V((4, TOK, SL), f32),
            V((TOK, D), f32),
            V((SL, D), f32),
            V((D, SL), f32),
            V((2, 2, 4, 8, 16, SL), bf16),
            V((2, 4, 8, 16, SL), bf16),
            V((2, CUT, D), bf16),
            V((CUT, D), bf16),
            V((2, 4, 8, 16, SL), bf16),
            V((2, 6, 4, 16, SL), bf16),
            V((2, 2, 4, 16, SL), bf16),
            V((2, 8, 16, SL), bf16),
            V((2, 8, 16, SL), bf16),
            V((2, 16, SL), bf16),
            V((8, CUT, 128), bf16),
            V((8, CUT, 128), bf16),
            V((4, 8, SL), f32),
            V((4, 8, SL), f32),
            V((1, D), f32),
            V((16, 1, D), f32),
            V((16, 1, SL), f32),
            V((16, 1, SL), f32),
            V((1, SL), f32),
            dma(10), dma(10), dma(4, 4), dma(3, 2), dma(3, 2), dma(3), dma(3), dma(3), dma(3), dma(3), dma(3),
            dma(3), dma(3), dma(2, 6), dma(2, 6), dma(5, 8), dma(5, 8), dma(2, 8, 2), dma(2, 8, 2),
            dma(8), dma(8), pltpu.SemaphoreType.DMA, pltpu.SemaphoreType.DMA, dma(3), dma(3), dma(16), dma(16),
            dma(16), dma(16), dma(16), dma(16), pltpu.SemaphoreType.REGULAR((5,)),
        ],
        compiler_params=pltpu.CompilerParams(
            collective_id=0, has_side_effects=True, vmem_limit_bytes=60 * 1024 * 1024
        ),
        name="exchange_compute",
    )(
        trunk, expand, shrink, cotangent, normgain.reshape(1, D), inscale, hidscale, actscale, outscale
    )
    tg, eg, sg, ing, hg, ag, og, gg = pl.pallas_call(
        finish_kernel,
        out_shape=[
            S((64, TOK), bf16),
            S((64, FF), f32),
            S((128, D), f32),
            S((1, D), f32),
            S((1, FF), f32),
            S((1, FF), f32),
            S((1, D), f32),
            S((1, D), f32),
        ],
        in_specs=vmem(4),
        out_specs=vmem(8),
        name="write_outputs",
    )(*(pltpu.with_memory_space_constraint(part, pltpu.VMEM) for part in parts))
    return tg.T, eg, sg, ing, hg, ag, og, gg.reshape(D)


def solution(mesh):
    finer = Mesh(mesh.devices.reshape(2, 4, 2, 8, 2), AXES)
    rows = P(MEMBER, None)
    in_specs = (P(DP, None), P(), rows, rows, rows, rows, rows, rows, P(MEMBER, DP, None))
    out_specs = (P(DP, MEMBER), rows, rows, rows, rows, rows, rows, P())
    return jax.shard_map(body, mesh=finer, in_specs=in_specs, out_specs=out_specs, check_vma=False)
```

```python
import jax
import jax.numpy as jnp
from jax import lax
from jax.experimental import pallas as pl
from jax.experimental.pallas import tpu as pltpu
from jax.sharding import Mesh
from jax.sharding import PartitionSpec as P

AXES = ("y", "x", "c", "z", "h")
MEMBER = ("y", "x", "c")
DP = ("z", "h")
TOK = 394
CUT = 208
HALF = 256
PIECES = (0, 512, 256, 768)
FULL = 416
D = 1024
FF = 2048
SL = 512
ITEMS = ((0, 0, HALF), (0, HALF, SL), (1, 0, SL))

eps = 1e-06
coeff = 0.7978845608028654
f32 = jnp.float32
bf16 = jnp.bfloat16
MESH = pl.DeviceIdType.MESH


def remote(src, dst, send, recv, **where):
    return pltpu.make_async_remote_copy(
        src_ref=src, dst_ref=dst, send_sem=send, recv_sem=recv, device_id=where, device_id_type=MESH
    )


def greet(barrier, **where):
    pl.semaphore_signal(barrier, inc=1, device_id=where, device_id_type=MESH)


def gelu_pair(hidden):
    inner = coeff * (hidden + 0.044715 * hidden * hidden * hidden)
    tangent = jnp.tanh(inner)
    active = 0.5 * hidden * (1.0 + tangent)
    slope = 0.5 * (1.0 + tangent) + 0.5 * hidden * (1.0 - tangent * tangent) * coeff * (
        1.0 + 3.0 * 0.044715 * hidden * hidden
    )
    return active, slope


def dot(a, b, ca, cb):
    return lax.dot_general(a, b, (((ca,), (cb,)), ((), ())), preferred_element_type=f32)


def row(v, i):
    return jnp.concatenate([v[i : i + 1], v[i + 1 : i + 2]], axis=1)


def added(*refs):
    total = refs[0].astype(f32)
    for r in refs[1:]:
        total = total + r.astype(f32)
    return total


def kernel(
    trunk, exp, shr, cot, gain_in, in_in, hid_in, act_in, out_in,
    tf, sh, ex, dvo,
    gain, inscale, hidscale, actscale, outscale, tbuf, vec, normed, gained, invs, cots, w1, w2, vecs, si, act, pa, actf, proj, total, sacc, eacc, half_back,
    pbuf, rbuf, t, rt, q, yb, mix, r, rz, res, tq, tr, sv, svr, gp, gpr, dv, dvr, dvs,
    ls, cs, cr, ws, wr, vs, vr, ss, sr, es, er,
    as_, ar, ys, yr, zs, zr, hs, hr, ts, tr_, fs, fr, bs, br, gs, gr, ds, dr, os_, or_, heard,
):
    y, x, c, z, h = (lax.axis_index(a) for a in AXES)
    xs = [lax.rem(x + o, 4) for o in range(4)]
    oy, oc = 1 - y, 1 - c
    me = z * 2 + h
    chip = y * 4 + x
    place = h * 2 + y
    sent = []

    def go(copy):
        copy.start()
        sent.append(copy)
        return copy

    barrier = pltpu.get_barrier_semaphore()

    for yo in (0, 1):
        for co in (0, 1):
            for xo in range(4):
                if yo or co or xo:
                    greet(barrier, y=oy if yo else y, x=xs[xo], c=oc if co else c)
    greet(barrier, y=oy, h=1 - h)
    greet(barrier, h=1 - h)
    above, below = lax.rem(z + 1, 8), lax.rem(z + 7, 8)
    greet(barrier, z=above)
    greet(barrier, z=below)

    def tell_z(i):
        greet(heard.at[i], z=above)
        greet(heard.at[i], z=below)

    def told(i, n):
        pl.semaphore_wait(heard.at[i], n)

    here = [
        pltpu.make_async_copy(trunk, tbuf, ls.at[0]),
        pltpu.make_async_copy(shr, w2.at[y, c], ls.at[1]),
        pltpu.make_async_copy(cot.at[0], cots.at[0], ls.at[2]),
    ]
    for half in (0, 1):
        here.append(
            pltpu.make_async_copy(
                exp.at[:, pl.ds(pl.multiple_of(1024 * half + 256 * x, 256), 256)],
                w1.at[y, x, c, :, pl.ds(256 * half, 256)],
                ls.at[3 + half],
            )
        )
    lines = []
    for i, (src, dst) in enumerate(
        ((in_in, inscale), (hid_in, hidscale), (act_in, actscale), (out_in, outscale), (gain_in, gain))
    ):
        lines.append(pltpu.make_async_copy(src, dst, ls.at[5 + i]))
    for copy in lines + here:
        copy.start()
    pl.semaphore_wait(barrier, 19)
    tell_z(0)

    slot_of = {1: 1, 3: 2, 2: 3}
    vec_copies, exp_copies = {}, {}
    for o in (1, 3, 2):
        for half in (0, 1):
            exp_copies[o, half] = go(remote(
                exp.at[:, pl.ds(pl.multiple_of(1024 * half + 256 * xs[o], 256), 256)],
                w1.at[y, x, c, :, pl.ds(256 * half, 256)],
                ws.at[o - 1, half], wr.at[o - 1, half], x=xs[o],
            ))
    shr_y = go(remote(shr, w2.at[y, c], ss.at[0], sr.at[0], y=oy))
    shr_c = go(remote(shr, w2.at[y, c], ss.at[1], sr.at[1], c=oc))
    for copy in lines:
        copy.wait()
    for xx in range(4):
        for i in (0, 1):
            vec[xx, i : i + 1] = inscale[:, SL * i : SL * i + SL]
            vec[xx, 2 + i : 3 + i] = outscale[:, SL * i : SL * i + SL]
            at = 1024 * i + 256 * xx
            vec[xx, 4:5, 256 * i : 256 * i + 256] = hidscale[:, at : at + 256]
            vec[xx, 5:6, 256 * i : 256 * i + 256] = actscale[:, at : at + 256]
        vec[xx, 6:8] = jnp.zeros((2, SL), f32)
    for o in (1, 3, 2):
        vec_copies[o] = go(remote(
            vec.at[xs[o]], vecs.at[slot_of[o]], vs.at[o - 1], vr.at[o - 1], x=xs[o]
        ))
    right_own, left_own = [], []
    for i, (lo, n) in enumerate(((0, HALF), (256, HALF), (512, SL))):
        piece = pl.ds(lo, n)
        right_own.append(remote(cot.at[0, :, piece], cots.at[1, :, piece], cs.at[i], cr.at[1, i], x=xs[1]))
    for i, (lo, n) in enumerate(((512, HALF), (768, HALF), (0, SL))):
        piece = pl.ds(lo, n)
        left_own.append(remote(cot.at[0, :, piece], cots.at[2, :, piece], cs.at[3 + i], cr.at[2, i], x=xs[3]))
    for i in range(3):
        go(right_own[i])
        go(left_own[i])

    vecs[0] = vec[x]
    here[0].wait()
    tokens = tbuf[...].astype(f32)
    centered = tokens - jnp.mean(tokens, axis=1, keepdims=True)
    variance = jnp.mean(centered * centered, axis=1, keepdims=True)
    inv = lax.rsqrt(variance + eps)
    normed[...] = centered * inv
    gained[...] = centered * inv * gain[...]
    invs[...] = jnp.broadcast_to(inv, invs.shape)
    total[...] = jnp.zeros_like(total)
    sacc[...] = jnp.zeros_like(sacc)
    eacc[...] = jnp.zeros_like(eacc)
    for copy in here[1:]:
        copy.wait()

    for o in (1, 3, 2):
        exp_copies[o, 0].wait_recv()
        exp_copies[o, 1].wait_recv()
    exp_y = go(remote(w1.at[y, :, c], w1.at[y, :, c], es.at[0], er.at[0], y=oy))
    exp_c = go(remote(w1.at[y, :, c], w1.at[y, :, c], es.at[1], er.at[1], c=oc))
    shr_y.wait_recv()
    shr_f = go(remote(w2.at[oy, c], w2.at[oy, c], ss.at[2], sr.at[2], c=oc))
    for o in (1, 3, 2):
        vec_copies[o].wait_recv()

    @pl.loop(0, 4)
    def _(k):
        si[k] = (gained[...] * row(vecs[k], 0)).astype(bf16)

    fwd = []
    for i, lo in enumerate(PIECES):
        (right_own, left_own)[i % 2][i // 2].wait_recv()
        src, to = ((1, xs[1]), (2, xs[3]))[i % 2]
        piece = pl.ds(lo, HALF)
        fwd.append(go(remote(cots.at[src, :, piece], cots.at[3, :, piece], cs.at[6 + i], cr.at[3, i], x=to)))
    exp_y.wait_recv()
    exp_f = go(remote(w1.at[oy, :, c], w1.at[oy, :, c], es.at[2], er.at[2], c=oc))
    for copy in (shr_c, exp_c, shr_f, exp_f):
        copy.wait_recv()
    told(0, 2)
    tell_z(1)

    @pl.loop(0, 4)
    def _(k):
        v = vecs[k]
        project = dot(si[k], w1[...].reshape(D, SL), 1, 0)
        active, slope = gelu_pair(project * v[4:5])
        proj[k] = project
        actf[k] = active
        act[k] = (active * v[5:6]).astype(bf16)
        pa[k] = slope * v[5:6]

    told(1, 2)
    tell_z(2)

    def seeds(k, v, at):
        scale_out = row(v, 2)
        second = w2[...].reshape(SL, D)
        if at is None:
            return cots[k], scale_out, second
        cut = lambda m: jnp.concatenate([m[:, at : at + HALF], m[:, at + 512 : at + 512 + HALF]], axis=1)
        seed = jnp.concatenate([cots[k, :, at : at + HALF], cots[k, :, at + 512 : at + 512 + HALF]], axis=1)
        return seed, cut(scale_out), cut(second)

    def back_of(seed, scale_out, second):
        return dot((seed.astype(f32) * scale_out).astype(bf16), second, 1, 1)

    def back_part(k, v, back):
        grad_act = jnp.sum(back * actf[k], axis=0, keepdims=True)
        back_hidden = back * pa[k]
        grad_hid = jnp.sum(back_hidden * proj[k], axis=0, keepdims=True)
        sv[k, 4:8] = jnp.concatenate([grad_hid, grad_act, jnp.zeros((2, SL), f32)], axis=0)
        return (back_hidden * v[4:5]).astype(bf16)

    def shrink_part(k, seed, second):
        both = dot(act[k], seed, 0, 0)
        return both, jnp.sum(second.astype(f32) * both, axis=0, keepdims=True)

    def expand_part(k, back_proj):
        eacc[...] += dot(si[k], back_proj, 0, 0)

    def norm_part(k, v, back_proj):
        back_norm = dot(back_proj, w1[...].reshape(D, SL), 1, 1)
        grad_in = jnp.sum(back_norm * gained[...], axis=0, keepdims=True)
        total[...] += back_norm * row(v, 0)
        sv[k, 0:2] = jnp.concatenate([grad_in[:, :SL], grad_in[:, SL:]], axis=0)

    @pl.loop(0, 3)
    def _(k):
        @pl.when(k == 1)
        def _():
            right_own[2].wait_recv()

        @pl.when(k == 2)
        def _():
            left_own[2].wait_recv()

        v = vecs[k]
        seed, scale_out, second = seeds(k, v, None)
        back_proj = back_part(k, v, back_of(seed, scale_out, second))
        both, grad_out = shrink_part(k, seed, second)
        sacc[...] += both * scale_out
        sv[k, 2:4] = jnp.concatenate([grad_out[:, :SL], grad_out[:, SL:]], axis=0)
        expand_part(k, back_proj)
        norm_part(k, v, back_proj)

    right, left, far = (lax.rem(place + o, 4) for o in (1, 3, 2))
    to_right = dict(y=lax.rem(right, 2), h=right // 2)
    to_left = dict(y=lax.rem(left, 2), h=left // 2)
    top, low = pl.ds(0, 4), pl.ds(4, 4)

    def lanes(it):
        i, lo, hi = ITEMS[it]
        return i, slice(lo, hi), pl.ds(lo, hi - lo)

    def core_step(it):
        i, _, l = lanes(it)
        return go(remote(pbuf.at[i, oc, :, :, :, l], rbuf.at[i, :, :, :, l], as_.at[it], ar.at[it], c=oc))

    def ring_start(it, copy):
        i, v, l = lanes(it)
        copy.wait_recv()
        q[i, :, :, :, v] = added(pbuf[i, c, :, :, :, v], rbuf[i, :, :, :, v]).astype(bf16)
        return [
            go(remote(q.at[i, far, top, :, l], yb.at[i, 0, :, :, l], ys.at[it, 0], yr.at[it, 0], **to_right)),
            go(remote(q.at[i, far, low, :, l], yb.at[i, 1, :, :, l], ys.at[it, 1], yr.at[it, 1], **to_left)),
            go(remote(q.at[i, right, low, :, l], yb.at[i, 2, :, :, l], ys.at[it, 2], yr.at[it, 2], **to_right)),
            go(remote(q.at[i, left, top, :, l], yb.at[i, 3, :, :, l], ys.at[it, 3], yr.at[it, 3], **to_left)),
        ]

    def ring_pass(it, copies):
        i, v, l = lanes(it)
        copies[0].wait_recv()
        mix[i, 0, :, :, v] = added(q[i, right, 0:4, :, v], yb[i, 0, :, :, v]).astype(bf16)
        copies.append(go(remote(
            mix.at[i, 0, :, :, l], yb.at[i, 4, :, :, l], ys.at[it, 4], yr.at[it, 4], **to_right
        )))
        copies[1].wait_recv()
        mix[i, 1, :, :, v] = added(q[i, left, 4:8, :, v], yb[i, 1, :, :, v]).astype(bf16)
        copies.append(go(remote(
            mix.at[i, 1, :, :, l], yb.at[i, 5, :, :, l], ys.at[it, 5], yr.at[it, 5], **to_left
        )))

    def deep_start(it, copies):
        i, v, l = lanes(it)
        for copy in copies[2:]:
            copy.wait_recv()
        r[i, 0:4, :, v] = added(q[i, place, 0:4, :, v], yb[i, 3, :, :, v], yb[i, 4, :, :, v]).astype(bf16)
        r[i, 4:8, :, v] = added(q[i, place, 4:8, :, v], yb[i, 2, :, :, v], yb[i, 5, :, :, v]).astype(bf16)
        out = []
        if i == 0:
            for o in (4, 3, 5, 2, 6, 1, 7):
                e = lax.rem(z + o, 8)
                out.append(go(remote(r.at[0, e, :, l], rz.at[0, z, :, l], zs.at[it, o], zr.at[it, o], z=e)))
            rz[0, z, :, v] = r[0, z, :, v]
            return out
        mine = pl.ds(pl.multiple_of(128 * x, 128), 128)
        for o in (4, 3, 5, 2, 6, 1, 7, 0):
            e = lax.rem(z + o, 8)
            for xo in range(4):
                if o or xo:
                    block = pl.ds(pl.multiple_of(128 * xs[xo], 128), 128)
                    out.append(go(remote(
                        r.at[1, e, :, block], rz.at[1, z, :, mine], zs.at[2 + xo, o], zr.at[2 + xo, o],
                        z=e, x=xs[xo],
                    )))
        rz[1, z, :, mine] = r[1, z, :, mine]
        return out

    def deep_sum(it, copies):
        i, v, _ = lanes(it)
        for copy in copies:
            copy.wait_recv()
        done = added(*(rz[i, e, :, v] for e in range(8))).astype(bf16)
        res[i, :, v] = done
        return done

    peers = []
    for o in range(1, 16):
        e = lax.rem(me + o, 16)
        peers.append((o, dict(z=e // 2, h=lax.rem(e, 2))))

    def shrink_blocks(it, both, scale_out):
        _, lo, hi = ITEMS[it]
        for cc in (0, 1):
            for hh in (0, 1):
                for yy in (0, 1):
                    at = (yy * 2 + cc) * 128
                    new = both[at : at + 128, HALF * hh : HALF * hh + HALF] * scale_out[:, HALF * hh : HALF * hh + HALF]
                    block = sacc[at : at + 128, SL * hh + lo : SL * hh + hi] + new
                    pbuf[0, cc, 2 * hh + yy, :, :, lo:hi] = block.astype(bf16).reshape(8, 16, HALF)

    told(2, 2)
    greet(heard.at[3], h=1 - h)
    v = vecs[3]
    fwd[0].wait_recv()
    fwd[1].wait_recv()
    seed, scale_out, second = seeds(3, v, 0)
    both, grad_first = shrink_part(3, seed, second)
    shrink_blocks(0, both, scale_out)
    core_s = core_step(0)
    half_back[...] = back_of(seed, scale_out, second)
    told(3, 1)
    for o in (1, 2, 3):
        greet(heard.at[4], x=xs[o])
    ring_s = ring_start(0, core_s)

    fwd[2].wait_recv()
    fwd[3].wait_recv()
    seed, scale_out, second = seeds(3, v, HALF)
    back_proj = back_part(3, v, half_back[...] + back_of(seed, scale_out, second))
    expand_part(3, back_proj)
    for cc in (0, 1):
        for hh in (0, 1):
            for yy in (0, 1):
                for xx in range(4):
                    at = ((yy * 4 + xx) * 2 + cc) * 64
                    for zz in range(8):
                        top_row, lane = at + zz // 2 * 16, (zz % 2 * 2 + hh) * 128
                        pbuf[1, cc, 2 * hh + yy, zz, :, 128 * xx : 128 * xx + 128] = eacc[
                            top_row : top_row + 16, lane : lane + 128
                        ].astype(bf16)
    core_e = core_step(2)
    ring_pass(0, ring_s)
    both, grad_last = shrink_part(3, seed, second)
    shrink_blocks(1, both, scale_out)
    core_l = core_step(1)
    ring_e = ring_start(2, core_e)
    norm_part(3, v, back_proj)
    ring_l = ring_start(1, core_l)
    sv[3, 2:4] = jnp.concatenate(
        [
            jnp.concatenate([grad_first[:, :HALF], grad_last[:, :HALF]], axis=1),
            jnp.concatenate([grad_first[:, HALF:], grad_last[:, HALF:]], axis=1),
        ],
        axis=0,
    )

    vector_copies = []
    for slot, xo in ((1, 3), (2, 1), (3, 2)):
        vector_copies.append(go(remote(sv.at[slot], svr.at[x], bs.at[xo - 1], br.at[xo - 1], x=xs[xo])))
    svr[x] = sv[0]
    whole = total[...]
    gp[...] = jnp.sum(whole * normed[...], axis=0, keepdims=True)
    gains = []
    for o in range(1, 16):
        yo, xo, co = o // 8, (o // 2) % 4, o % 2
        gains.append(go(remote(
            gp, gpr.at[chip * 2 + c], gs.at[o], gr.at[o], y=oy if yo else y, x=xs[xo], c=oc if co else c
        )))
    gpr[chip * 2 + c] = gp[...]
    unit = whole * gain[...]
    inner = jnp.mean(unit * normed[...], axis=1, keepdims=True)
    back_trunk = invs[:, :1] * (unit - jnp.mean(unit, axis=1, keepdims=True) - normed[...] * inner)
    term = (cots[0].astype(f32) + back_trunk).astype(bf16)
    t[0] = term[:CUT]
    t[1, : TOK - CUT] = term[CUT:]
    t[1, TOK - CUT :] = jnp.zeros((FULL - TOK, D), bf16)
    core_t = go(remote(t.at[oc], rt, as_.at[3], ar.at[3], c=oc))

    ring_pass(2, ring_e)
    ring_pass(1, ring_l)
    told(4, 3)
    deep_s = deep_start(0, ring_s)
    deep_e = deep_start(2, ring_e)
    deep_l = deep_start(1, ring_l)

    core_t.wait_recv()
    joint = added(t[c], rt[...]).astype(bf16)
    for g in range(8):
        tq[g] = joint[:, 128 * g : 128 * g + 128]
    tiles = []
    for g in range(1, 8):
        yo, xo = g // 4, g % 4
        ty, tx = oy if yo else y, xs[xo]
        tiles.append(go(remote(tq.at[ty * 4 + tx], tr.at[chip], ts.at[g], tr_.at[g], y=ty, x=tx)))
    tr[chip] = tq[chip]

    for copy in vector_copies + gains:
        copy.wait_recv()
    sums = svr[0] + svr[1] + svr[2] + svr[3]
    gain_sum = gpr[0]
    for m in range(1, 16):
        gain_sum = gain_sum + gpr[m]
    zero = jnp.zeros((1, SL), f32)
    for i in range(4):
        dv[i] = sums[i : i + 1]
        dv[4 + i] = svr[i, 4:5]
        dv[8 + i] = svr[i, 5:6]
    dv[12] = gain_sum[:, :SL]
    dv[13] = gain_sum[:, SL:]
    dv[14] = zero
    dv[15] = zero
    small = []
    for o, where in peers:
        e = where["z"] * 2 + where["h"]
        small.append(go(remote(dv.at[e], dvr.at[me], ds.at[o], dr.at[o], **where)))
    dvr[me] = dv[me]

    outs = (sh, ex)

    def spread(it):
        i, _, l = lanes(it)
        copies = {}
        for o in (2, 6, 1, 7, 0):
            e = lax.rem(z + o, 8)
            for ho in (0, 1):
                if o or ho:
                    copies[o, ho] = go(remote(
                        res.at[i, :, l], outs[i].at[me, :, l], hs.at[it, o, ho], hr.at[it, o, ho],
                        z=e, h=1 - h if ho else h,
                    ))
        return copies

    def relay(it, copies):
        i, _, l = lanes(it)
        for o, further in ((2, (4, 3)), (6, (5,))):
            for ho in (0, 1):
                copies[o, ho].wait_recv()
                part = outs[i].at[lax.rem(z + 8 - o, 8) * 2 + (1 - h if ho else h), :, l]
                for far_o in further:
                    copies[far_o, ho] = go(remote(
                        part, part, hs.at[it, far_o, ho], hr.at[it, far_o, ho],
                        z=lax.rem(z + far_o - o + 8, 8),
                    ))

    done = deep_sum(0, deep_s)
    spread_s = spread(0)
    sh[me, :, :HALF] = done
    done = deep_sum(2, deep_e)
    spread_e = spread(2)
    ex[me] = done
    done = deep_sum(1, deep_l)
    spread_l = spread(1)
    sh[me, :, HALF:] = done

    for copy in tiles:
        copy.wait_recv()
    tf[c] = added(*(tr[g] for g in range(8))).astype(bf16)
    finish = go(remote(tf.at[c], tf.at[c], fs, fr, c=oc))

    for copy in small:
        copy.wait_recv()
    line = dvr[0]
    for p in range(1, 16):
        line = line + dvr[p]
    dvs[...] = line
    lines = []
    for o, where in peers:
        lines.append(go(remote(dvs, dvo.at[me], os_.at[o], or_.at[o], **where)))
    dvo[me] = line

    relay(0, spread_s)
    relay(2, spread_e)
    relay(1, spread_l)

    for copy in [finish] + lines:
        copy.wait_recv()
    for copies in (spread_s, spread_e, spread_l):
        for (o, ho), copy in copies.items():
            if o not in (2, 6):
                copy.wait_recv()

    for copy in sent:
        copy.wait_send()


def finish_kernel(tf, sh, ex, dvo, tg, eg, sg, ing, hg, ag, og, gg):
    c = lax.axis_index("c")
    turned = tf[...].reshape(FULL, 128).astype(f32).T
    tg[...] = jnp.where(c == 0, turned[:64], turned[64:])[:, :TOK].astype(bf16)
    for i in (0, 1):
        ing[:, SL * i : SL * i + SL] = dvo[i]
        og[:, SL * i : SL * i + SL] = dvo[2 + i]
        gg[:, SL * i : SL * i + SL] = dvo[12 + i]
        for xx in range(4):
            at = 1024 * i + 256 * xx
            hg[:, at : at + 256] = dvo[4 + xx][:, 256 * i : 256 * i + 256]
            ag[:, at : at + 256] = dvo[8 + xx][:, 256 * i : 256 * i + 256]
    for p in range(16):
        low, lane = p // 4 * 16, p % 4 // 2 * 1024 + p % 2 * 128
        for xx in range(4):
            at = lane + 256 * xx
            eg[low : low + 16, at : at + 128] = ex[p, :, 128 * xx : 128 * xx + 128].astype(f32)
        sg[16 * (p // 2) : 16 * (p // 2) + 16, SL * (p % 2) : SL * (p % 2) + SL] = sh[p].astype(f32)


def vmem(n):
    return [pl.BlockSpec(memory_space=pltpu.VMEM)] * n


def dma(*shape):
    return pltpu.SemaphoreType.DMA(shape)


def body(trunk, normgain, expand, shrink, inscale, hidscale, actscale, outscale, cotangent):
    S = jax.ShapeDtypeStruct
    V = pltpu.VMEM
    parts = pl.pallas_call(
        kernel,
        out_shape=[
            V((2, CUT, 128), bf16),
            V((16, 16, SL), bf16),
            V((16, 16, SL), bf16),
            V((16, 1, SL), f32),
        ],
        in_specs=[pl.BlockSpec(memory_space=pl.ANY)] * 9,
        out_specs=vmem(4),
        scratch_shapes=[
            V((1, D), f32),
            V((1, D), f32),
            V((1, FF), f32),
            V((1, FF), f32),
            V((1, D), f32),
            V((TOK, D), bf16),
            V((4, 8, SL), f32),
            V((TOK, D), f32),
            V((TOK, D), f32),
            V((TOK, 128), f32),
            V((4, TOK, D), bf16),
            V((2, 4, 2, 64, SL), bf16),
            V((2, 2, 128, D), bf16),
            V((4, 8, SL), f32),
            V((4, TOK, D), bf16),
            V((4, TOK, SL), bf16),
            V((4, TOK, SL), f32),
            V((4, TOK, SL), f32),
            V((4, TOK, SL), f32),
            V((TOK, D), f32),
            V((SL, D), f32),
            V((D, SL), f32),
            V((TOK, SL), f32),
            V((2, 2, 4, 8, 16, SL), bf16),
            V((2, 4, 8, 16, SL), bf16),
            V((2, CUT, D), bf16),
            V((CUT, D), bf16),
            V((2, 4, 8, 16, SL), bf16),
            V((2, 6, 4, 16, SL), bf16),
            V((2, 2, 4, 16, SL), bf16),
            V((2, 8, 16, SL), bf16),
            V((2, 8, 16, SL), bf16),
            V((2, 16, SL), bf16),
            V((8, CUT, 128), bf16),
            V((8, CUT, 128), bf16),
            V((4, 8, SL), f32),
            V((4, 8, SL), f32),
            V((1, D), f32),
            V((16, 1, D), f32),
            V((16, 1, SL), f32),
            V((16, 1, SL), f32),
            V((1, SL), f32),
            dma(10), dma(10), dma(4, 4), dma(3, 2), dma(3, 2), dma(3), dma(3), dma(3), dma(3), dma(3), dma(3),
            dma(4), dma(4), dma(3, 6), dma(3, 6), dma(6, 8), dma(6, 8), dma(3, 8, 2), dma(3, 8, 2),
            dma(8), dma(8), pltpu.SemaphoreType.DMA, pltpu.SemaphoreType.DMA, dma(3), dma(3), dma(16), dma(16),
            dma(16), dma(16), dma(16), dma(16), pltpu.SemaphoreType.REGULAR((5,)),
        ],
        compiler_params=pltpu.CompilerParams(
            collective_id=0, has_side_effects=True, vmem_limit_bytes=60 * 1024 * 1024
        ),
        name="exchange_compute",
    )(
        trunk, expand, shrink, cotangent, normgain.reshape(1, D), inscale, hidscale, actscale, outscale
    )
    tg, eg, sg, ing, hg, ag, og, gg = pl.pallas_call(
        finish_kernel,
        out_shape=[
            S((64, TOK), bf16),
            S((64, FF), f32),
            S((128, D), f32),
            S((1, D), f32),
            S((1, FF), f32),
            S((1, FF), f32),
            S((1, D), f32),
            S((1, D), f32),
        ],
        in_specs=vmem(4),
        out_specs=vmem(8),
        name="write_outputs",
    )(*(pltpu.with_memory_space_constraint(part, pltpu.VMEM) for part in parts))
    return tg.T, eg, sg, ing, hg, ag, og, gg.reshape(D)


def solution(mesh):
    finer = Mesh(mesh.devices.reshape(2, 4, 2, 8, 2), AXES)
    rows = P(MEMBER, None)
    in_specs = (P(DP, None), P(), rows, rows, rows, rows, rows, rows, P(MEMBER, DP, None))
    out_specs = (P(DP, MEMBER), rows, rows, rows, rows, rows, rows, P())
    return jax.shard_map(body, mesh=finer, in_specs=in_specs, out_specs=out_specs, check_vma=False)
```

```python
import jax
import jax.numpy as jnp
from jax import lax
from jax.experimental import pallas as pl
from jax.experimental.pallas import tpu as pltpu
from jax.sharding import Mesh
from jax.sharding import PartitionSpec as P

AXES = ("y", "x", "c", "z", "h")
MEMBER = ("y", "x", "c")
DP = ("z", "h")
TOK = 394
CUT = 208
HALF = 256
PIECES = (0, 512, 256, 768)
FULL = 416
D = 1024
FF = 2048
SL = 512
ITEMS = ((0, 0, HALF), (0, HALF, SL), (1, 0, SL))

eps = 1e-06
coeff = 0.7978845608028654
f32 = jnp.float32
bf16 = jnp.bfloat16
MESH = pl.DeviceIdType.MESH


def remote(src, dst, send, recv, **where):
    return pltpu.make_async_remote_copy(
        src_ref=src, dst_ref=dst, send_sem=send, recv_sem=recv, device_id=where, device_id_type=MESH
    )


def greet(barrier, **where):
    pl.semaphore_signal(barrier, inc=1, device_id=where, device_id_type=MESH)


def gelu_pair(hidden):
    inner = coeff * (hidden + 0.044715 * hidden * hidden * hidden)
    tangent = jnp.tanh(inner)
    active = 0.5 * hidden * (1.0 + tangent)
    slope = 0.5 * (1.0 + tangent) + 0.5 * hidden * (1.0 - tangent * tangent) * coeff * (
        1.0 + 3.0 * 0.044715 * hidden * hidden
    )
    return active, slope


def dot(a, b, ca, cb):
    return lax.dot_general(a, b, (((ca,), (cb,)), ((), ())), preferred_element_type=f32)


def row(v, i):
    return jnp.concatenate([v[i : i + 1], v[i + 1 : i + 2]], axis=1)


def added(*refs):
    total = refs[0].astype(f32)
    for r in refs[1:]:
        total = total + r.astype(f32)
    return total


def kernel(
    trunk, exp, shr, cot, gain_in, in_in, hid_in, act_in, out_in,
    tf, sh, ex, dvo,
    gain, inscale, hidscale, actscale, outscale, tbuf, vec, normed, gained, invs, cots, w1, w2, vecs, si, act, pa, actf, proj, total, sacc, eacc, half_back,
    pbuf, rbuf, t, rt, q, yb, mix, r, rz, res, tq, tr, sv, svr, gp, gpr, dv, dvr, dvs,
    ls, cs, cr, ws, wr, vs, vr, ss, sr, es, er,
    as_, ar, ys, yr, zs, zr, hs, hr, ts, tr_, fs, fr, bs, br, gs, gr, ds, dr, os_, or_, heard,
):
    y, x, c, z, h = (lax.axis_index(a) for a in AXES)
    xs = [lax.rem(x + o, 4) for o in range(4)]
    oy, oc = 1 - y, 1 - c
    me = z * 2 + h
    chip = y * 4 + x
    place = h * 2 + y
    sent = []

    def go(copy):
        copy.start()
        sent.append(copy)
        return copy

    barrier = pltpu.get_barrier_semaphore()

    for yo in (0, 1):
        for co in (0, 1):
            for xo in range(4):
                if yo or co or xo:
                    greet(barrier, y=oy if yo else y, x=xs[xo], c=oc if co else c)
    greet(barrier, y=oy, h=1 - h)
    greet(barrier, h=1 - h)
    above, below = lax.rem(z + 1, 8), lax.rem(z + 7, 8)
    greet(barrier, z=above)
    greet(barrier, z=below)

    def tell_z(i):
        greet(heard.at[i], z=above)
        greet(heard.at[i], z=below)

    def told(i, n):
        pl.semaphore_wait(heard.at[i], n)

    here = [
        pltpu.make_async_copy(trunk, tbuf, ls.at[0]),
        pltpu.make_async_copy(shr, w2.at[y, c], ls.at[1]),
        pltpu.make_async_copy(cot.at[0], cots.at[0], ls.at[2]),
    ]
    for half in (0, 1):
        here.append(
            pltpu.make_async_copy(
                exp.at[:, pl.ds(pl.multiple_of(1024 * half + 256 * x, 256), 256)],
                w1.at[y, x, c, :, pl.ds(256 * half, 256)],
                ls.at[3 + half],
            )
        )
    lines = []
    for i, (src, dst) in enumerate(
        ((in_in, inscale), (hid_in, hidscale), (act_in, actscale), (out_in, outscale), (gain_in, gain))
    ):
        lines.append(pltpu.make_async_copy(src, dst, ls.at[5 + i]))
    for copy in lines + here:
        copy.start()
    pl.semaphore_wait(barrier, 19)
    tell_z(0)

    slot_of = {1: 1, 3: 2, 2: 3}
    vec_copies, exp_copies = {}, {}
    rows_here = pl.ds(pl.multiple_of(32 * h, 32), 32)
    rows_there = pl.ds(pl.multiple_of(32 * (1 - h), 32), 32)
    wide_here = pl.ds(pl.multiple_of(64 * h, 64), 64)
    for o in (1, 3, 2):
        for half in (0, 1):
            exp_copies[o, half] = go(remote(
                exp.at[rows_here, pl.ds(pl.multiple_of(1024 * half + 256 * xs[o], 256), 256)],
                w1.at[y, x, c, rows_here, pl.ds(256 * half, 256)],
                ws.at[o - 1, half], wr.at[o - 1, half], x=xs[o],
            ))
    shr_y = go(remote(shr.at[wide_here], w2.at[y, c, wide_here], ss.at[0], sr.at[0], y=oy))
    shr_n = go(remote(shr.at[wide_here], w2.at[y, c, wide_here], ss.at[3], sr.at[3], y=oy, h=1 - h))
    shr_c = go(remote(shr, w2.at[y, c], ss.at[1], sr.at[1], c=oc))
    for copy in lines:
        copy.wait()
    for xx in range(4):
        for i in (0, 1):
            vec[xx, i : i + 1] = inscale[:, SL * i : SL * i + SL]
            vec[xx, 2 + i : 3 + i] = outscale[:, SL * i : SL * i + SL]
            at = 1024 * i + 256 * xx
            vec[xx, 4:5, 256 * i : 256 * i + 256] = hidscale[:, at : at + 256]
            vec[xx, 5:6, 256 * i : 256 * i + 256] = actscale[:, at : at + 256]
        vec[xx, 6:8] = jnp.zeros((2, SL), f32)
    for o in (1, 3, 2):
        vec_copies[o] = go(remote(
            vec.at[xs[o]], vecs.at[slot_of[o]], vs.at[o - 1], vr.at[o - 1], x=xs[o]
        ))
    right_own, left_own = [], []
    for i, (lo, n) in enumerate(((0, HALF), (256, HALF), (512, SL))):
        piece = pl.ds(lo, n)
        right_own.append(remote(cot.at[0, :, piece], cots.at[1, :, piece], cs.at[i], cr.at[1, i], x=xs[1]))
    for i, (lo, n) in enumerate(((512, HALF), (768, HALF), (0, SL))):
        piece = pl.ds(lo, n)
        left_own.append(remote(cot.at[0, :, piece], cots.at[2, :, piece], cs.at[3 + i], cr.at[2, i], x=xs[3]))
    for i in range(3):
        go(right_own[i])
        go(left_own[i])

    vecs[0] = vec[x]
    here[0].wait()
    tokens = tbuf[...].astype(f32)
    centered = tokens - jnp.mean(tokens, axis=1, keepdims=True)
    variance = jnp.mean(centered * centered, axis=1, keepdims=True)
    inv = lax.rsqrt(variance + eps)
    normed[...] = centered * inv
    gained[...] = centered * inv * gain[...]
    invs[...] = jnp.broadcast_to(inv, invs.shape)
    total[...] = jnp.zeros_like(total)
    sacc[...] = jnp.zeros_like(sacc)
    eacc[...] = jnp.zeros_like(eacc)
    for copy in here[1:]:
        copy.wait()

    for o in (1, 3, 2):
        exp_copies[o, 0].wait_recv()
        exp_copies[o, 1].wait_recv()
    exp_h = []
    for o in (1, 2, 3):
        part = w1.at[y, xs[o], c, rows_here]
        exp_h.append(go(remote(part, part, es.at[o - 1], er.at[o - 1], h=1 - h)))
    part = w1.at[y, :, c, rows_here]
    exp_y = go(remote(part, part, es.at[3], er.at[3], y=oy))
    exp_n = go(remote(part, part, es.at[4], er.at[4], y=oy, h=1 - h))
    exp_c = go(remote(part, part, es.at[5], er.at[5], c=oc))
    shr_y.wait_recv()
    shr_n.wait_recv()
    shr_f = go(remote(w2.at[oy, c], w2.at[oy, c], ss.at[2], sr.at[2], c=oc))
    for o in (1, 3, 2):
        vec_copies[o].wait_recv()

    @pl.loop(0, 4)
    def _(k):
        si[k] = (gained[...] * row(vecs[k], 0)).astype(bf16)

    for copy in exp_h:
        copy.wait_recv()
    part = w1.at[y, :, c, rows_there]
    exp_d = go(remote(part, part, es.at[6], er.at[6], c=oc))

    fwd = []
    for i, lo in enumerate(PIECES):
        (right_own, left_own)[i % 2][i // 2].wait_recv()
        src, to = ((1, xs[1]), (2, xs[3]))[i % 2]
        piece = pl.ds(lo, HALF)
        fwd.append(go(remote(cots.at[src, :, piece], cots.at[3, :, piece], cs.at[6 + i], cr.at[3, i], x=to)))
    exp_y.wait_recv()
    exp_n.wait_recv()
    exp_f = go(remote(w1.at[oy, :, c], w1.at[oy, :, c], es.at[7], er.at[7], c=oc))
    for copy in (shr_c, exp_c, exp_d, shr_f, exp_f):
        copy.wait_recv()
    told(0, 2)
    tell_z(1)

    @pl.loop(0, 4)
    def _(k):
        v = vecs[k]
        project = dot(si[k], w1[...].reshape(D, SL), 1, 0)
        active, slope = gelu_pair(project * v[4:5])
        proj[k] = project
        actf[k] = active
        act[k] = (active * v[5:6]).astype(bf16)
        pa[k] = slope * v[5:6]

    told(1, 2)
    tell_z(2)

    def seeds(k, v, at):
        scale_out = row(v, 2)
        second = w2[...].reshape(SL, D)
        if at is None:
            return cots[k], scale_out, second
        cut = lambda m: jnp.concatenate([m[:, at : at + HALF], m[:, at + 512 : at + 512 + HALF]], axis=1)
        seed = jnp.concatenate([cots[k, :, at : at + HALF], cots[k, :, at + 512 : at + 512 + HALF]], axis=1)
        return seed, cut(scale_out), cut(second)

    def back_of(seed, scale_out, second):
        return dot((seed.astype(f32) * scale_out).astype(bf16), second, 1, 1)

    def back_part(v, back, k):
        return (back * pa[k] * v[4:5]).astype(bf16)

    def back_sums(back, k):
        grad_act = jnp.sum(back * actf[k], axis=0, keepdims=True)
        grad_hid = jnp.sum(back * pa[k] * proj[k], axis=0, keepdims=True)
        sv[k, 4:8] = jnp.concatenate([grad_hid, grad_act, jnp.zeros((2, SL), f32)], axis=0)

    def shrink_part(k, seed, second):
        both = dot(act[k], seed, 0, 0)
        return both, jnp.sum(second.astype(f32) * both, axis=0, keepdims=True)

    def expand_part(k, back_proj):
        eacc[...] += dot(si[k], back_proj, 0, 0)

    def norm_part(k, v, back_proj):
        back_norm = dot(back_proj, w1[...].reshape(D, SL), 1, 1)
        grad_in = jnp.sum(back_norm * gained[...], axis=0, keepdims=True)
        total[...] += back_norm * row(v, 0)
        sv[k, 0:2] = jnp.concatenate([grad_in[:, :SL], grad_in[:, SL:]], axis=0)

    @pl.loop(0, 3)
    def _(k):
        @pl.when(k == 1)
        def _():
            right_own[2].wait_recv()

        @pl.when(k == 2)
        def _():
            left_own[2].wait_recv()

        v = vecs[k]
        seed, scale_out, second = seeds(k, v, None)
        back = back_of(seed, scale_out, second)
        back_proj = back_part(v, back, k)
        back_sums(back, k)
        both, grad_out = shrink_part(k, seed, second)
        sacc[...] += both * scale_out
        sv[k, 2:4] = jnp.concatenate([grad_out[:, :SL], grad_out[:, SL:]], axis=0)
        expand_part(k, back_proj)
        norm_part(k, v, back_proj)

    right, left, far = (lax.rem(place + o, 4) for o in (1, 3, 2))
    to_right = dict(y=lax.rem(right, 2), h=right // 2)
    to_left = dict(y=lax.rem(left, 2), h=left // 2)
    top, low = pl.ds(0, 4), pl.ds(4, 4)

    def lanes(it):
        i, lo, hi = ITEMS[it]
        return i, slice(lo, hi), pl.ds(lo, hi - lo)

    def core_step(it):
        i, _, l = lanes(it)
        return go(remote(pbuf.at[i, oc, :, :, :, l], rbuf.at[i, :, :, :, l], as_.at[it], ar.at[it], c=oc))

    def ring_start(it, copy):
        i, v, l = lanes(it)
        copy.wait_recv()
        q[i, :, :, :, v] = added(pbuf[i, c, :, :, :, v], rbuf[i, :, :, :, v]).astype(bf16)
        return [
            go(remote(q.at[i, far, top, :, l], yb.at[i, 0, :, :, l], ys.at[it, 0], yr.at[it, 0], **to_right)),
            go(remote(q.at[i, far, low, :, l], yb.at[i, 1, :, :, l], ys.at[it, 1], yr.at[it, 1], **to_left)),
            go(remote(q.at[i, right, low, :, l], yb.at[i, 2, :, :, l], ys.at[it, 2], yr.at[it, 2], **to_right)),
            go(remote(q.at[i, left, top, :, l], yb.at[i, 3, :, :, l], ys.at[it, 3], yr.at[it, 3], **to_left)),
        ]

    def ring_pass(it, copies):
        i, v, l = lanes(it)
        copies[0].wait_recv()
        mix[i, 0, :, :, v] = added(q[i, right, 0:4, :, v], yb[i, 0, :, :, v]).astype(bf16)
        copies.append(go(remote(
            mix.at[i, 0, :, :, l], yb.at[i, 4, :, :, l], ys.at[it, 4], yr.at[it, 4], **to_right
        )))
        copies[1].wait_recv()
        mix[i, 1, :, :, v] = added(q[i, left, 4:8, :, v], yb[i, 1, :, :, v]).astype(bf16)
        copies.append(go(remote(
            mix.at[i, 1, :, :, l], yb.at[i, 5, :, :, l], ys.at[it, 5], yr.at[it, 5], **to_left
        )))

    def deep_start(it, copies):
        i, v, l = lanes(it)
        for copy in copies[2:]:
            copy.wait_recv()
        r[i, 0:4, :, v] = added(q[i, place, 0:4, :, v], yb[i, 3, :, :, v], yb[i, 4, :, :, v]).astype(bf16)
        r[i, 4:8, :, v] = added(q[i, place, 4:8, :, v], yb[i, 2, :, :, v], yb[i, 5, :, :, v]).astype(bf16)
        out = []
        if i == 0:
            for o in (4, 3, 5, 2, 6, 1, 7):
                e = lax.rem(z + o, 8)
                out.append(go(remote(r.at[0, e, :, l], rz.at[0, z, :, l], zs.at[it, o], zr.at[it, o], z=e)))
            rz[0, z, :, v] = r[0, z, :, v]
            return out
        mine = pl.ds(pl.multiple_of(128 * x, 128), 128)
        for o in (4, 3, 5, 2, 6, 1, 7, 0):
            e = lax.rem(z + o, 8)
            for xo in range(4):
                if o or xo:
                    block = pl.ds(pl.multiple_of(128 * xs[xo], 128), 128)
                    out.append(go(remote(
                        r.at[1, e, :, block], rz.at[1, z, :, mine], zs.at[2 + xo, o], zr.at[2 + xo, o],
                        z=e, x=xs[xo],
                    )))
        rz[1, z, :, mine] = r[1, z, :, mine]
        return out

    def deep_sum(it, copies):
        i, v, _ = lanes(it)
        for copy in copies:
            copy.wait_recv()
        done = added(*(rz[i, e, :, v] for e in range(8))).astype(bf16)
        res[i, :, v] = done
        return done

    peers = []
    for o in range(1, 16):
        e = lax.rem(me + o, 16)
        peers.append((o, dict(z=e // 2, h=lax.rem(e, 2))))

    def shrink_blocks(it, both, scale_out):
        _, lo, hi = ITEMS[it]
        for cc in (0, 1):
            for hh in (0, 1):
                for yy in (0, 1):
                    at = (yy * 2 + cc) * 128
                    new = both[at : at + 128, HALF * hh : HALF * hh + HALF] * scale_out[:, HALF * hh : HALF * hh + HALF]
                    block = sacc[at : at + 128, SL * hh + lo : SL * hh + hi] + new
                    pbuf[0, cc, 2 * hh + yy, :, :, lo:hi] = block.astype(bf16).reshape(8, 16, HALF)

    told(2, 2)
    greet(heard.at[3], h=1 - h)
    v = vecs[3]
    fwd[0].wait_recv()
    fwd[1].wait_recv()
    seed, scale_out, second = seeds(3, v, 0)
    both, grad_first = shrink_part(3, seed, second)
    shrink_blocks(0, both, scale_out)
    core_s = core_step(0)
    half_back[...] = back_of(seed, scale_out, second)
    told(3, 1)
    for o in (1, 2, 3):
        greet(heard.at[4], x=xs[o])
    ring_s = ring_start(0, core_s)

    fwd[2].wait_recv()
    fwd[3].wait_recv()
    seed, scale_out, second = seeds(3, v, HALF)
    back = half_back[...] + back_of(seed, scale_out, second)
    back_proj = back_part(v, back, 3)
    expand_part(3, back_proj)
    for cc in (0, 1):
        for hh in (0, 1):
            for yy in (0, 1):
                for xx in range(4):
                    at = ((yy * 4 + xx) * 2 + cc) * 64
                    for zz in range(8):
                        top_row, lane = at + zz // 2 * 16, (zz % 2 * 2 + hh) * 128
                        pbuf[1, cc, 2 * hh + yy, zz, :, 128 * xx : 128 * xx + 128] = eacc[
                            top_row : top_row + 16, lane : lane + 128
                        ].astype(bf16)
    core_e = core_step(2)
    ring_pass(0, ring_s)
    both, grad_last = shrink_part(3, seed, second)
    shrink_blocks(1, both, scale_out)
    core_l = core_step(1)
    ring_e = ring_start(2, core_e)
    back_sums(back, 3)
    norm_part(3, v, back_proj)
    ring_l = ring_start(1, core_l)
    sv[3, 2:4] = jnp.concatenate(
        [
            jnp.concatenate([grad_first[:, :HALF], grad_last[:, :HALF]], axis=1),
            jnp.concatenate([grad_first[:, HALF:], grad_last[:, HALF:]], axis=1),
        ],
        axis=0,
    )

    vector_copies = []
    for slot, xo in ((1, 3), (2, 1), (3, 2)):
        vector_copies.append(go(remote(sv.at[slot], svr.at[x], bs.at[xo - 1], br.at[xo - 1], x=xs[xo])))
    svr[x] = sv[0]
    whole = total[...]
    gp[...] = jnp.sum(whole * normed[...], axis=0, keepdims=True)
    gains = []
    for o in range(1, 16):
        yo, xo, co = o // 8, (o // 2) % 4, o % 2
        gains.append(go(remote(
            gp, gpr.at[chip * 2 + c], gs.at[o], gr.at[o], y=oy if yo else y, x=xs[xo], c=oc if co else c
        )))
    gpr[chip * 2 + c] = gp[...]
    unit = whole * gain[...]
    inner = jnp.mean(unit * normed[...], axis=1, keepdims=True)
    back_trunk = invs[:, :1] * (unit - jnp.mean(unit, axis=1, keepdims=True) - normed[...] * inner)
    term = (cots[0].astype(f32) + back_trunk).astype(bf16)
    t[0] = term[:CUT]
    t[1, : TOK - CUT] = term[CUT:]
    t[1, TOK - CUT :] = jnp.zeros((FULL - TOK, D), bf16)
    core_t = go(remote(t.at[oc], rt, as_.at[3], ar.at[3], c=oc))

    ring_pass(2, ring_e)
    ring_pass(1, ring_l)
    told(4, 3)
    deep_s = deep_start(0, ring_s)
    deep_e = deep_start(2, ring_e)
    deep_l = deep_start(1, ring_l)

    core_t.wait_recv()
    joint = added(t[c], rt[...]).astype(bf16)
    for g in range(8):
        tq[g] = joint[:, 128 * g : 128 * g + 128]
    tiles = []
    for g in range(1, 8):
        yo, xo = g // 4, g % 4
        ty, tx = oy if yo else y, xs[xo]
        tiles.append(go(remote(tq.at[ty * 4 + tx], tr.at[chip], ts.at[g], tr_.at[g], y=ty, x=tx)))
    tr[chip] = tq[chip]

    for copy in vector_copies + gains:
        copy.wait_recv()
    sums = svr[0] + svr[1] + svr[2] + svr[3]
    gain_sum = gpr[0]
    for m in range(1, 16):
        gain_sum = gain_sum + gpr[m]
    zero = jnp.zeros((1, SL), f32)
    for i in range(4):
        dv[i] = sums[i : i + 1]
        dv[4 + i] = svr[i, 4:5]
        dv[8 + i] = svr[i, 5:6]
    dv[12] = gain_sum[:, :SL]
    dv[13] = gain_sum[:, SL:]
    dv[14] = zero
    dv[15] = zero
    small = []
    for o, where in peers:
        e = where["z"] * 2 + where["h"]
        small.append(go(remote(dv.at[e], dvr.at[me], ds.at[o], dr.at[o], **where)))
    dvr[me] = dv[me]

    outs = (sh, ex)

    def spread(it):
        i, _, l = lanes(it)
        copies = {}
        for o in (2, 6, 1, 7, 0):
            e = lax.rem(z + o, 8)
            for ho in (0, 1):
                if o or ho:
                    copies[o, ho] = go(remote(
                        res.at[i, :, l], outs[i].at[me, :, l], hs.at[it, o, ho], hr.at[it, o, ho],
                        z=e, h=1 - h if ho else h,
                    ))
        return copies

    def relay(it, copies):
        i, _, l = lanes(it)
        for o, further in ((2, (4, 3)), (6, (5,))):
            for ho in (0, 1):
                copies[o, ho].wait_recv()
                part = outs[i].at[lax.rem(z + 8 - o, 8) * 2 + (1 - h if ho else h), :, l]
                for far_o in further:
                    copies[far_o, ho] = go(remote(
                        part, part, hs.at[it, far_o, ho], hr.at[it, far_o, ho],
                        z=lax.rem(z + far_o - o + 8, 8),
                    ))

    done = deep_sum(0, deep_s)
    spread_s = spread(0)
    sh[me, :, :HALF] = done
    done = deep_sum(2, deep_e)
    spread_e = spread(2)
    ex[me] = done
    done = deep_sum(1, deep_l)
    spread_l = spread(1)
    sh[me, :, HALF:] = done

    for copy in tiles:
        copy.wait_recv()
    tf[c] = added(*(tr[g] for g in range(8))).astype(bf16)
    finish = go(remote(tf.at[c], tf.at[c], fs, fr, c=oc))

    for copy in small:
        copy.wait_recv()
    line = dvr[0]
    for p in range(1, 16):
        line = line + dvr[p]
    dvs[...] = line
    lines = []
    for o, where in peers:
        lines.append(go(remote(dvs, dvo.at[me], os_.at[o], or_.at[o], **where)))
    dvo[me] = line

    relay(0, spread_s)
    relay(2, spread_e)
    relay(1, spread_l)

    for copy in [finish] + lines:
        copy.wait_recv()
    for copies in (spread_s, spread_e, spread_l):
        for (o, ho), copy in copies.items():
            if o not in (2, 6):
                copy.wait_recv()

    for copy in sent:
        copy.wait_send()


def finish_kernel(tf, sh, ex, dvo, tg, eg, sg, ing, hg, ag, og, gg):
    c = lax.axis_index("c")
    turned = tf[...].reshape(FULL, 128).astype(f32).T
    tg[...] = jnp.where(c == 0, turned[:64], turned[64:])[:, :TOK].astype(bf16)
    for i in (0, 1):
        ing[:, SL * i : SL * i + SL] = dvo[i]
        og[:, SL * i : SL * i + SL] = dvo[2 + i]
        gg[:, SL * i : SL * i + SL] = dvo[12 + i]
        for xx in range(4):
            at = 1024 * i + 256 * xx
            hg[:, at : at + 256] = dvo[4 + xx][:, 256 * i : 256 * i + 256]
            ag[:, at : at + 256] = dvo[8 + xx][:, 256 * i : 256 * i + 256]
    for p in range(16):
        low, lane = p // 4 * 16, p % 4 // 2 * 1024 + p % 2 * 128
        for xx in range(4):
            at = lane + 256 * xx
            eg[low : low + 16, at : at + 128] = ex[p, :, 128 * xx : 128 * xx + 128].astype(f32)
        sg[16 * (p // 2) : 16 * (p // 2) + 16, SL * (p % 2) : SL * (p % 2) + SL] = sh[p].astype(f32)


def vmem(n):
    return [pl.BlockSpec(memory_space=pltpu.VMEM)] * n


def dma(*shape):
    return pltpu.SemaphoreType.DMA(shape)


def body(trunk, normgain, expand, shrink, inscale, hidscale, actscale, outscale, cotangent):
    S = jax.ShapeDtypeStruct
    V = pltpu.VMEM
    parts = pl.pallas_call(
        kernel,
        out_shape=[
            V((2, CUT, 128), bf16),
            V((16, 16, SL), bf16),
            V((16, 16, SL), bf16),
            V((16, 1, SL), f32),
        ],
        in_specs=[pl.BlockSpec(memory_space=pl.ANY)] * 9,
        out_specs=vmem(4),
        scratch_shapes=[
            V((1, D), f32),
            V((1, D), f32),
            V((1, FF), f32),
            V((1, FF), f32),
            V((1, D), f32),
            V((TOK, D), bf16),
            V((4, 8, SL), f32),
            V((TOK, D), f32),
            V((TOK, D), f32),
            V((TOK, 128), f32),
            V((4, TOK, D), bf16),
            V((2, 4, 2, 64, SL), bf16),
            V((2, 2, 128, D), bf16),
            V((4, 8, SL), f32),
            V((4, TOK, D), bf16),
            V((4, TOK, SL), bf16),
            V((4, TOK, SL), f32),
            V((4, TOK, SL), f32),
            V((4, TOK, SL), f32),
            V((TOK, D), f32),
            V((SL, D), f32),
            V((D, SL), f32),
            V((TOK, SL), f32),
            V((2, 2, 4, 8, 16, SL), bf16),
            V((2, 4, 8, 16, SL), bf16),
            V((2, CUT, D), bf16),
            V((CUT, D), bf16),
            V((2, 4, 8, 16, SL), bf16),
            V((2, 6, 4, 16, SL), bf16),
            V((2, 2, 4, 16, SL), bf16),
            V((2, 8, 16, SL), bf16),
            V((2, 8, 16, SL), bf16),
            V((2, 16, SL), bf16),
            V((8, CUT, 128), bf16),
            V((8, CUT, 128), bf16),
            V((4, 8, SL), f32),
            V((4, 8, SL), f32),
            V((1, D), f32),
            V((16, 1, D), f32),
            V((16, 1, SL), f32),
            V((16, 1, SL), f32),
            V((1, SL), f32),
            dma(10), dma(10), dma(4, 4), dma(3, 2), dma(3, 2), dma(3), dma(3), dma(4), dma(4), dma(8), dma(8),
            dma(4), dma(4), dma(3, 6), dma(3, 6), dma(6, 8), dma(6, 8), dma(3, 8, 2), dma(3, 8, 2),
            dma(8), dma(8), pltpu.SemaphoreType.DMA, pltpu.SemaphoreType.DMA, dma(3), dma(3), dma(16), dma(16),
            dma(16), dma(16), dma(16), dma(16), pltpu.SemaphoreType.REGULAR((5,)),
        ],
        compiler_params=pltpu.CompilerParams(
            collective_id=0, has_side_effects=True, vmem_limit_bytes=60 * 1024 * 1024
        ),
        name="exchange_compute",
    )(
        trunk, expand, shrink, cotangent, normgain.reshape(1, D), inscale, hidscale, actscale, outscale
    )
    tg, eg, sg, ing, hg, ag, og, gg = pl.pallas_call(
        finish_kernel,
        out_shape=[
            S((64, TOK), bf16),
            S((64, FF), f32),
            S((128, D), f32),
            S((1, D), f32),
            S((1, FF), f32),
            S((1, FF), f32),
            S((1, D), f32),
            S((1, D), f32),
        ],
        in_specs=vmem(4),
        out_specs=vmem(8),
        name="write_outputs",
    )(*(pltpu.with_memory_space_constraint(part, pltpu.VMEM) for part in parts))
    return tg.T, eg, sg, ing, hg, ag, og, gg.reshape(D)


def solution(mesh):
    finer = Mesh(mesh.devices.reshape(2, 4, 2, 8, 2), AXES)
    rows = P(MEMBER, None)
    in_specs = (P(DP, None), P(), rows, rows, rows, rows, rows, rows, P(MEMBER, DP, None))
    out_specs = (P(DP, MEMBER), rows, rows, rows, rows, rows, rows, P())
    return jax.shard_map(body, mesh=finer, in_specs=in_specs, out_specs=out_specs, check_vma=False)
```

```python
import jax
import jax.numpy as jnp
from jax import lax
from jax.experimental import pallas as pl
from jax.experimental.pallas import tpu as pltpu
from jax.sharding import Mesh
from jax.sharding import PartitionSpec as P

AXES = ("y", "x", "c", "z", "h")
MEMBER = ("y", "x", "c")
DP = ("z", "h")
TOK = 394
CUT = 208
HALF = 256
PIECES = (0, 512, 256, 768)
FULL = 416
D = 1024
FF = 2048
SL = 512
ITEMS = ((0, 0, HALF), (0, HALF, SL), (1, 0, SL))

eps = 1e-06
coeff = 0.7978845608028654
f32 = jnp.float32
bf16 = jnp.bfloat16
MESH = pl.DeviceIdType.MESH


def remote(src, dst, send, recv, **where):
    return pltpu.make_async_remote_copy(
        src_ref=src, dst_ref=dst, send_sem=send, recv_sem=recv, device_id=where, device_id_type=MESH
    )


def greet(barrier, **where):
    pl.semaphore_signal(barrier, inc=1, device_id=where, device_id_type=MESH)


def gelu_pair(hidden):
    inner = coeff * (hidden + 0.044715 * hidden * hidden * hidden)
    tangent = jnp.tanh(inner)
    active = 0.5 * hidden * (1.0 + tangent)
    slope = 0.5 * (1.0 + tangent) + 0.5 * hidden * (1.0 - tangent * tangent) * coeff * (
        1.0 + 3.0 * 0.044715 * hidden * hidden
    )
    return active, slope


def dot(a, b, ca, cb):
    return lax.dot_general(a, b, (((ca,), (cb,)), ((), ())), preferred_element_type=f32)


def row(v, i):
    return jnp.concatenate([v[i : i + 1], v[i + 1 : i + 2]], axis=1)


def added(*refs):
    total = refs[0].astype(f32)
    for r in refs[1:]:
        total = total + r.astype(f32)
    return total


def kernel(
    trunk, exp, shr, cot, gain_in, in_in, hid_in, act_in, out_in,
    tf, sh, ex, dvo,
    gain, inscale, hidscale, actscale, outscale, tbuf, vec, normed, gained, invs, cots, w1, w2, vecs, si, act, pa, actf, proj, total, sacc, eacc, half_back,
    pbuf, rbuf, t, rt, q, yb, mix, r, rz, res, tq, tr, sv, svr, gp, gpr, dv, dvr, dvs,
    ls, cs, cr, ws, wr, vs, vr, ss, sr, es, er,
    as_, ar, ys, yr, zs, zr, hs, hr, ts, tr_, fs, fr, bs, br, gs, gr, ds, dr, os_, or_, heard,
):
    y, x, c, z, h = (lax.axis_index(a) for a in AXES)
    xs = [lax.rem(x + o, 4) for o in range(4)]
    oy, oc = 1 - y, 1 - c
    me = z * 2 + h
    chip = y * 4 + x
    place = h * 2 + y
    sent = []

    def go(copy):
        copy.start()
        sent.append(copy)
        return copy

    barrier = pltpu.get_barrier_semaphore()

    for yo in (0, 1):
        for co in (0, 1):
            for xo in range(4):
                if yo or co or xo:
                    greet(barrier, y=oy if yo else y, x=xs[xo], c=oc if co else c)
    greet(barrier, y=oy, h=1 - h)
    greet(barrier, h=1 - h)
    above, below = lax.rem(z + 1, 8), lax.rem(z + 7, 8)
    greet(barrier, z=above)
    greet(barrier, z=below)

    def tell_z(i):
        greet(heard.at[i], z=above)
        greet(heard.at[i], z=below)

    def told(i, n):
        pl.semaphore_wait(heard.at[i], n)

    here = [
        pltpu.make_async_copy(trunk, tbuf, ls.at[0]),
        pltpu.make_async_copy(shr, w2.at[y, c], ls.at[1]),
        pltpu.make_async_copy(cot.at[0], cots.at[0], ls.at[2]),
    ]
    for half in (0, 1):
        here.append(
            pltpu.make_async_copy(
                exp.at[:, pl.ds(pl.multiple_of(1024 * half + 256 * x, 256), 256)],
                w1.at[y, x, c, :, pl.ds(256 * half, 256)],
                ls.at[3 + half],
            )
        )
    lines = []
    for i, (src, dst) in enumerate(
        ((in_in, inscale), (hid_in, hidscale), (act_in, actscale), (out_in, outscale), (gain_in, gain))
    ):
        lines.append(pltpu.make_async_copy(src, dst, ls.at[5 + i]))
    for copy in lines + here:
        copy.start()
    pl.semaphore_wait(barrier, 19)
    tell_z(0)

    slot_of = {1: 1, 3: 2, 2: 3}
    vec_copies, exp_copies = {}, {}
    rows_here = pl.ds(pl.multiple_of(32 * h, 32), 32)
    rows_there = pl.ds(pl.multiple_of(32 * (1 - h), 32), 32)
    wide_here = pl.ds(pl.multiple_of(64 * h, 64), 64)
    for o in (1, 3, 2):
        for half in (0, 1):
            exp_copies[o, half] = go(remote(
                exp.at[rows_here, pl.ds(pl.multiple_of(1024 * half + 256 * xs[o], 256), 256)],
                w1.at[y, x, c, rows_here, pl.ds(256 * half, 256)],
                ws.at[o - 1, half], wr.at[o - 1, half], x=xs[o],
            ))
    shr_y = go(remote(shr.at[wide_here], w2.at[y, c, wide_here], ss.at[0], sr.at[0], y=oy))
    shr_n = go(remote(shr.at[wide_here], w2.at[y, c, wide_here], ss.at[3], sr.at[3], y=oy, h=1 - h))
    shr_c = go(remote(shr, w2.at[y, c], ss.at[1], sr.at[1], c=oc))
    for copy in lines:
        copy.wait()
    for xx in range(4):
        for i in (0, 1):
            vec[xx, i : i + 1] = inscale[:, SL * i : SL * i + SL]
            vec[xx, 2 + i : 3 + i] = outscale[:, SL * i : SL * i + SL]
            at = 1024 * i + 256 * xx
            vec[xx, 4:5, 256 * i : 256 * i + 256] = hidscale[:, at : at + 256]
            vec[xx, 5:6, 256 * i : 256 * i + 256] = actscale[:, at : at + 256]
        vec[xx, 6:8] = jnp.zeros((2, SL), f32)
    for o in (1, 3, 2):
        vec_copies[o] = go(remote(
            vec.at[xs[o]], vecs.at[slot_of[o]], vs.at[o - 1], vr.at[o - 1], x=xs[o]
        ))
    right_own, left_own = [], []
    for i, (lo, n) in enumerate(((0, HALF), (256, HALF), (512, SL))):
        piece = pl.ds(lo, n)
        right_own.append(remote(cot.at[0, :, piece], cots.at[1, :, piece], cs.at[i], cr.at[1, i], x=xs[1]))
    for i, (lo, n) in enumerate(((512, HALF), (768, HALF), (0, SL))):
        piece = pl.ds(lo, n)
        left_own.append(remote(cot.at[0, :, piece], cots.at[2, :, piece], cs.at[3 + i], cr.at[2, i], x=xs[3]))
    for i in range(3):
        go(right_own[i])
        go(left_own[i])

    vecs[0] = vec[x]
    here[0].wait()
    tokens = tbuf[...].astype(f32)
    centered = tokens - jnp.mean(tokens, axis=1, keepdims=True)
    variance = jnp.mean(centered * centered, axis=1, keepdims=True)
    inv = lax.rsqrt(variance + eps)
    normed[...] = centered * inv
    gained[...] = centered * inv * gain[...]
    invs[...] = jnp.broadcast_to(inv, invs.shape)
    total[...] = jnp.zeros_like(total)
    sacc[...] = jnp.zeros_like(sacc)
    eacc[...] = jnp.zeros_like(eacc)
    for copy in here[1:]:
        copy.wait()

    for o in (1, 3, 2):
        exp_copies[o, 0].wait_recv()
        exp_copies[o, 1].wait_recv()
    exp_h = []
    for o in (1, 2, 3):
        part = w1.at[y, xs[o], c, rows_here]
        exp_h.append(go(remote(part, part, es.at[o - 1], er.at[o - 1], h=1 - h)))
    part = w1.at[y, :, c, rows_here]
    exp_y = go(remote(part, part, es.at[3], er.at[3], y=oy))
    exp_n = go(remote(part, part, es.at[4], er.at[4], y=oy, h=1 - h))
    exp_c = go(remote(part, part, es.at[5], er.at[5], c=oc))
    shr_y.wait_recv()
    shr_n.wait_recv()
    shr_f = go(remote(w2.at[oy, c], w2.at[oy, c], ss.at[2], sr.at[2], c=oc))
    for o in (1, 3, 2):
        vec_copies[o].wait_recv()

    @pl.loop(0, 4)
    def _(k):
        si[k] = (gained[...] * row(vecs[k], 0)).astype(bf16)

    for copy in exp_h:
        copy.wait_recv()
    part = w1.at[y, :, c, rows_there]
    exp_d = go(remote(part, part, es.at[6], er.at[6], c=oc))

    fwd = []
    for i, lo in enumerate(PIECES):
        (right_own, left_own)[i % 2][i // 2].wait_recv()
        src, to = ((1, xs[1]), (2, xs[3]))[i % 2]
        piece = pl.ds(lo, HALF)
        fwd.append(go(remote(cots.at[src, :, piece], cots.at[3, :, piece], cs.at[6 + i], cr.at[3, i], x=to)))
    exp_y.wait_recv()
    exp_n.wait_recv()
    exp_f = go(remote(w1.at[oy, :, c], w1.at[oy, :, c], es.at[7], er.at[7], c=oc))
    for copy in (shr_c, exp_c, exp_d, shr_f, exp_f):
        copy.wait_recv()
    told(0, 2)
    tell_z(1)

    @pl.loop(0, 4)
    def _(k):
        v = vecs[k]
        project = dot(si[k], w1[...].reshape(D, SL), 1, 0)
        active, slope = gelu_pair(project * v[4:5])
        proj[k] = project
        actf[k] = active
        act[k] = (active * v[5:6]).astype(bf16)
        pa[k] = slope * v[5:6]

    told(1, 2)
    tell_z(2)

    def seeds(k, v, at):
        scale_out = row(v, 2)
        second = w2[...].reshape(SL, D)
        if at is None:
            return cots[k], scale_out, second
        cut = lambda m: jnp.concatenate([m[:, at : at + HALF], m[:, at + 512 : at + 512 + HALF]], axis=1)
        seed = jnp.concatenate([cots[k, :, at : at + HALF], cots[k, :, at + 512 : at + 512 + HALF]], axis=1)
        return seed, cut(scale_out), cut(second)

    def back_of(seed, scale_out, second):
        return dot((seed.astype(f32) * scale_out).astype(bf16), second, 1, 1)

    def back_part(v, back, k):
        return (back * pa[k] * v[4:5]).astype(bf16)

    def back_sums(back, k):
        grad_act = jnp.sum(back * actf[k], axis=0, keepdims=True)
        grad_hid = jnp.sum(back * pa[k] * proj[k], axis=0, keepdims=True)
        sv[k, 4:8] = jnp.concatenate([grad_hid, grad_act, jnp.zeros((2, SL), f32)], axis=0)

    def shrink_part(k, seed, second):
        both = dot(act[k], seed, 0, 0)
        return both, jnp.sum(second.astype(f32) * both, axis=0, keepdims=True)

    def expand_part(k, back_proj):
        eacc[...] += dot(si[k], back_proj, 0, 0)

    def norm_part(k, v, back_proj):
        back_norm = dot(back_proj, w1[...].reshape(D, SL), 1, 1)
        grad_in = jnp.sum(back_norm * gained[...], axis=0, keepdims=True)
        total[...] += back_norm * row(v, 0)
        sv[k, 0:2] = jnp.concatenate([grad_in[:, :SL], grad_in[:, SL:]], axis=0)

    @pl.loop(0, 3)
    def _(k):
        @pl.when(k == 1)
        def _():
            right_own[2].wait_recv()

        @pl.when(k == 2)
        def _():
            left_own[2].wait_recv()

        v = vecs[k]
        seed, scale_out, second = seeds(k, v, None)
        back = back_of(seed, scale_out, second)
        back_proj = back_part(v, back, k)
        back_sums(back, k)
        both, grad_out = shrink_part(k, seed, second)
        sacc[...] += both * scale_out
        sv[k, 2:4] = jnp.concatenate([grad_out[:, :SL], grad_out[:, SL:]], axis=0)
        expand_part(k, back_proj)
        norm_part(k, v, back_proj)

    right, left, far = (lax.rem(place + o, 4) for o in (1, 3, 2))
    to_right = dict(y=lax.rem(right, 2), h=right // 2)
    to_left = dict(y=lax.rem(left, 2), h=left // 2)
    top, low = pl.ds(0, 4), pl.ds(4, 4)

    def lanes(it):
        i, lo, hi = ITEMS[it]
        return i, slice(lo, hi), pl.ds(lo, hi - lo)

    def core_step(it):
        i, _, l = lanes(it)
        return go(remote(pbuf.at[i, oc, :, :, :, l], rbuf.at[i, :, :, :, l], as_.at[it], ar.at[it], c=oc))

    def ring_start(it, copy):
        i, v, l = lanes(it)
        copy.wait_recv()
        q[i, :, :, :, v] = added(pbuf[i, c, :, :, :, v], rbuf[i, :, :, :, v]).astype(bf16)
        return [
            go(remote(q.at[i, far, top, :, l], yb.at[i, 0, :, :, l], ys.at[it, 0], yr.at[it, 0], **to_right)),
            go(remote(q.at[i, far, low, :, l], yb.at[i, 1, :, :, l], ys.at[it, 1], yr.at[it, 1], **to_left)),
            go(remote(q.at[i, right, low, :, l], yb.at[i, 2, :, :, l], ys.at[it, 2], yr.at[it, 2], **to_right)),
            go(remote(q.at[i, left, top, :, l], yb.at[i, 3, :, :, l], ys.at[it, 3], yr.at[it, 3], **to_left)),
        ]

    def ring_pass(it, copies):
        i, v, l = lanes(it)
        copies[0].wait_recv()
        mix[i, 0, :, :, v] = added(q[i, right, 0:4, :, v], yb[i, 0, :, :, v]).astype(bf16)
        copies.append(go(remote(
            mix.at[i, 0, :, :, l], yb.at[i, 4, :, :, l], ys.at[it, 4], yr.at[it, 4], **to_right
        )))
        copies[1].wait_recv()
        mix[i, 1, :, :, v] = added(q[i, left, 4:8, :, v], yb[i, 1, :, :, v]).astype(bf16)
        copies.append(go(remote(
            mix.at[i, 1, :, :, l], yb.at[i, 5, :, :, l], ys.at[it, 5], yr.at[it, 5], **to_left
        )))

    def deep_start(it, copies):
        i, v, l = lanes(it)
        for copy in copies[2:]:
            copy.wait_recv()
        r[i, 0:4, :, v] = added(q[i, place, 0:4, :, v], yb[i, 3, :, :, v], yb[i, 4, :, :, v]).astype(bf16)
        r[i, 4:8, :, v] = added(q[i, place, 4:8, :, v], yb[i, 2, :, :, v], yb[i, 5, :, :, v]).astype(bf16)
        out = []
        if i == 0:
            for o in (4, 3, 5, 2, 6, 1, 7):
                e = lax.rem(z + o, 8)
                out.append(go(remote(r.at[0, e, :, l], rz.at[0, z, :, l], zs.at[it, o], zr.at[it, o], z=e)))
            rz[0, z, :, v] = r[0, z, :, v]
            return out
        mine = pl.ds(pl.multiple_of(128 * x, 128), 128)
        for o in (4, 3, 5, 2, 6, 1, 7, 0):
            e = lax.rem(z + o, 8)
            for xo in range(4):
                if o or xo:
                    block = pl.ds(pl.multiple_of(128 * xs[xo], 128), 128)
                    out.append(go(remote(
                        r.at[1, e, :, block], rz.at[1, z, :, mine], zs.at[2 + xo, o], zr.at[2 + xo, o],
                        z=e, x=xs[xo],
                    )))
        rz[1, z, :, mine] = r[1, z, :, mine]
        return out

    def deep_sum(it, copies):
        i, v, _ = lanes(it)
        for copy in copies:
            copy.wait_recv()
        done = added(*(rz[i, e, :, v] for e in range(8))).astype(bf16)
        res[i, :, v] = done
        return done

    peers = []
    for o in range(1, 16):
        e = lax.rem(me + o, 16)
        peers.append((o, dict(z=e // 2, h=lax.rem(e, 2))))

    def shrink_blocks(it, both, scale_out):
        _, lo, hi = ITEMS[it]
        for cc in (0, 1):
            for hh in (0, 1):
                for yy in (0, 1):
                    at = (yy * 2 + cc) * 128
                    new = both[at : at + 128, HALF * hh : HALF * hh + HALF] * scale_out[:, HALF * hh : HALF * hh + HALF]
                    block = sacc[at : at + 128, SL * hh + lo : SL * hh + hi] + new
                    pbuf[0, cc, 2 * hh + yy, :, :, lo:hi] = block.astype(bf16).reshape(8, 16, HALF)

    told(2, 2)
    greet(heard.at[3], h=1 - h)
    v = vecs[3]
    fwd[0].wait_recv()
    fwd[1].wait_recv()
    seed, scale_out, second = seeds(3, v, 0)
    both, grad_first = shrink_part(3, seed, second)
    shrink_blocks(0, both, scale_out)
    core_s = core_step(0)
    half_back[...] = back_of(seed, scale_out, second)
    told(3, 1)
    for o in (1, 2, 3):
        greet(heard.at[4], x=xs[o])
    ring_s = ring_start(0, core_s)

    fwd[2].wait_recv()
    fwd[3].wait_recv()
    seed, scale_out, second = seeds(3, v, HALF)
    back = half_back[...] + back_of(seed, scale_out, second)
    back_proj = back_part(v, back, 3)
    expand_part(3, back_proj)
    for cc in (0, 1):
        for hh in (0, 1):
            for yy in (0, 1):
                for xx in range(4):
                    at = ((yy * 4 + xx) * 2 + cc) * 64
                    for zz in range(8):
                        top_row, lane = at + zz // 2 * 16, (zz % 2 * 2 + hh) * 128
                        pbuf[1, cc, 2 * hh + yy, zz, :, 128 * xx : 128 * xx + 128] = eacc[
                            top_row : top_row + 16, lane : lane + 128
                        ].astype(bf16)
    core_e = core_step(2)
    ring_pass(0, ring_s)
    both, grad_last = shrink_part(3, seed, second)
    shrink_blocks(1, both, scale_out)
    core_l = core_step(1)
    ring_e = ring_start(2, core_e)
    back_sums(back, 3)
    norm_part(3, v, back_proj)
    ring_l = ring_start(1, core_l)
    told(4, 3)
    deep_s = deep_start(0, ring_s)
    sv[3, 2:4] = jnp.concatenate(
        [
            jnp.concatenate([grad_first[:, :HALF], grad_last[:, :HALF]], axis=1),
            jnp.concatenate([grad_first[:, HALF:], grad_last[:, HALF:]], axis=1),
        ],
        axis=0,
    )

    outs = (sh, ex)

    def spread(it):
        i, _, l = lanes(it)
        copies = {}
        for o in (2, 6, 1, 7, 0):
            e = lax.rem(z + o, 8)
            for ho in (0, 1):
                if o or ho:
                    copies[o, ho] = go(remote(
                        res.at[i, :, l], outs[i].at[me, :, l], hs.at[it, o, ho], hr.at[it, o, ho],
                        z=e, h=1 - h if ho else h,
                    ))
        return copies

    def relay(it, copies):
        i, _, l = lanes(it)
        for o, further in ((2, (4, 3)), (6, (5,))):
            for ho in (0, 1):
                copies[o, ho].wait_recv()
                part = outs[i].at[lax.rem(z + 8 - o, 8) * 2 + (1 - h if ho else h), :, l]
                for far_o in further:
                    copies[far_o, ho] = go(remote(
                        part, part, hs.at[it, far_o, ho], hr.at[it, far_o, ho],
                        z=lax.rem(z + far_o - o + 8, 8),
                    ))

    vector_copies = []
    for slot, xo in ((1, 3), (2, 1), (3, 2)):
        vector_copies.append(go(remote(sv.at[slot], svr.at[x], bs.at[xo - 1], br.at[xo - 1], x=xs[xo])))
    svr[x] = sv[0]
    whole = total[...]
    gp[...] = jnp.sum(whole * normed[...], axis=0, keepdims=True)
    gains = []
    for o in range(1, 16):
        yo, xo, co = o // 8, (o // 2) % 4, o % 2
        gains.append(go(remote(
            gp, gpr.at[chip * 2 + c], gs.at[o], gr.at[o], y=oy if yo else y, x=xs[xo], c=oc if co else c
        )))
    gpr[chip * 2 + c] = gp[...]
    unit = whole * gain[...]
    inner = jnp.mean(unit * normed[...], axis=1, keepdims=True)
    back_trunk = invs[:, :1] * (unit - jnp.mean(unit, axis=1, keepdims=True) - normed[...] * inner)
    term = (cots[0].astype(f32) + back_trunk).astype(bf16)
    t[0] = term[:CUT]
    t[1, : TOK - CUT] = term[CUT:]
    t[1, TOK - CUT :] = jnp.zeros((FULL - TOK, D), bf16)
    core_t = go(remote(t.at[oc], rt, as_.at[3], ar.at[3], c=oc))

    ring_pass(2, ring_e)
    ring_pass(1, ring_l)
    deep_e = deep_start(2, ring_e)
    deep_l = deep_start(1, ring_l)

    core_t.wait_recv()
    joint = added(t[c], rt[...]).astype(bf16)
    for g in range(8):
        tq[g] = joint[:, 128 * g : 128 * g + 128]
    tiles = []
    for g in range(1, 8):
        yo, xo = g // 4, g % 4
        ty, tx = oy if yo else y, xs[xo]
        tiles.append(go(remote(tq.at[ty * 4 + tx], tr.at[chip], ts.at[g], tr_.at[g], y=ty, x=tx)))
    tr[chip] = tq[chip]

    done = deep_sum(0, deep_s)
    spread_s = spread(0)
    sh[me, :, :HALF] = done

    for copy in vector_copies + gains:
        copy.wait_recv()
    sums = svr[0] + svr[1] + svr[2] + svr[3]
    gain_sum = gpr[0]
    for m in range(1, 16):
        gain_sum = gain_sum + gpr[m]
    zero = jnp.zeros((1, SL), f32)
    for i in range(4):
        dv[i] = sums[i : i + 1]
        dv[4 + i] = svr[i, 4:5]
        dv[8 + i] = svr[i, 5:6]
    dv[12] = gain_sum[:, :SL]
    dv[13] = gain_sum[:, SL:]
    dv[14] = zero
    dv[15] = zero
    small = []
    for o, where in peers:
        e = where["z"] * 2 + where["h"]
        small.append(go(remote(dv.at[e], dvr.at[me], ds.at[o], dr.at[o], **where)))
    dvr[me] = dv[me]

    done = deep_sum(2, deep_e)
    spread_e = spread(2)
    ex[me] = done
    done = deep_sum(1, deep_l)
    spread_l = spread(1)
    sh[me, :, HALF:] = done
    for copy in small:
        copy.wait_recv()
    line = dvr[0]
    for p in range(1, 16):
        line = line + dvr[p]
    dvs[...] = line
    lines = []
    for o, where in peers:
        lines.append(go(remote(dvs, dvo.at[me], os_.at[o], or_.at[o], **where)))
    dvo[me] = line
    relay(0, spread_s)

    for copy in tiles:
        copy.wait_recv()
    tf[c] = added(*(tr[g] for g in range(8))).astype(bf16)
    finish = go(remote(tf.at[c], tf.at[c], fs, fr, c=oc))

    relay(2, spread_e)
    relay(1, spread_l)

    for copy in [finish] + lines:
        copy.wait_recv()
    for copies in (spread_s, spread_e, spread_l):
        for (o, ho), copy in copies.items():
            if o not in (2, 6):
                copy.wait_recv()

    for copy in sent:
        copy.wait_send()


def finish_kernel(tf, sh, ex, dvo, tg, eg, sg, ing, hg, ag, og, gg):
    c = lax.axis_index("c")
    turned = tf[...].reshape(FULL, 128).astype(f32).T
    tg[...] = jnp.where(c == 0, turned[:64], turned[64:])[:, :TOK].astype(bf16)
    for i in (0, 1):
        ing[:, SL * i : SL * i + SL] = dvo[i]
        og[:, SL * i : SL * i + SL] = dvo[2 + i]
        gg[:, SL * i : SL * i + SL] = dvo[12 + i]
        for xx in range(4):
            at = 1024 * i + 256 * xx
            hg[:, at : at + 256] = dvo[4 + xx][:, 256 * i : 256 * i + 256]
            ag[:, at : at + 256] = dvo[8 + xx][:, 256 * i : 256 * i + 256]
    for p in range(16):
        low, lane = p // 4 * 16, p % 4 // 2 * 1024 + p % 2 * 128
        for xx in range(4):
            at = lane + 256 * xx
            eg[low : low + 16, at : at + 128] = ex[p, :, 128 * xx : 128 * xx + 128].astype(f32)
        sg[16 * (p // 2) : 16 * (p // 2) + 16, SL * (p % 2) : SL * (p % 2) + SL] = sh[p].astype(f32)


def vmem(n):
    return [pl.BlockSpec(memory_space=pltpu.VMEM)] * n


def dma(*shape):
    return pltpu.SemaphoreType.DMA(shape)


def body(trunk, normgain, expand, shrink, inscale, hidscale, actscale, outscale, cotangent):
    S = jax.ShapeDtypeStruct
    V = pltpu.VMEM
    parts = pl.pallas_call(
        kernel,
        out_shape=[
            V((2, CUT, 128), bf16),
            V((16, 16, SL), bf16),
            V((16, 16, SL), bf16),
            V((16, 1, SL), f32),
        ],
        in_specs=[pl.BlockSpec(memory_space=pl.ANY)] * 9,
        out_specs=vmem(4),
        scratch_shapes=[
            V((1, D), f32),
            V((1, D), f32),
            V((1, FF), f32),
            V((1, FF), f32),
            V((1, D), f32),
            V((TOK, D), bf16),
            V((4, 8, SL), f32),
            V((TOK, D), f32),
            V((TOK, D), f32),
            V((TOK, 128), f32),
            V((4, TOK, D), bf16),
            V((2, 4, 2, 64, SL), bf16),
            V((2, 2, 128, D), bf16),
            V((4, 8, SL), f32),
            V((4, TOK, D), bf16),
            V((4, TOK, SL), bf16),
            V((4, TOK, SL), f32),
            V((4, TOK, SL), f32),
            V((4, TOK, SL), f32),
            V((TOK, D), f32),
            V((SL, D), f32),
            V((D, SL), f32),
            V((TOK, SL), f32),
            V((2, 2, 4, 8, 16, SL), bf16),
            V((2, 4, 8, 16, SL), bf16),
            V((2, CUT, D), bf16),
            V((CUT, D), bf16),
            V((2, 4, 8, 16, SL), bf16),
            V((2, 6, 4, 16, SL), bf16),
            V((2, 2, 4, 16, SL), bf16),
            V((2, 8, 16, SL), bf16),
            V((2, 8, 16, SL), bf16),
            V((2, 16, SL), bf16),
            V((8, CUT, 128), bf16),
            V((8, CUT, 128), bf16),
            V((4, 8, SL), f32),
            V((4, 8, SL), f32),
            V((1, D), f32),
            V((16, 1, D), f32),
            V((16, 1, SL), f32),
            V((16, 1, SL), f32),
            V((1, SL), f32),
            dma(10), dma(10), dma(4, 4), dma(3, 2), dma(3, 2), dma(3), dma(3), dma(4), dma(4), dma(8), dma(8),
            dma(4), dma(4), dma(3, 6), dma(3, 6), dma(6, 8), dma(6, 8), dma(3, 8, 2), dma(3, 8, 2),
            dma(8), dma(8), pltpu.SemaphoreType.DMA, pltpu.SemaphoreType.DMA, dma(3), dma(3), dma(16), dma(16),
            dma(16), dma(16), dma(16), dma(16), pltpu.SemaphoreType.REGULAR((5,)),
        ],
        compiler_params=pltpu.CompilerParams(
            collective_id=0, has_side_effects=True, vmem_limit_bytes=60 * 1024 * 1024
        ),
        name="exchange_compute",
    )(
        trunk, expand, shrink, cotangent, normgain.reshape(1, D), inscale, hidscale, actscale, outscale
    )
    tg, eg, sg, ing, hg, ag, og, gg = pl.pallas_call(
        finish_kernel,
        out_shape=[
            S((64, TOK), bf16),
            S((64, FF), f32),
            S((128, D), f32),
            S((1, D), f32),
            S((1, FF), f32),
            S((1, FF), f32),
            S((1, D), f32),
            S((1, D), f32),
        ],
        in_specs=vmem(4),
        out_specs=vmem(8),
        name="write_outputs",
    )(*(pltpu.with_memory_space_constraint(part, pltpu.VMEM) for part in parts))
    return tg.T, eg, sg, ing, hg, ag, og, gg.reshape(D)


def solution(mesh):
    finer = Mesh(mesh.devices.reshape(2, 4, 2, 8, 2), AXES)
    rows = P(MEMBER, None)
    in_specs = (P(DP, None), P(), rows, rows, rows, rows, rows, rows, P(MEMBER, DP, None))
    out_specs = (P(DP, MEMBER), rows, rows, rows, rows, rows, rows, P())
    return jax.shard_map(body, mesh=finer, in_specs=in_specs, out_specs=out_specs, check_vma=False)
```

```python
import jax
import jax.numpy as jnp
from jax import lax
from jax.experimental import pallas as pl
from jax.experimental.pallas import tpu as pltpu
from jax.sharding import Mesh
from jax.sharding import PartitionSpec as P

AXES = ("y", "x", "c", "z", "h")
MEMBER = ("y", "x", "c")
DP = ("z", "h")
TOK = 394
CUT = 208
HALF = 256
PIECES = (0, 512, 256, 768)
FULL = 416
D = 1024
FF = 2048
SL = 512
ITEMS = ((0, 0, HALF), (0, HALF, SL), (1, 0, SL))

eps = 1e-06
coeff = 0.7978845608028654
f32 = jnp.float32
bf16 = jnp.bfloat16
MESH = pl.DeviceIdType.MESH


def remote(src, dst, send, recv, **where):
    return pltpu.make_async_remote_copy(
        src_ref=src, dst_ref=dst, send_sem=send, recv_sem=recv, device_id=where, device_id_type=MESH
    )


def greet(barrier, **where):
    pl.semaphore_signal(barrier, inc=1, device_id=where, device_id_type=MESH)


def gelu_pair(hidden):
    inner = coeff * (hidden + 0.044715 * hidden * hidden * hidden)
    tangent = jnp.tanh(inner)
    active = 0.5 * hidden * (1.0 + tangent)
    slope = 0.5 * (1.0 + tangent) + 0.5 * hidden * (1.0 - tangent * tangent) * coeff * (
        1.0 + 3.0 * 0.044715 * hidden * hidden
    )
    return active, slope


def dot(a, b, ca, cb):
    return lax.dot_general(a, b, (((ca,), (cb,)), ((), ())), preferred_element_type=f32)


def row(v, i):
    return jnp.concatenate([v[i : i + 1], v[i + 1 : i + 2]], axis=1)


def added(*refs):
    total = refs[0].astype(f32)
    for r in refs[1:]:
        total = total + r.astype(f32)
    return total


def kernel(
    trunk, exp, shr, cot, gain_in, in_in, hid_in, act_in, out_in,
    tf, sh, ex, dvo,
    gain, inscale, hidscale, actscale, outscale, tbuf, vec, normed, gained, invs, cots, w1, w2, vecs, si, act, pa, actf, proj, total, sacc, eacc, half_back,
    pbuf, rbuf, t, rt, q, yb, mix, r, rz, res, tq, tr, sv, svr, gp, gpr, dv, dvr, dvs,
    ls, cs, cr, ws, wr, vs, vr, ss, sr, es, er,
    as_, ar, ys, yr, zs, zr, hs, hr, ts, tr_, fs, fr, bs, br, gs, gr, ds, dr, os_, or_, heard,
):
    y, x, c, z, h = (lax.axis_index(a) for a in AXES)
    xs = [lax.rem(x + o, 4) for o in range(4)]
    oy, oc = 1 - y, 1 - c
    me = z * 2 + h
    chip = y * 4 + x
    place = h * 2 + y
    sent = []

    def go(copy):
        copy.start()
        sent.append(copy)
        return copy

    def drain(n):
        for copy in sent[:n]:
            copy.wait_send()
        del sent[:n]

    barrier = pltpu.get_barrier_semaphore()

    for yo in (0, 1):
        for co in (0, 1):
            for xo in range(4):
                if yo or co or xo:
                    greet(barrier, y=oy if yo else y, x=xs[xo], c=oc if co else c)
    greet(barrier, y=oy, h=1 - h)
    greet(barrier, h=1 - h)
    above, below = lax.rem(z + 1, 8), lax.rem(z + 7, 8)
    greet(barrier, z=above)
    greet(barrier, z=below)

    def tell_z(i):
        greet(heard.at[i], z=above)
        greet(heard.at[i], z=below)

    def told(i, n):
        pl.semaphore_wait(heard.at[i], n)

    here = [
        pltpu.make_async_copy(trunk, tbuf, ls.at[0]),
        pltpu.make_async_copy(shr, w2.at[y, c], ls.at[1]),
        pltpu.make_async_copy(cot.at[0], cots.at[0], ls.at[2]),
    ]
    for half in (0, 1):
        here.append(
            pltpu.make_async_copy(
                exp.at[:, pl.ds(pl.multiple_of(1024 * half + 256 * x, 256), 256)],
                w1.at[y, x, c, :, pl.ds(256 * half, 256)],
                ls.at[3 + half],
            )
        )
    lines = []
    for i, (src, dst) in enumerate(
        ((in_in, inscale), (hid_in, hidscale), (act_in, actscale), (out_in, outscale), (gain_in, gain))
    ):
        lines.append(pltpu.make_async_copy(src, dst, ls.at[5 + i]))
    for copy in lines + here:
        copy.start()
    pl.semaphore_wait(barrier, 19)
    tell_z(0)

    slot_of = {1: 1, 3: 2, 2: 3}
    vec_copies, exp_copies = {}, {}
    rows_here = pl.ds(pl.multiple_of(32 * h, 32), 32)
    rows_there = pl.ds(pl.multiple_of(32 * (1 - h), 32), 32)
    wide_here = pl.ds(pl.multiple_of(64 * h, 64), 64)
    for o in (1, 3, 2):
        for half in (0, 1):
            exp_copies[o, half] = go(remote(
                exp.at[rows_here, pl.ds(pl.multiple_of(1024 * half + 256 * xs[o], 256), 256)],
                w1.at[y, x, c, rows_here, pl.ds(256 * half, 256)],
                ws.at[o - 1, half], wr.at[o - 1, half], x=xs[o],
            ))
    shr_y = go(remote(shr.at[wide_here], w2.at[y, c, wide_here], ss.at[0], sr.at[0], y=oy))
    shr_n = go(remote(shr.at[wide_here], w2.at[y, c, wide_here], ss.at[3], sr.at[3], y=oy, h=1 - h))
    shr_c = go(remote(shr, w2.at[y, c], ss.at[1], sr.at[1], c=oc))
    for copy in lines:
        copy.wait()
    for xx in range(4):
        for i in (0, 1):
            vec[xx, i : i + 1] = inscale[:, SL * i : SL * i + SL]
            vec[xx, 2 + i : 3 + i] = outscale[:, SL * i : SL * i + SL]
            at = 1024 * i + 256 * xx
            vec[xx, 4:5, 256 * i : 256 * i + 256] = hidscale[:, at : at + 256]
            vec[xx, 5:6, 256 * i : 256 * i + 256] = actscale[:, at : at + 256]
        vec[xx, 6:8] = jnp.zeros((2, SL), f32)
    for o in (1, 3, 2):
        vec_copies[o] = go(remote(
            vec.at[xs[o]], vecs.at[slot_of[o]], vs.at[o - 1], vr.at[o - 1], x=xs[o]
        ))
    right_own, left_own = [], []
    for i, (lo, n) in enumerate(((0, HALF), (256, HALF), (512, SL))):
        piece = pl.ds(lo, n)
        right_own.append(remote(cot.at[0, :, piece], cots.at[1, :, piece], cs.at[i], cr.at[1, i], x=xs[1]))
    for i, (lo, n) in enumerate(((512, HALF), (768, HALF), (0, SL))):
        piece = pl.ds(lo, n)
        left_own.append(remote(cot.at[0, :, piece], cots.at[2, :, piece], cs.at[3 + i], cr.at[2, i], x=xs[3]))
    for i in range(3):
        go(right_own[i])
        go(left_own[i])

    vecs[0] = vec[x]
    here[0].wait()
    tokens = tbuf[...].astype(f32)
    centered = tokens - jnp.mean(tokens, axis=1, keepdims=True)
    variance = jnp.mean(centered * centered, axis=1, keepdims=True)
    inv = lax.rsqrt(variance + eps)
    normed[...] = centered * inv
    gained[...] = centered * inv * gain[...]
    invs[...] = jnp.broadcast_to(inv, invs.shape)
    total[...] = jnp.zeros_like(total)
    sacc[...] = jnp.zeros_like(sacc)
    eacc[...] = jnp.zeros_like(eacc)
    for copy in here[1:]:
        copy.wait()

    for o in (1, 3, 2):
        exp_copies[o, 0].wait_recv()
        exp_copies[o, 1].wait_recv()
    exp_h = []
    for o in (1, 2, 3):
        part = w1.at[y, xs[o], c, rows_here]
        exp_h.append(go(remote(part, part, es.at[o - 1], er.at[o - 1], h=1 - h)))
    part = w1.at[y, :, c, rows_here]
    exp_y = go(remote(part, part, es.at[3], er.at[3], y=oy))
    exp_n = go(remote(part, part, es.at[4], er.at[4], y=oy, h=1 - h))
    exp_c = go(remote(part, part, es.at[5], er.at[5], c=oc))
    shr_y.wait_recv()
    shr_n.wait_recv()
    shr_f = go(remote(w2.at[oy, c], w2.at[oy, c], ss.at[2], sr.at[2], c=oc))
    for o in (1, 3, 2):
        vec_copies[o].wait_recv()

    @pl.loop(0, 4)
    def _(k):
        si[k] = (gained[...] * row(vecs[k], 0)).astype(bf16)

    for copy in exp_h:
        copy.wait_recv()
    part = w1.at[y, :, c, rows_there]
    exp_d = go(remote(part, part, es.at[6], er.at[6], c=oc))

    fwd = []
    for i, lo in enumerate(PIECES):
        (right_own, left_own)[i % 2][i // 2].wait_recv()
        src, to = ((1, xs[1]), (2, xs[3]))[i % 2]
        piece = pl.ds(lo, HALF)
        fwd.append(go(remote(cots.at[src, :, piece], cots.at[3, :, piece], cs.at[6 + i], cr.at[3, i], x=to)))
    exp_y.wait_recv()
    exp_n.wait_recv()
    exp_f = go(remote(w1.at[oy, :, c], w1.at[oy, :, c], es.at[7], er.at[7], c=oc))
    for copy in (shr_c, exp_c, exp_d, shr_f, exp_f):
        copy.wait_recv()
    told(0, 2)
    tell_z(1)

    @pl.loop(0, 4)
    def _(k):
        v = vecs[k]
        project = dot(si[k], w1[...].reshape(D, SL), 1, 0)
        active, slope = gelu_pair(project * v[4:5])
        proj[k] = project
        actf[k] = active
        act[k] = (active * v[5:6]).astype(bf16)
        pa[k] = slope * v[5:6]

    told(1, 2)
    tell_z(2)

    def seeds(k, v, at):
        scale_out = row(v, 2)
        second = w2[...].reshape(SL, D)
        if at is None:
            return cots[k], scale_out, second
        cut = lambda m: jnp.concatenate([m[:, at : at + HALF], m[:, at + 512 : at + 512 + HALF]], axis=1)
        seed = jnp.concatenate([cots[k, :, at : at + HALF], cots[k, :, at + 512 : at + 512 + HALF]], axis=1)
        return seed, cut(scale_out), cut(second)

    def back_of(seed, scale_out, second):
        return dot((seed.astype(f32) * scale_out).astype(bf16), second, 1, 1)

    def back_part(v, back, k):
        return (back * pa[k] * v[4:5]).astype(bf16)

    def back_sums(back, k):
        grad_act = jnp.sum(back * actf[k], axis=0, keepdims=True)
        grad_hid = jnp.sum(back * pa[k] * proj[k], axis=0, keepdims=True)
        sv[k, 4:8] = jnp.concatenate([grad_hid, grad_act, jnp.zeros((2, SL), f32)], axis=0)

    def shrink_part(k, seed, second):
        both = dot(act[k], seed, 0, 0)
        return both, jnp.sum(second.astype(f32) * both, axis=0, keepdims=True)

    def expand_part(k, back_proj):
        eacc[...] += dot(si[k], back_proj, 0, 0)

    def norm_part(k, v, back_proj):
        back_norm = dot(back_proj, w1[...].reshape(D, SL), 1, 1)
        grad_in = jnp.sum(back_norm * gained[...], axis=0, keepdims=True)
        total[...] += back_norm * row(v, 0)
        sv[k, 0:2] = jnp.concatenate([grad_in[:, :SL], grad_in[:, SL:]], axis=0)

    @pl.loop(0, 3)
    def _(k):
        @pl.when(k == 1)
        def _():
            right_own[2].wait_recv()

        @pl.when(k == 2)
        def _():
            left_own[2].wait_recv()

        v = vecs[k]
        seed, scale_out, second = seeds(k, v, None)
        back = back_of(seed, scale_out, second)
        back_proj = back_part(v, back, k)
        back_sums(back, k)
        both, grad_out = shrink_part(k, seed, second)
        sacc[...] += both * scale_out
        sv[k, 2:4] = jnp.concatenate([grad_out[:, :SL], grad_out[:, SL:]], axis=0)
        expand_part(k, back_proj)
        norm_part(k, v, back_proj)

    right, left, far = (lax.rem(place + o, 4) for o in (1, 3, 2))
    to_right = dict(y=lax.rem(right, 2), h=right // 2)
    to_left = dict(y=lax.rem(left, 2), h=left // 2)
    top, low = pl.ds(0, 4), pl.ds(4, 4)

    def lanes(it):
        i, lo, hi = ITEMS[it]
        return i, slice(lo, hi), pl.ds(lo, hi - lo)

    def core_step(it):
        i, _, l = lanes(it)
        return go(remote(pbuf.at[i, oc, :, :, :, l], rbuf.at[i, :, :, :, l], as_.at[it], ar.at[it], c=oc))

    def ring_start(it, copy):
        i, v, l = lanes(it)
        copy.wait_recv()
        q[i, :, :, :, v] = added(pbuf[i, c, :, :, :, v], rbuf[i, :, :, :, v]).astype(bf16)
        return [
            go(remote(q.at[i, far, top, :, l], yb.at[i, 0, :, :, l], ys.at[it, 0], yr.at[it, 0], **to_right)),
            go(remote(q.at[i, far, low, :, l], yb.at[i, 1, :, :, l], ys.at[it, 1], yr.at[it, 1], **to_left)),
            go(remote(q.at[i, right, low, :, l], yb.at[i, 2, :, :, l], ys.at[it, 2], yr.at[it, 2], **to_right)),
            go(remote(q.at[i, left, top, :, l], yb.at[i, 3, :, :, l], ys.at[it, 3], yr.at[it, 3], **to_left)),
        ]

    def ring_pass(it, copies):
        i, v, l = lanes(it)
        copies[0].wait_recv()
        mix[i, 0, :, :, v] = added(q[i, right, 0:4, :, v], yb[i, 0, :, :, v]).astype(bf16)
        copies.append(go(remote(
            mix.at[i, 0, :, :, l], yb.at[i, 4, :, :, l], ys.at[it, 4], yr.at[it, 4], **to_right
        )))
        copies[1].wait_recv()
        mix[i, 1, :, :, v] = added(q[i, left, 4:8, :, v], yb[i, 1, :, :, v]).astype(bf16)
        copies.append(go(remote(
            mix.at[i, 1, :, :, l], yb.at[i, 5, :, :, l], ys.at[it, 5], yr.at[it, 5], **to_left
        )))

    def deep_start(it, copies):
        i, v, l = lanes(it)
        for copy in copies[2:]:
            copy.wait_recv()
        r[i, 0:4, :, v] = added(q[i, place, 0:4, :, v], yb[i, 3, :, :, v], yb[i, 4, :, :, v]).astype(bf16)
        r[i, 4:8, :, v] = added(q[i, place, 4:8, :, v], yb[i, 2, :, :, v], yb[i, 5, :, :, v]).astype(bf16)
        out = []
        if i == 0:
            for o in (4, 3, 5, 2, 6, 1, 7):
                e = lax.rem(z + o, 8)
                out.append(go(remote(r.at[0, e, :, l], rz.at[0, z, :, l], zs.at[it, o], zr.at[it, o], z=e)))
            rz[0, z, :, v] = r[0, z, :, v]
            return out
        mine = pl.ds(pl.multiple_of(128 * x, 128), 128)
        for o in (4, 3, 5, 2, 6, 1, 7, 0):
            e = lax.rem(z + o, 8)
            for xo in range(4):
                if o or xo:
                    block = pl.ds(pl.multiple_of(128 * xs[xo], 128), 128)
                    out.append(go(remote(
                        r.at[1, e, :, block], rz.at[1, z, :, mine], zs.at[2 + xo, o], zr.at[2 + xo, o],
                        z=e, x=xs[xo],
                    )))
        rz[1, z, :, mine] = r[1, z, :, mine]
        return out

    def deep_sum(it, copies):
        i, v, _ = lanes(it)
        for copy in copies:
            copy.wait_recv()
        done = added(*(rz[i, e, :, v] for e in range(8))).astype(bf16)
        res[i, :, v] = done
        return done

    peers = []
    for o in range(1, 16):
        e = lax.rem(me + o, 16)
        peers.append((o, dict(z=e // 2, h=lax.rem(e, 2))))

    def shrink_blocks(it, both, scale_out):
        _, lo, hi = ITEMS[it]
        for cc in (0, 1):
            for hh in (0, 1):
                for yy in (0, 1):
                    at = (yy * 2 + cc) * 128
                    new = both[at : at + 128, HALF * hh : HALF * hh + HALF] * scale_out[:, HALF * hh : HALF * hh + HALF]
                    block = sacc[at : at + 128, SL * hh + lo : SL * hh + hi] + new
                    pbuf[0, cc, 2 * hh + yy, :, :, lo:hi] = block.astype(bf16).reshape(8, 16, HALF)

    told(2, 2)
    greet(heard.at[3], h=1 - h)
    v = vecs[3]
    fwd[0].wait_recv()
    fwd[1].wait_recv()
    seed, scale_out, second = seeds(3, v, 0)
    both, grad_first = shrink_part(3, seed, second)
    shrink_blocks(0, both, scale_out)
    core_s = core_step(0)
    half_back[...] = back_of(seed, scale_out, second)
    told(3, 1)
    for o in (1, 2, 3):
        greet(heard.at[4], x=xs[o])
    ring_s = ring_start(0, core_s)

    fwd[2].wait_recv()
    fwd[3].wait_recv()
    seed, scale_out, second = seeds(3, v, HALF)
    back = half_back[...] + back_of(seed, scale_out, second)
    back_proj = back_part(v, back, 3)
    expand_part(3, back_proj)
    for cc in (0, 1):
        for hh in (0, 1):
            for yy in (0, 1):
                for xx in range(4):
                    at = ((yy * 4 + xx) * 2 + cc) * 64
                    for zz in range(8):
                        top_row, lane = at + zz // 2 * 16, (zz % 2 * 2 + hh) * 128
                        pbuf[1, cc, 2 * hh + yy, zz, :, 128 * xx : 128 * xx + 128] = eacc[
                            top_row : top_row + 16, lane : lane + 128
                        ].astype(bf16)
    core_e = core_step(2)
    ring_pass(0, ring_s)
    both, grad_last = shrink_part(3, seed, second)
    shrink_blocks(1, both, scale_out)
    core_l = core_step(1)
    ring_e = ring_start(2, core_e)
    back_sums(back, 3)
    norm_part(3, v, back_proj)
    ring_l = ring_start(1, core_l)
    told(4, 3)
    deep_s = deep_start(0, ring_s)
    sv[3, 2:4] = jnp.concatenate(
        [
            jnp.concatenate([grad_first[:, :HALF], grad_last[:, :HALF]], axis=1),
            jnp.concatenate([grad_first[:, HALF:], grad_last[:, HALF:]], axis=1),
        ],
        axis=0,
    )

    outs = (sh, ex)

    def spread(it):
        i, _, l = lanes(it)
        copies = {}
        for o in (2, 6, 1, 7, 0):
            e = lax.rem(z + o, 8)
            for ho in (0, 1):
                if o or ho:
                    copies[o, ho] = go(remote(
                        res.at[i, :, l], outs[i].at[me, :, l], hs.at[it, o, ho], hr.at[it, o, ho],
                        z=e, h=1 - h if ho else h,
                    ))
        return copies

    def relay(it, copies):
        i, _, l = lanes(it)
        for o, further in ((2, (4, 3)), (6, (5,))):
            for ho in (0, 1):
                copies[o, ho].wait_recv()
                part = outs[i].at[lax.rem(z + 8 - o, 8) * 2 + (1 - h if ho else h), :, l]
                for far_o in further:
                    copies[far_o, ho] = go(remote(
                        part, part, hs.at[it, far_o, ho], hr.at[it, far_o, ho],
                        z=lax.rem(z + far_o - o + 8, 8),
                    ))

    vector_copies = []
    for slot, xo in ((1, 3), (2, 1), (3, 2)):
        vector_copies.append(go(remote(sv.at[slot], svr.at[x], bs.at[xo - 1], br.at[xo - 1], x=xs[xo])))
    svr[x] = sv[0]
    whole = total[...]
    gp[...] = jnp.sum(whole * normed[...], axis=0, keepdims=True)
    gains = []
    for o in range(1, 16):
        yo, xo, co = o // 8, (o // 2) % 4, o % 2
        gains.append(go(remote(
            gp, gpr.at[chip * 2 + c], gs.at[o], gr.at[o], y=oy if yo else y, x=xs[xo], c=oc if co else c
        )))
    gpr[chip * 2 + c] = gp[...]
    unit = whole * gain[...]
    inner = jnp.mean(unit * normed[...], axis=1, keepdims=True)
    back_trunk = invs[:, :1] * (unit - jnp.mean(unit, axis=1, keepdims=True) - normed[...] * inner)
    term = (cots[0].astype(f32) + back_trunk).astype(bf16)
    t[0] = term[:CUT]
    t[1, : TOK - CUT] = term[CUT:]
    t[1, TOK - CUT :] = jnp.zeros((FULL - TOK, D), bf16)
    core_t = go(remote(t.at[oc], rt, as_.at[3], ar.at[3], c=oc))

    ring_pass(2, ring_e)
    ring_pass(1, ring_l)
    deep_e = deep_start(2, ring_e)
    first_sends = len(sent)
    deep_l = deep_start(1, ring_l)

    core_t.wait_recv()
    joint = added(t[c], rt[...]).astype(bf16)
    for g in range(8):
        tq[g] = joint[:, 128 * g : 128 * g + 128]
    tiles = []
    for g in range(1, 8):
        yo, xo = g // 4, g % 4
        ty, tx = oy if yo else y, xs[xo]
        tiles.append(go(remote(tq.at[ty * 4 + tx], tr.at[chip], ts.at[g], tr_.at[g], y=ty, x=tx)))
    tr[chip] = tq[chip]

    done = deep_sum(0, deep_s)
    spread_s = spread(0)
    sh[me, :, :HALF] = done

    for copy in vector_copies + gains:
        copy.wait_recv()
    sums = svr[0] + svr[1] + svr[2] + svr[3]
    gain_sum = gpr[0]
    for m in range(1, 16):
        gain_sum = gain_sum + gpr[m]
    zero = jnp.zeros((1, SL), f32)
    for i in range(4):
        dv[i] = sums[i : i + 1]
        dv[4 + i] = svr[i, 4:5]
        dv[8 + i] = svr[i, 5:6]
    dv[12] = gain_sum[:, :SL]
    dv[13] = gain_sum[:, SL:]
    dv[14] = zero
    dv[15] = zero
    small = []
    for o, where in peers:
        e = where["z"] * 2 + where["h"]
        small.append(go(remote(dv.at[e], dvr.at[me], ds.at[o], dr.at[o], **where)))
    dvr[me] = dv[me]

    drain(first_sends)
    other_sends = len(sent)
    done = deep_sum(2, deep_e)
    spread_e = spread(2)
    ex[me] = done
    done = deep_sum(1, deep_l)
    spread_l = spread(1)
    sh[me, :, HALF:] = done
    for copy in small:
        copy.wait_recv()
    line = dvr[0]
    for p in range(1, 16):
        line = line + dvr[p]
    dvs[...] = line
    lines = []
    for o, where in peers:
        lines.append(go(remote(dvs, dvo.at[me], os_.at[o], or_.at[o], **where)))
    dvo[me] = line
    relay(0, spread_s)

    for copy in tiles:
        copy.wait_recv()
    tf[c] = added(*(tr[g] for g in range(8))).astype(bf16)
    finish = go(remote(tf.at[c], tf.at[c], fs, fr, c=oc))

    drain(other_sends)
    relay(2, spread_e)
    relay(1, spread_l)

    for copy in [finish] + lines:
        copy.wait_recv()
    for copies in (spread_s, spread_e, spread_l):
        for (o, ho), copy in copies.items():
            if o not in (2, 6):
                copy.wait_recv()

    drain(len(sent))


def finish_kernel(tf, sh, ex, dvo, tg, eg, sg, ing, hg, ag, og, gg):
    c = lax.axis_index("c")
    turned = tf[...].reshape(FULL, 128).astype(f32).T
    tg[...] = jnp.where(c == 0, turned[:64], turned[64:])[:, :TOK].astype(bf16)
    for i in (0, 1):
        ing[:, SL * i : SL * i + SL] = dvo[i]
        og[:, SL * i : SL * i + SL] = dvo[2 + i]
        gg[:, SL * i : SL * i + SL] = dvo[12 + i]
        for xx in range(4):
            at = 1024 * i + 256 * xx
            hg[:, at : at + 256] = dvo[4 + xx][:, 256 * i : 256 * i + 256]
            ag[:, at : at + 256] = dvo[8 + xx][:, 256 * i : 256 * i + 256]
    for p in range(16):
        low, lane = p // 4 * 16, p % 4 // 2 * 1024 + p % 2 * 128
        for xx in range(4):
            at = lane + 256 * xx
            eg[low : low + 16, at : at + 128] = ex[p, :, 128 * xx : 128 * xx + 128].astype(f32)
        sg[16 * (p // 2) : 16 * (p // 2) + 16, SL * (p % 2) : SL * (p % 2) + SL] = sh[p].astype(f32)


def vmem(n):
    return [pl.BlockSpec(memory_space=pltpu.VMEM)] * n


def dma(*shape):
    return pltpu.SemaphoreType.DMA(shape)


def body(trunk, normgain, expand, shrink, inscale, hidscale, actscale, outscale, cotangent):
    S = jax.ShapeDtypeStruct
    V = pltpu.VMEM
    parts = pl.pallas_call(
        kernel,
        out_shape=[
            V((2, CUT, 128), bf16),
            V((16, 16, SL), bf16),
            V((16, 16, SL), bf16),
            V((16, 1, SL), f32),
        ],
        in_specs=[pl.BlockSpec(memory_space=pl.ANY)] * 9,
        out_specs=vmem(4),
        scratch_shapes=[
            V((1, D), f32),
            V((1, D), f32),
            V((1, FF), f32),
            V((1, FF), f32),
            V((1, D), f32),
            V((TOK, D), bf16),
            V((4, 8, SL), f32),
            V((TOK, D), f32),
            V((TOK, D), f32),
            V((TOK, 128), f32),
            V((4, TOK, D), bf16),
            V((2, 4, 2, 64, SL), bf16),
            V((2, 2, 128, D), bf16),
            V((4, 8, SL), f32),
            V((4, TOK, D), bf16),
            V((4, TOK, SL), bf16),
            V((4, TOK, SL), f32),
            V((4, TOK, SL), f32),
            V((4, TOK, SL), f32),
            V((TOK, D), f32),
            V((SL, D), f32),
            V((D, SL), f32),
            V((TOK, SL), f32),
            V((2, 2, 4, 8, 16, SL), bf16),
            V((2, 4, 8, 16, SL), bf16),
            V((2, CUT, D), bf16),
            V((CUT, D), bf16),
            V((2, 4, 8, 16, SL), bf16),
            V((2, 6, 4, 16, SL), bf16),
            V((2, 2, 4, 16, SL), bf16),
            V((2, 8, 16, SL), bf16),
            V((2, 8, 16, SL), bf16),
            V((2, 16, SL), bf16),
            V((8, CUT, 128), bf16),
            V((8, CUT, 128), bf16),
            V((4, 8, SL), f32),
            V((4, 8, SL), f32),
            V((1, D), f32),
            V((16, 1, D), f32),
            V((16, 1, SL), f32),
            V((16, 1, SL), f32),
            V((1, SL), f32),
            dma(10), dma(10), dma(4, 4), dma(3, 2), dma(3, 2), dma(3), dma(3), dma(4), dma(4), dma(8), dma(8),
            dma(4), dma(4), dma(3, 6), dma(3, 6), dma(6, 8), dma(6, 8), dma(3, 8, 2), dma(3, 8, 2),
            dma(8), dma(8), pltpu.SemaphoreType.DMA, pltpu.SemaphoreType.DMA, dma(3), dma(3), dma(16), dma(16),
            dma(16), dma(16), dma(16), dma(16), pltpu.SemaphoreType.REGULAR((5,)),
        ],
        compiler_params=pltpu.CompilerParams(
            collective_id=0, has_side_effects=True, vmem_limit_bytes=60 * 1024 * 1024
        ),
        name="exchange_compute",
    )(
        trunk, expand, shrink, cotangent, normgain.reshape(1, D), inscale, hidscale, actscale, outscale
    )
    tg, eg, sg, ing, hg, ag, og, gg = pl.pallas_call(
        finish_kernel,
        out_shape=[
            S((64, TOK), bf16),
            S((64, FF), f32),
            S((128, D), f32),
            S((1, D), f32),
            S((1, FF), f32),
            S((1, FF), f32),
            S((1, D), f32),
            S((1, D), f32),
        ],
        in_specs=vmem(4),
        out_specs=vmem(8),
        name="write_outputs",
    )(*(pltpu.with_memory_space_constraint(part, pltpu.VMEM) for part in parts))
    return tg.T, eg, sg, ing, hg, ag, og, gg.reshape(D)


def solution(mesh):
    finer = Mesh(mesh.devices.reshape(2, 4, 2, 8, 2), AXES)
    rows = P(MEMBER, None)
    in_specs = (P(DP, None), P(), rows, rows, rows, rows, rows, rows, P(MEMBER, DP, None))
    out_specs = (P(DP, MEMBER), rows, rows, rows, rows, rows, rows, P())
    return jax.shard_map(body, mesh=finer, in_specs=in_specs, out_specs=out_specs, check_vma=False)
```
